32 devices in a mesh: grp: 4 (over y, x), col: 8 (over z, core).
Axes of the slice: x: 2, y: 2, z: 4, core: 2. Of those that a mesh axis runs over, the one named last changes fastest.
Arguments:
- start_block: float32 [16, 8192], P(None, ('grp', 'col')), may hold values from -6 to 6
- tile_values: float32 [4, 8, 32, 256, 256], P('grp', 'col'), may hold values from 0 to 1, as said below
- tile_row: int32 [4, 8, 32], P('grp', 'col'), may hold values from 0 to 31, as said below
- tile_col: int32 [4, 8, 32], P('grp', 'col'), may hold values from 0 to 31, as said below
- tile_count: int32 [4, 8], P('grp', 'col'), may hold values from 8 to 32, as said below
Outputs:
- basis: float32 [5, 16, 8192], P(None, None, ('grp', 'col'))
- projections: float32 [4, 4, 16, 16], replicated
- factors: float32 [5, 16, 16], replicated
The draws below stay inside these ranges and needn't reach their ends.
Inputs may be any that keep to these rules, and one draw needn't show every extreme that they name: `tile_row`: A tile of the device at grp index g lies in tile rows g * 8 * 1 to (g + 1) * 8 - 1. `tile_col`: A tile column t of the device at col index c has (t) % 8 == c. Coordinate pairs may repeat; repeated tiles add. The live tiles of a device are its first tile_count slots; some device has all 32 slots live. `tile_values`: entries are nonnegative.
All inputs are finite; a program needn't handle non-finite values.
Results may differ from the reference program's by a relative error of at most 0.0003.
Values sent between devices are 32-bit elements; how exact they have to be, the bound alone decides.
A program may use at most 64 MiB of HBM per device.

```python
import math
import jax
import jax.numpy as jnp
from jax import lax

TILE = 256
BLOCK = 16
ITERS = 4
ROW_TILES = 1
SLOTS = 32
NODES = 8192
N_GRP = 4
N_COL = 8


def draw_tile_row(key, part):
    offsets = jax.random.randint(jax.random.fold_in(key, 11), (N_GRP, N_COL, SLOTS), 0, N_COL * ROW_TILES, dtype=jnp.int32)
    groups = jnp.arange(N_GRP, dtype=jnp.int32)[:, None, None]
    return groups * (N_COL * ROW_TILES) + offsets


def draw_tile_col(key, part):
    group_pick = jax.random.randint(jax.random.fold_in(key, 21), (N_GRP, N_COL, SLOTS), 0, N_GRP, dtype=jnp.int32)
    within = jax.random.randint(jax.random.fold_in(key, 22), (N_GRP, N_COL, SLOTS), 0, ROW_TILES, dtype=jnp.int32)
    columns = jnp.arange(N_COL, dtype=jnp.int32)[None, :, None]
    return (group_pick * N_COL + columns) * ROW_TILES + within


def draw_tile_count(key, part):
    counts = jax.random.randint(jax.random.fold_in(key, 31), (N_GRP, N_COL), max(1, SLOTS // 4), SLOTS + 1, dtype=jnp.int32)
    chosen = jax.random.randint(jax.random.fold_in(key, 32), (), 0, N_GRP * N_COL, dtype=jnp.int32)
    flat_index = jnp.arange(N_GRP * N_COL, dtype=jnp.int32).reshape(N_GRP, N_COL)
    return jnp.where(flat_index == chosen, SLOTS, counts).astype(jnp.int32)


def draw_tile_values(key, part):
    array_shape = (N_GRP, N_COL, SLOTS, TILE, TILE)
    lowest = 0.1
    entries = jax.random.uniform(jax.random.fold_in(key, 41), array_shape, jnp.float32)
    row_scale = jnp.exp(jax.random.uniform(jax.random.fold_in(key, 42), (N_GRP, N_COL, SLOTS, TILE, 1), jnp.float32, math.log(lowest), 0.0))
    col_scale = jnp.exp(jax.random.uniform(jax.random.fold_in(key, 43), (N_GRP, N_COL, SLOTS, 1, TILE), jnp.float32, math.log(lowest), 0.0))
    return entries * row_scale * col_scale * (20.0 * ROW_TILES / (SLOTS * TILE))


def block_scale(stream_key, shape, cuts, low, largest):
    level = 1.0
    for axis_at, blocks in cuts:
        draws = jax.random.uniform(jax.random.fold_in(jax.random.fold_in(stream_key, 6), axis_at), (blocks,), jnp.float32, low / len(cuts), largest / len(cuts))
        level = level * jnp.repeat(jnp.exp(draws), shape[axis_at] // blocks).reshape((-1,) + (1,) * (len(shape) - 1 - axis_at))
    return level


def noise(key, dims, deviation, limit, cuts=(), held_as=jnp.bfloat16):
    drawn = deviation * jax.random.normal(key, dims, jnp.float32)
    if cuts:
        drawn = drawn * block_scale(key, dims, cuts, -0.22, 0.18)
    return jnp.clip(drawn, -limit, limit).astype(held_as)


def setup_inputs(seed: int = 0) -> dict:
    splits = jax.random.split(jax.random.key(seed), 6)
    start_block = noise(splits[0], (BLOCK, NODES), 1.0, 6.0, ((1, 32),), jnp.float32)
    tile_values = draw_tile_values(jax.random.fold_in(splits[5], 71), 0)
    tile_row = draw_tile_row(jax.random.fold_in(splits[5], 71), 0)
    tile_col = draw_tile_col(jax.random.fold_in(splits[5], 71), 0)
    tile_count = draw_tile_count(jax.random.fold_in(splits[5], 71), 0)
    return {"start_block": start_block, "tile_values": tile_values, "tile_row": tile_row, "tile_col": tile_col, "tile_count": tile_count}


highest = lax.Precision.HIGHEST

def apply_weights(vector, flat_tiles, flat_rows, flat_cols, flat_live):

    def visit_tile(running, scan_item):
        tile_block, row_tile, col_tile, weight = scan_item
        row_start = (row_tile * TILE).astype(jnp.int32)
        col_start = (col_tile * TILE).astype(jnp.int32)
        col_piece = lax.dynamic_slice_in_dim(vector, col_start, TILE, 1)
        row_piece = lax.dynamic_slice_in_dim(vector, row_start, TILE, 1)
        into_rows = jnp.dot(col_piece, tile_block.T, precision=highest) * weight
        into_cols = jnp.dot(row_piece, tile_block, precision=highest) * weight
        current = lax.dynamic_slice_in_dim(running, row_start, TILE, 1)
        running = lax.dynamic_update_slice_in_dim(running, current + into_rows, row_start, 1)
        current = lax.dynamic_slice_in_dim(running, col_start, TILE, 1)
        running = lax.dynamic_update_slice_in_dim(running, current + into_cols, col_start, 1)
        return (running, None)
    initial = jnp.zeros(vector.shape, jnp.float32)
    result, unused = lax.scan(visit_tile, initial, (flat_tiles, flat_rows, flat_cols, flat_live))
    return result

def orthonormal(block_rows):
    gram_now = jnp.dot(block_rows, block_rows.T, precision=highest) / NODES
    factor = jnp.linalg.cholesky(gram_now)
    solved = jax.scipy.linalg.solve_triangular(factor, block_rows, lower=True)
    return (solved, factor)

def reference(start_block, tile_values, tile_row, tile_col, tile_count):
    flat_tiles = tile_values.reshape(-1, TILE, TILE)
    flat_rows = tile_row.reshape(-1).astype(jnp.int32)
    flat_cols = tile_col.reshape(-1).astype(jnp.int32)
    live_mask = jnp.arange(SLOTS, dtype=jnp.int32)[None, None, :] < tile_count[:, :, None]
    flat_live = live_mask.reshape(-1).astype(jnp.float32)
    ones_row = jnp.ones((1, NODES), jnp.float32)
    degree = apply_weights(ones_row, flat_tiles, flat_rows, flat_cols, flat_live)

    def laplace(vector):
        return degree * vector - apply_weights(vector, flat_tiles, flat_rows, flat_cols, flat_live)
    first_block, factor = orthonormal(start_block)
    basis_list = [first_block]
    factor_list = [factor]
    projections = jnp.zeros((ITERS, ITERS, BLOCK, BLOCK), jnp.float32)
    for step_index in range(ITERS):
        applied = laplace(basis_list[-1])
        stacked = jnp.stack(basis_list)
        coeffs = jnp.einsum('an,jbn->jab', applied, stacked, precision=highest) / NODES
        applied = applied - jnp.einsum('jab,jbn->an', coeffs, stacked, precision=highest)
        next_block, factor = orthonormal(applied)
        basis_list.append(next_block)
        factor_list.append(factor)
        projections = projections.at[step_index, :step_index + 1].set(coeffs)
    return (jnp.stack(basis_list), projections, jnp.stack(factor_list))
```

```python
import functools

import jax
import jax.numpy as jnp
from jax import lax
from jax.experimental import pallas as pl
from jax.experimental.pallas import tpu as pltpu
from jax.sharding import PartitionSpec as P

ITERS = 4
HIGHEST = lax.Precision.HIGHEST
MESH = pl.DeviceIdType.MESH
F32 = jnp.float32
BF16 = jnp.bfloat16
I32 = jnp.int32
LANES = 128
CHUNK = 8


def dot_nt(left, right, precision=None):
    dims = (((1,), (1,)), ((), ()))
    return lax.dot_general(left, right, dims, precision=precision, preferred_element_type=F32)


def dot_nn(left, right, precision=None):
    dims = (((1,), (0,)), ((), ()))
    return lax.dot_general(left, right, dims, precision=precision, preferred_element_type=F32)


def split_two(value):
    high = value.astype(BF16)
    low = (value - high.astype(F32)).astype(BF16)
    return high, low


def factorize(gram):
    width = gram.shape[0]
    row = lax.broadcasted_iota(I32, gram.shape, 0)
    lane = lax.broadcasted_iota(I32, gram.shape, 1)
    unit = jnp.where(lane == row, 1.0, 0.0).astype(F32)
    work = jnp.where((lane >= width) & (lane < 2 * width), gram, unit)
    for j in range(width):
        column = jnp.broadcast_to(work[:, width + j : width + j + 1], work.shape)
        pivot_row = jnp.broadcast_to(work[j : j + 1, :], work.shape)
        pivot = jnp.broadcast_to(column[j : j + 1, :], work.shape)
        scale = jnp.where(row > j, column / pivot, 0.0)
        work = work - scale * pivot_row
    diagonal = jnp.sum(jnp.where(lane == row + width, work, 0.0), axis=1, keepdims=True)
    work = work / jnp.sqrt(diagonal)
    upper = jnp.where((lane < 2 * width) & (lane >= row + width), work, 0.0)
    inverse = jnp.where(lane <= row, work, 0.0)
    return upper, inverse


def factor_of(upper):
    width = upper.shape[0]
    return upper[:, width : 2 * width].T


def far_first(size):
    return sorted(range(1, size), key=lambda d: (-min(d, size - d), d)) + [0]


def kernel(
    grp_size, col_size, node_total,
    start_ref, tiles_ref, row_ref, col_ref, count_ref,
    basis_ref, proj_ref, factors_ref,
    raw, merged, high, low, rows_v, cols_v, table_v, table,
    u_ref, lr_ref, stack, lstack, row_panel, col_panel, row_split, col_split,
    acc_row, acc_col, got_row, got_col, deg_row, deg_col, deg_got_row, deg_got_col,
    degree_ref, sigma_ref, coeff_ref, red_col, red_grp, end_col, end_grp,
    tile_sem, in_sem, gather_row_sem, gather_col_sem, scatter_row_sem, scatter_col_sem,
    deg_row_sem, deg_col_sem, red_col_sem, red_grp_sem, end_col_sem, end_grp_sem,
):
    grp = lax.axis_index("grp")
    col = lax.axis_index("col")
    slots, tile_size = raw.shape[0], raw.shape[1]
    width = u_ref.shape[1]
    small = (width, LANES)
    row = lax.broadcasted_iota(I32, small, 0)
    lane = lax.broadcasted_iota(I32, small, 1)

    def load_tile(s):
        return pltpu.make_async_copy(tiles_ref.at[s], raw.at[s], tile_sem.at[s])

    loads = (
        pltpu.make_async_copy(start_ref, u_ref.at[0], in_sem.at[0]),
        pltpu.make_async_copy(row_ref, rows_v, in_sem.at[1]),
        pltpu.make_async_copy(col_ref, cols_v, in_sem.at[2]),
    )
    for copy in loads:
        copy.start()

    def start_load(s, carry):
        load_tile(s).start()
        return carry

    lax.fori_loop(0, slots, start_load, 0)

    barrier = pltpu.get_barrier_semaphore()

    def greet_col(d, carry):
        pl.semaphore_signal(
            barrier, inc=1, device_id=(grp, lax.rem(col + d, col_size)), device_id_type=MESH
        )
        return carry

    def greet_grp(d, carry):
        pl.semaphore_signal(
            barrier, inc=1, device_id=(lax.rem(grp + d, grp_size), col), device_id_type=MESH
        )
        return carry

    lax.fori_loop(1, col_size, greet_col, 0)
    lax.fori_loop(1, grp_size, greet_grp, 0)

    def copy_to(axis, d, source, target, sems):
        size = col_size if axis == "col" else grp_size
        peer = lax.rem((col if axis == "col" else grp) + d, size)
        return pltpu.make_async_remote_copy(
            src_ref=source(peer),
            dst_ref=target,
            send_sem=sems.at[0, d],
            recv_sem=sems.at[1, d],
            device_id=(grp, peer) if axis == "col" else (peer, col),
            device_id_type=MESH,
        )

    def exchange(axis, source, target, sems, start):
        size = col_size if axis == "col" else grp_size

        def visit(d, carry):
            copy = copy_to(axis, d, source, target, sems)
            if start:
                copy.start()
            else:
                copy.wait()
            return carry

        lax.fori_loop(1, size, visit, 0, unroll=size <= 8)

    def gather_col(par, start):
        exchange("grp", lambda peer: u_ref.at[par], col_panel.at[par, grp], gather_col_sem.at[par], start)

    def gather_row(par, start):
        exchange("col", lambda peer: u_ref.at[par], row_panel.at[par, col], gather_row_sem.at[par], start)

    def spread(axis, buf, sems, start):
        me = col if axis == "col" else grp
        exchange(axis, lambda peer: buf.at[me], buf.at[me], sems, start)

    def position(r, q):
        return table[0, r * grp_size + q]

    def send_rows(par, r, d, with_degree):
        copy_to("col", d, lambda peer: acc_row.at[r], got_row.at[par, col], scatter_row_sem.at[par]).start()
        if with_degree:
            copy_to("col", d, lambda peer: deg_row.at[r], deg_got_row.at[col], deg_row_sem).start()

    def halves(panel, par, size, split, with_degree):
        for place in range(size):
            first, second = split_two(panel[par, place])
            at = pl.ds(place * tile_size, tile_size)
            split[:width, at] = first
            split[width : 2 * width, at] = second
            if with_degree:
                split[2 * width :, at] = jnp.ones((width, tile_size), BF16)

    def rows_of(r, with_degree):
        left = col_split[...] if with_degree else col_split[: 2 * width]
        firsts = jnp.concatenate([high[position(r, q)] for q in range(grp_size)], axis=1)
        seconds = jnp.concatenate([low[position(r, q)] for q in range(grp_size)], axis=1)
        total = dot_nt(left, firsts)
        rest = dot_nt(left[:width], seconds)
        piece = total[:width] + total[width : 2 * width] + rest
        if not with_degree:
            return piece, None
        return piece, total[2 * width : 2 * width + 1] + dot_nt(left[2 * width :], seconds)[:1]

    def cols_of(q, with_degree):
        piece, degree = 0.0, 0.0
        chunk = CHUNK if col_size % CHUNK == 0 else 1
        for base in range(0, col_size, chunk):
            at = pl.ds(base * tile_size, chunk * tile_size)
            left = row_split[:, at] if with_degree else row_split[: 2 * width, at]
            places = [position(base + r, q) for r in range(chunk)]
            firsts = jnp.concatenate([high[p] for p in places], axis=0)
            seconds = jnp.concatenate([low[p] for p in places], axis=0)
            total = dot_nn(left, firsts)
            rest = dot_nn(left[:width], seconds)
            piece = piece + total[:width] + total[width : 2 * width] + rest
            if with_degree:
                extra = dot_nn(left[2 * width :], seconds)
                degree = degree + total[2 * width : 2 * width + 1] + extra[:1]
        return piece, degree

    def all_rows(par, with_degree):
        def visit(d, carry):
            r = lax.rem(col + d, col_size)
            piece, degree = rows_of(r, with_degree)
            acc_row[r] = piece
            if with_degree:
                deg_row[r] = degree
            return carry

        if col_size <= 8:
            order = far_first(col_size)
            for base in range(0, col_size, 4):
                for d in order[base : base + 4]:
                    visit(d, 0)
                for d in order[base : base + 4]:
                    if d:
                        send_rows(par, lax.rem(col + d, col_size), d, with_degree)
        else:
            def go(d, carry):
                visit(d, 0)
                send_rows(par, lax.rem(col + d, col_size), d, with_degree)
                return carry

            lax.fori_loop(1, col_size, go, 0)
            visit(0, 0)
        got_row[par, col] = acc_row[col]
        if with_degree:
            deg_got_row[col] = deg_row[col]

    def all_cols(par, with_degree):
        for d in far_first(grp_size):
            q = lax.rem(grp + d, grp_size)
            piece, degree = cols_of(q, with_degree)
            acc_col[q] = piece
            if with_degree:
                deg_col[q] = degree
        exchange("grp", lambda peer: acc_col.at[peer], got_col.at[par, grp], scatter_col_sem.at[par], True)
        got_col[par, grp] = acc_col[grp]
        if with_degree:
            exchange("grp", lambda peer: deg_col.at[peer], deg_got_col.at[grp], deg_col_sem, True)
            deg_got_col[grp] = deg_col[grp]

    def collect(par, with_degree):
        exchange("col", lambda peer: acc_row.at[peer], got_row.at[par, col], scatter_row_sem.at[par], False)
        exchange("grp", lambda peer: acc_col.at[peer], got_col.at[par, grp], scatter_col_sem.at[par], False)
        if with_degree:
            exchange("col", lambda peer: deg_row.at[peer], deg_got_row.at[col], deg_row_sem, False)
            exchange("grp", lambda peer: deg_col.at[peer], deg_got_col.at[grp], deg_col_sem, False)
            degree_ref[...] = jnp.sum(deg_got_row[...], axis=0) + jnp.sum(deg_got_col[...], axis=0)
        total = jnp.sum(got_row[par], axis=0) + jnp.sum(got_col[par], axis=0)
        return degree_ref[...] * u_ref[par] - total

    loads[0].wait()
    stack[...] = jnp.zeros_like(stack)
    lstack[...] = jnp.zeros_like(lstack)
    start = u_ref[0]
    stack[0] = start
    stack[1] = start
    row_panel[0, col] = start
    col_panel[0, grp] = start
    pl.semaphore_wait(barrier, col_size + grp_size - 2)
    gather_col(0, True)
    gather_row(0, True)

    loads[1].wait()
    loads[2].wait()
    spots = table.shape[1]
    offset = rows_v[...] - grp * col_size
    pick = lax.div(cols_v[...] - col, col_size)
    place = jnp.clip(offset, 0, col_size - 1) * grp_size + jnp.clip(pick, 0, grp_size - 1)
    square = (slots, slots)
    down = lax.broadcasted_iota(I32, square, 0)
    across = lax.broadcasted_iota(I32, square, 1)
    wide = jnp.broadcast_to(place, square)
    tall = jnp.sum(jnp.where(down == across, wide, 0), axis=1, keepdims=True)
    same = (wide == jnp.broadcast_to(tall, square)) & (down < across)
    before = jnp.max(jnp.where(same, down, -1), axis=0, keepdims=True)
    before = jnp.where(before < 0, slots, before)
    long = (slots, spots)
    depth = lax.broadcasted_iota(I32, long, 0)
    spot = lax.broadcasted_iota(I32, long, 1)
    here = (jnp.broadcast_to(tall, long) == spot) & (depth < count_ref[0])
    last = jnp.max(jnp.where(here, depth, -1), axis=0, keepdims=True)
    table_v[0:1, :] = jnp.where(last < 0, slots, last)
    table_v[1:2, :slots] = before
    move = pltpu.make_async_copy(table_v, table, in_sem.at[3])
    move.start()
    empty = jnp.zeros((tile_size, tile_size), F32)
    merged[slots] = empty
    high[slots] = empty.astype(BF16)
    low[slots] = empty.astype(BF16)
    move.wait()

    def merge(s, carry):
        load_tile(s).wait()
        value = raw[s] + merged[table[1, s]]
        merged[s] = value
        first, second = split_two(value)
        high[s] = first
        low[s] = second
        return carry

    lax.fori_loop(0, slots, merge, 0)

    gather_col(0, False)
    halves(col_panel, 0, grp_size, col_split, True)
    all_rows(0, True)
    gather_row(0, False)
    halves(row_panel, 0, col_size, row_split, True)
    all_cols(0, True)
    applied = collect(0, True)
    lr_ref[...] = applied
    u_ref[1] = applied
    sigma_ref[...] = jnp.zeros_like(sigma_ref)

    def settle(total, inverse):
        left = inverse[:, :width]
        fresh = dot_nn(left, jnp.concatenate([stack[1], lr_ref[...]], axis=1), HIGHEST)
        newest, image = fresh[:, :tile_size], fresh[:, tile_size:]
        pad = jnp.concatenate([inverse, jnp.zeros((LANES - width, LANES), F32)], axis=0)
        mixed = dot_nt(total[:, :width], pad[:, :width], HIGHEST)
        coeffs = jnp.where(lane < width, mixed, jnp.where((lane >= 2 * width) & (lane < 5 * width), total, 0.0))
        stack[0] = newest
        lstack[0] = image
        return left, newest, image, coeffs

    def step(k, carry):
        par = lax.rem(k + 1, 2)
        row_panel[par, col] = u_ref[par]
        col_panel[par, grp] = u_ref[par]
        gather_col(par, True)
        gather_row(par, True)
        block = stack[0:4].reshape(4 * width, tile_size)
        block = jnp.concatenate([block, block], axis=0)
        both = dot_nt(jnp.concatenate([u_ref[par], stack[1]], axis=0), block, HIGHEST)
        gram_lanes = (lax.rem(lane, 4 * width) >= width) & (lax.rem(lane, 4 * width) < 2 * width)
        part = jnp.where(gram_lanes, both[width:], both[:width])
        half = width // 2
        red_col[par, col] = jnp.where(lane[:half] < LANES // 2, part[:half], part[half:])
        spread("col", red_col.at[par], red_col_sem.at[par], True)

        gather_col(par, False)
        halves(col_panel, par, grp_size, col_split, False)
        all_rows(par, False)

        spread("col", red_col.at[par], red_col_sem.at[par], False)
        red_grp[par, grp] = jnp.sum(red_col[par], axis=0)
        spread("grp", red_grp.at[par], red_grp_sem.at[par], True)

        gather_row(par, False)
        halves(row_panel, par, col_size, row_split, False)
        all_cols(par, False)

        spread("grp", red_grp.at[par], red_grp_sem.at[par], False)
        packed = jnp.sum(red_grp[par], axis=0) / node_total
        total = jnp.concatenate([packed, pltpu.roll(packed, LANES // 2, 1)], axis=0)
        total = jnp.where(lane < LANES // 2, total, 0.0)
        upper, inverse = factorize(total)
        left, newest, image, coeffs = settle(total, inverse)
        factors_ref[k] = factor_of(upper)
        basis_ref[k] = newest
        now = dot_nn(coeffs, jnp.concatenate([stack[...].reshape(LANES, tile_size),
                                              lstack[...].reshape(LANES, tile_size)], axis=1), HIGHEST)
        residual = dot_nn(left, u_ref[par] - now[:, :tile_size], HIGHEST)
        known = now[:, tile_size:]
        found = dot_nn(left, coeffs, HIGHEST)
        found = found + jnp.where(lane == row, sigma_ref[:, :LANES], 0.0)
        coeff_ref[k] = found
        mean = jnp.sum(jnp.where(lane == row, found, 0.0), axis=1, keepdims=True)
        mean = jnp.sum(mean, axis=0, keepdims=True) / width
        sigma = jnp.where(k == 0, jnp.broadcast_to(mean, sigma_ref.shape), sigma_ref[...])
        stack[k + 2] = newest
        lstack[k + 2] = image
        stack[0] = residual
        stack[1] = residual

        applied = collect(par, False)
        image_next = dot_nn(left, applied - known, HIGHEST)
        lr_ref[...] = image_next
        u_ref[1 - par] = image_next - sigma * residual
        sigma_ref[...] = sigma
        return carry

    lax.fori_loop(0, ITERS - 1, step, 0)

    k = ITERS - 1
    par = ITERS % 2
    block_u = u_ref[par]
    stack[5] = block_u
    both = dot_nt(jnp.concatenate([block_u, stack[1]], axis=0), stack[...].reshape(LANES, tile_size), HIGHEST)
    end_col[col] = jnp.where((lane >= width) & (lane < 2 * width), both[width:], both[:width])
    spread("col", end_col, end_col_sem, True)
    spread("col", end_col, end_col_sem, False)
    end_grp[grp] = jnp.sum(end_col[...], axis=0)
    spread("grp", end_grp, end_grp_sem, True)
    spread("grp", end_grp, end_grp_sem, False)
    total = jnp.sum(end_grp[...], axis=0) / node_total
    upper, inverse = factorize(total)
    left, newest, image, coeffs = settle(total, inverse)
    factors_ref[k] = factor_of(upper)
    basis_ref[k] = newest
    now = dot_nn(coeffs, stack[...].reshape(LANES, tile_size), HIGHEST)
    residual = dot_nn(left, block_u - now, HIGHEST)
    found = dot_nn(left, coeffs, HIGHEST)
    coeff_ref[k] = found + jnp.where(lane == row, sigma_ref[:, :LANES], 0.0)
    inner = total[:, 5 * width : 6 * width] - dot_nt(coeffs, coeffs, HIGHEST)
    outer = dot_nt(dot_nn(left, inner, HIGHEST), left, HIGHEST)
    gram = jnp.concatenate([outer] * (LANES // width), axis=1)
    upper, inverse = factorize(gram)
    factors_ref[ITERS] = factor_of(upper)
    basis_ref[ITERS] = dot_nn(inverse[:, :width], residual, HIGHEST)
    proj_ref[...] = jnp.zeros_like(proj_ref)
    for k in range(ITERS):
        for j in range(k):
            proj_ref[k, j] = coeff_ref[k, :, (j + 2) * width : (j + 3) * width]
        proj_ref[k, k] = coeff_ref[k, :, :width]


def solution(mesh):
    grp_size, col_size = mesh.shape["grp"], mesh.shape["col"]

    def body(start_block, tile_values, tile_row, tile_col, tile_count):
        width, shard_len = start_block.shape
        slots, tile_size = tile_values.shape[2], tile_values.shape[3]
        assert shard_len == tile_size and LANES // width == 8
        places = LANES // width
        node_total = shard_len * grp_size * col_size
        spots = -(-max(grp_size * col_size, slots) // LANES) * LANES
        vmem = pl.BlockSpec(memory_space=pltpu.VMEM)
        smem = pl.BlockSpec(memory_space=pltpu.SMEM)
        hbm = pl.BlockSpec(memory_space=pl.ANY)
        block = (width, tile_size)
        line = (1, tile_size)
        tiles = (slots + 1, tile_size, tile_size)
        packed = (width // 2, LANES)
        small = (width, LANES)

        def sems(*sizes):
            return pltpu.SemaphoreType.DMA(sizes)

        return pl.pallas_call(
            functools.partial(kernel, grp_size, col_size, node_total),
            out_shape=(
                jax.ShapeDtypeStruct((ITERS + 1,) + block, F32),
                jax.ShapeDtypeStruct((ITERS, ITERS, width, width), F32),
                jax.ShapeDtypeStruct((ITERS + 1, width, width), F32),
            ),
            in_specs=[hbm, hbm, hbm, hbm, smem],
            out_specs=(vmem, vmem, vmem),
            scratch_shapes=[
                pltpu.VMEM((slots, tile_size, tile_size), F32),
                pltpu.VMEM(tiles, F32),
                pltpu.VMEM(tiles, BF16),
                pltpu.VMEM(tiles, BF16),
                pltpu.VMEM((1, slots), I32),
                pltpu.VMEM((1, slots), I32),
                pltpu.VMEM((8, spots), I32),
                pltpu.SMEM((8, spots), I32),
                pltpu.VMEM((2,) + block, F32),
                pltpu.VMEM(block, F32),
                pltpu.VMEM((places,) + block, F32),
                pltpu.VMEM((places,) + block, F32),
                pltpu.VMEM((2, col_size) + block, F32),
                pltpu.VMEM((2, grp_size) + block, F32),
                pltpu.VMEM((3 * width, col_size * tile_size), BF16),
                pltpu.VMEM((3 * width, grp_size * tile_size), BF16),
                pltpu.VMEM((col_size,) + block, F32),
                pltpu.VMEM((grp_size,) + block, F32),
                pltpu.VMEM((2, col_size) + block, F32),
                pltpu.VMEM((2, grp_size) + block, F32),
                pltpu.VMEM((col_size,) + line, F32),
                pltpu.VMEM((grp_size,) + line, F32),
                pltpu.VMEM((col_size,) + line, F32),
                pltpu.VMEM((grp_size,) + line, F32),
                pltpu.VMEM(line, F32),
                pltpu.VMEM(block, F32),
                pltpu.VMEM((ITERS,) + small, F32),
                pltpu.VMEM((2, col_size) + packed, F32),
                pltpu.VMEM((2, grp_size) + packed, F32),
                pltpu.VMEM((col_size,) + small, F32),
                pltpu.VMEM((grp_size,) + small, F32),
                sems(slots),
                sems(4),
                sems(2, 2, col_size), sems(2, 2, grp_size),
                sems(2, 2, col_size), sems(2, 2, grp_size),
                sems(2, col_size), sems(2, grp_size),
                sems(2, 2, col_size), sems(2, 2, grp_size),
                sems(2, col_size), sems(2, grp_size),
            ],
            compiler_params=pltpu.CompilerParams(
                collective_id=0, has_side_effects=True, vmem_limit_bytes=60 * 1024 * 1024
            ),
        )(
            start_block,
            tile_values.reshape(slots, tile_size, tile_size),
            tile_row.reshape(1, slots),
            tile_col.reshape(1, slots),
            tile_count.reshape(1),
        )

    in_specs = (
        P(None, ("grp", "col")),
        P("grp", "col", None, None, None),
        P("grp", "col", None),
        P("grp", "col", None),
        P("grp", "col"),
    )
    out_specs = (P(None, None, ("grp", "col")), P(), P())
    return jax.shard_map(body, mesh=mesh, in_specs=in_specs, out_specs=out_specs, check_vma=False)
```

```python
import functools

import jax
import jax.numpy as jnp
from jax import lax
from jax.experimental import pallas as pl
from jax.experimental.pallas import tpu as pltpu
from jax.sharding import PartitionSpec as P

ITERS = 4
HIGHEST = lax.Precision.HIGHEST
MESH = pl.DeviceIdType.MESH
F32 = jnp.float32
BF16 = jnp.bfloat16
I32 = jnp.int32
LANES = 128
CHUNK = 8
STRIDE = 4


def dot_nt(left, right, precision=None):
    dims = (((1,), (1,)), ((), ()))
    return lax.dot_general(left, right, dims, precision=precision, preferred_element_type=F32)


def dot_nn(left, right, precision=None):
    dims = (((1,), (0,)), ((), ()))
    return lax.dot_general(left, right, dims, precision=precision, preferred_element_type=F32)


def split_two(value):
    high = value.astype(BF16)
    low = (value - high.astype(F32)).astype(BF16)
    return high, low


def factorize(gram):
    width = gram.shape[0]
    shape = gram.shape
    row = lax.broadcasted_iota(I32, shape, 0)
    lane = lax.broadcasted_iota(I32, shape, 1)
    unit = jnp.where(lane == row, 1.0, 0.0).astype(F32)
    work = jnp.where((lane >= width) & (lane < 2 * width), gram, unit)
    diagonal = jnp.ones(shape, F32)
    for base in range(0, width, STRIDE):
        tall = [jnp.broadcast_to(work[:, width + base + i : width + base + i + 1], shape) for i in range(STRIDE)]
        wide = [jnp.broadcast_to(work[base + i : base + i + 1, :], shape) for i in range(STRIDE)]
        cell = {
            (m, i): jnp.broadcast_to(tall[i][base + m : base + m + 1, :], shape)
            for i in range(STRIDE)
            for m in range(i, STRIDE)
        }
        for i in range(STRIDE):
            inverse = 1.0 / cell[i, i]
            diagonal = jnp.where(row == base + i, cell[i, i], diagonal)
            scale = jnp.where(row > base + i, tall[i] * inverse, 0.0)
            work = work - scale * wide[i]
            for m in range(i + 1, STRIDE):
                ratio = cell[m, i] * inverse
                wide[m] = wide[m] - ratio * wide[i]
                tall[m] = tall[m] - scale * cell[m, i]
                for n in range(m, STRIDE):
                    cell[n, m] = cell[n, m] - ratio * cell[n, i]
    work = work / jnp.sqrt(diagonal)
    upper = jnp.where((lane < 2 * width) & (lane >= row + width), work, 0.0)
    inverse = jnp.where(lane <= row, work, 0.0)
    return upper, inverse


def factor_of(upper):
    width = upper.shape[0]
    return upper[:, width : 2 * width].T


def far_first(size):
    return sorted(range(1, size), key=lambda d: (-min(d, size - d), d)) + [0]


def kernel(
    grp_size, col_size, node_total,
    start_ref, tiles_ref, row_ref, col_ref, count_ref,
    basis_ref, proj_ref, factors_ref,
    raw, merged, high, low, high_t, low_t, rows_v, cols_v, table_v, table,
    u_ref, lr_ref, stack, lstack, row_panel, col_panel, row_split, col_split,
    acc_row, acc_col, got_row, got_col, deg_row, deg_col, deg_got_row, deg_got_col,
    degree_ref, sigma_ref, coeff_ref, red_col, red_grp, end_col, end_grp,
    tile_sem, in_sem, gather_row_sem, gather_col_sem, scatter_row_sem, scatter_col_sem,
    deg_row_sem, deg_col_sem, red_col_sem, red_grp_sem, end_col_sem, end_grp_sem,
):
    grp = lax.axis_index("grp")
    col = lax.axis_index("col")
    slots, tile_size = raw.shape[0], raw.shape[1]
    width = u_ref.shape[1]
    small = (width, LANES)
    row = lax.broadcasted_iota(I32, small, 0)
    lane = lax.broadcasted_iota(I32, small, 1)

    def load_tile(s):
        return pltpu.make_async_copy(tiles_ref.at[s], raw.at[s], tile_sem.at[s])

    loads = (
        pltpu.make_async_copy(start_ref, u_ref.at[0], in_sem.at[0]),
        pltpu.make_async_copy(row_ref, rows_v, in_sem.at[1]),
        pltpu.make_async_copy(col_ref, cols_v, in_sem.at[2]),
    )
    for copy in loads:
        copy.start()

    def start_load(s, carry):
        load_tile(s).start()
        return carry

    lax.fori_loop(0, slots, start_load, 0)

    barrier = pltpu.get_barrier_semaphore()

    def greet_col(d, carry):
        pl.semaphore_signal(
            barrier, inc=1, device_id=(grp, lax.rem(col + d, col_size)), device_id_type=MESH
        )
        return carry

    def greet_grp(d, carry):
        pl.semaphore_signal(
            barrier, inc=1, device_id=(lax.rem(grp + d, grp_size), col), device_id_type=MESH
        )
        return carry

    lax.fori_loop(1, col_size, greet_col, 0)
    lax.fori_loop(1, grp_size, greet_grp, 0)

    def copy_to(axis, d, source, target, sems):
        size = col_size if axis == "col" else grp_size
        peer = lax.rem((col if axis == "col" else grp) + d, size)
        return pltpu.make_async_remote_copy(
            src_ref=source(peer),
            dst_ref=target,
            send_sem=sems.at[0, d],
            recv_sem=sems.at[1, d],
            device_id=(grp, peer) if axis == "col" else (peer, col),
            device_id_type=MESH,
        )

    def exchange(axis, source, target, sems, start):
        size = col_size if axis == "col" else grp_size

        def visit(d, carry):
            copy = copy_to(axis, d, source, target, sems)
            if start:
                copy.start()
            else:
                copy.wait()
            return carry

        lax.fori_loop(1, size, visit, 0, unroll=size <= 8)

    def gather_col(par, start):
        exchange("grp", lambda peer: u_ref.at[par], col_panel.at[par, grp], gather_col_sem.at[par], start)

    def gather_row(par, start):
        exchange("col", lambda peer: u_ref.at[par], row_panel.at[par, col], gather_row_sem.at[par], start)

    def spread(axis, buf, sems, start):
        me = col if axis == "col" else grp
        exchange(axis, lambda peer: buf.at[me], buf.at[me], sems, start)

    def position(r, q):
        return table[0, r * grp_size + q]

    def send_rows(par, r, d, with_degree):
        copy_to("col", d, lambda peer: acc_row.at[r], got_row.at[par, col], scatter_row_sem.at[par]).start()
        if with_degree:
            copy_to("col", d, lambda peer: deg_row.at[r], deg_got_row.at[col], deg_row_sem).start()

    def halves(panel, par, size, split, with_degree):
        for place in range(size):
            first, second = split_two(panel[par, place])
            at = pl.ds(place * tile_size, tile_size)
            split[:width, at] = first
            if with_degree:
                split[width : 2 * width, at] = jnp.ones((width, tile_size), BF16)
                split[2 * width :, at] = second
            else:
                split[width : 2 * width, at] = second

    def combine(total, rest, with_degree):
        if not with_degree:
            return total[:width] + total[width:] + rest, None
        piece = total[:width] + total[2 * width :] + rest[:width]
        return piece, total[width : width + 1] + rest[width : width + 1]

    def rows_of(r, with_degree):
        places = [position(r, q) for q in range(grp_size)]
        if with_degree:
            left = col_split[...]
            firsts = jnp.concatenate([high[p] for p in places], axis=1)
            seconds = jnp.concatenate([low[p] for p in places], axis=1)
            return combine(dot_nt(left, firsts), dot_nt(left[: 2 * width], seconds), True)
        left = col_split[: 2 * width]
        firsts = jnp.concatenate([high_t[p] for p in places], axis=0)
        seconds = jnp.concatenate([low_t[p] for p in places], axis=0)
        return combine(dot_nn(left, firsts), dot_nn(left[:width], seconds), False)

    def cols_of(q, with_degree):
        piece, degree = 0.0, 0.0
        chunk = CHUNK if col_size % CHUNK == 0 else 1
        for base in range(0, col_size, chunk):
            at = pl.ds(base * tile_size, chunk * tile_size)
            left = row_split[:, at] if with_degree else row_split[: 2 * width, at]
            places = [position(base + r, q) for r in range(chunk)]
            firsts = jnp.concatenate([high[p] for p in places], axis=0)
            seconds = jnp.concatenate([low[p] for p in places], axis=0)
            rest = dot_nn(left[: 2 * width] if with_degree else left[:width], seconds)
            part, extra = combine(dot_nn(left, firsts), rest, with_degree)
            piece = piece + part
            if with_degree:
                degree = degree + extra
        return piece, degree

    def all_rows(par, with_degree):
        def visit(d, carry):
            r = lax.rem(col + d, col_size)
            piece, degree = rows_of(r, with_degree)
            acc_row[r] = piece
            if with_degree:
                deg_row[r] = degree
            return carry

        if col_size <= 8:
            order = far_first(col_size)
            for base in range(0, col_size, 4):
                for d in order[base : base + 4]:
                    visit(d, 0)
                for d in order[base : base + 4]:
                    if d:
                        send_rows(par, lax.rem(col + d, col_size), d, with_degree)
        else:
            def go(d, carry):
                visit(d, 0)
                send_rows(par, lax.rem(col + d, col_size), d, with_degree)
                return carry

            lax.fori_loop(1, col_size, go, 0)
            visit(0, 0)
        got_row[par, col] = acc_row[col]
        if with_degree:
            deg_got_row[col] = deg_row[col]

    def all_cols(par, with_degree):
        for d in far_first(grp_size):
            q = lax.rem(grp + d, grp_size)
            piece, degree = cols_of(q, with_degree)
            acc_col[q] = piece
            if with_degree:
                deg_col[q] = degree
        exchange("grp", lambda peer: acc_col.at[peer], got_col.at[par, grp], scatter_col_sem.at[par], True)
        got_col[par, grp] = acc_col[grp]
        if with_degree:
            exchange("grp", lambda peer: deg_col.at[peer], deg_got_col.at[grp], deg_col_sem, True)
            deg_got_col[grp] = deg_col[grp]

    def collect(par, with_degree):
        exchange("col", lambda peer: acc_row.at[peer], got_row.at[par, col], scatter_row_sem.at[par], False)
        exchange("grp", lambda peer: acc_col.at[peer], got_col.at[par, grp], scatter_col_sem.at[par], False)
        if with_degree:
            exchange("col", lambda peer: deg_row.at[peer], deg_got_row.at[col], deg_row_sem, False)
            exchange("grp", lambda peer: deg_col.at[peer], deg_got_col.at[grp], deg_col_sem, False)
            degree_ref[...] = jnp.sum(deg_got_row[...], axis=0) + jnp.sum(deg_got_col[...], axis=0)
        total = jnp.sum(got_row[par], axis=0) + jnp.sum(got_col[par], axis=0)
        return degree_ref[...] * u_ref[par] - total

    loads[0].wait()
    stack[...] = jnp.zeros_like(stack)
    lstack[...] = jnp.zeros_like(lstack)
    start = u_ref[0]
    stack[0] = start
    stack[1] = start
    row_panel[0, col] = start
    col_panel[0, grp] = start
    pl.semaphore_wait(barrier, col_size + grp_size - 2)
    gather_col(0, True)
    gather_row(0, True)

    loads[1].wait()
    loads[2].wait()
    spots = table.shape[1]
    offset = rows_v[...] - grp * col_size
    pick = lax.div(cols_v[...] - col, col_size)
    place = jnp.clip(offset, 0, col_size - 1) * grp_size + jnp.clip(pick, 0, grp_size - 1)
    square = (slots, slots)
    down = lax.broadcasted_iota(I32, square, 0)
    across = lax.broadcasted_iota(I32, square, 1)
    wide = jnp.broadcast_to(place, square)
    tall = jnp.sum(jnp.where(down == across, wide, 0), axis=1, keepdims=True)
    same = (wide == jnp.broadcast_to(tall, square)) & (down < across)
    before = jnp.max(jnp.where(same, down, -1), axis=0, keepdims=True)
    before = jnp.where(before < 0, slots, before)
    long = (slots, spots)
    depth = lax.broadcasted_iota(I32, long, 0)
    spot = lax.broadcasted_iota(I32, long, 1)
    here = (jnp.broadcast_to(tall, long) == spot) & (depth < count_ref[0])
    last = jnp.max(jnp.where(here, depth, -1), axis=0, keepdims=True)
    table_v[0:1, :] = jnp.where(last < 0, slots, last)
    table_v[1:2, :slots] = before
    move = pltpu.make_async_copy(table_v, table, in_sem.at[3])
    move.start()
    empty = jnp.zeros((tile_size, tile_size), F32)
    merged[slots] = empty
    high[slots] = empty.astype(BF16)
    low[slots] = empty.astype(BF16)
    high_t[slots] = empty.astype(BF16)
    low_t[slots] = empty.astype(BF16)
    move.wait()

    def merge(s, carry):
        load_tile(s).wait()
        value = raw[s] + merged[table[1, s]]
        merged[s] = value
        first, second = split_two(value)
        high[s] = first
        low[s] = second
        return carry

    lax.fori_loop(0, slots, merge, 0)

    gather_col(0, False)
    halves(col_panel, 0, grp_size, col_split, True)
    all_rows(0, True)
    gather_row(0, False)
    halves(row_panel, 0, col_size, row_split, True)
    all_cols(0, True)

    def turn(s, carry):
        high_t[s] = high[s].T
        low_t[s] = low[s].T
        return carry

    lax.fori_loop(0, slots, turn, 0, unroll=4)
    applied = collect(0, True)
    lr_ref[...] = applied
    u_ref[1] = applied
    sigma_ref[...] = jnp.zeros_like(sigma_ref)

    def settle(total, inverse):
        left = inverse[:, :width]
        fresh = dot_nn(left, jnp.concatenate([stack[1], lr_ref[...]], axis=1), HIGHEST)
        newest, image = fresh[:, :tile_size], fresh[:, tile_size:]
        pad = jnp.concatenate([inverse, jnp.zeros((LANES - width, LANES), F32)], axis=0)
        mixed = dot_nt(total[:, :width], pad[:, :width], HIGHEST)
        coeffs = jnp.where(lane < width, mixed, jnp.where((lane >= 2 * width) & (lane < 5 * width), total, 0.0))
        stack[0] = newest
        lstack[0] = image
        return left, newest, image, coeffs

    def step(k, carry):
        par = lax.rem(k + 1, 2)
        row_panel[par, col] = u_ref[par]
        col_panel[par, grp] = u_ref[par]
        gather_col(par, True)
        gather_row(par, True)
        block = stack[0:4].reshape(4 * width, tile_size)
        block = jnp.concatenate([block, block], axis=0)
        both = dot_nt(jnp.concatenate([u_ref[par], stack[1]], axis=0), block, HIGHEST)
        gram_lanes = (lax.rem(lane, 4 * width) >= width) & (lax.rem(lane, 4 * width) < 2 * width)
        part = jnp.where(gram_lanes, both[width:], both[:width])
        half = width // 2
        red_col[par, col] = jnp.where(lane[:half] < LANES // 2, part[:half], part[half:])
        spread("col", red_col.at[par], red_col_sem.at[par], True)

        gather_col(par, False)
        halves(col_panel, par, grp_size, col_split, False)
        all_rows(par, False)

        spread("col", red_col.at[par], red_col_sem.at[par], False)
        red_grp[par, grp] = jnp.sum(red_col[par], axis=0)
        spread("grp", red_grp.at[par], red_grp_sem.at[par], True)

        gather_row(par, False)
        halves(row_panel, par, col_size, row_split, False)
        all_cols(par, False)

        spread("grp", red_grp.at[par], red_grp_sem.at[par], False)
        packed = jnp.sum(red_grp[par], axis=0) / node_total
        total = jnp.concatenate([packed, pltpu.roll(packed, LANES // 2, 1)], axis=0)
        total = jnp.where(lane < LANES // 2, total, 0.0)
        upper, inverse = factorize(total)
        left, newest, image, coeffs = settle(total, inverse)
        factors_ref[k] = factor_of(upper)
        basis_ref[k] = newest
        now = dot_nn(coeffs, jnp.concatenate([stack[...].reshape(LANES, tile_size),
                                              lstack[...].reshape(LANES, tile_size)], axis=1), HIGHEST)
        residual = dot_nn(left, u_ref[par] - now[:, :tile_size], HIGHEST)
        known = now[:, tile_size:]
        found = dot_nn(left, coeffs, HIGHEST)
        found = found + jnp.where(lane == row, sigma_ref[:, :LANES], 0.0)
        coeff_ref[k] = found
        mean = jnp.sum(jnp.where(lane == row, found, 0.0), axis=1, keepdims=True)
        mean = jnp.sum(mean, axis=0, keepdims=True) / width
        sigma = jnp.where(k == 0, jnp.broadcast_to(mean, sigma_ref.shape), sigma_ref[...])
        stack[k + 2] = newest
        lstack[k + 2] = image
        stack[0] = residual
        stack[1] = residual

        applied = collect(par, False)
        image_next = dot_nn(left, applied - known, HIGHEST)
        lr_ref[...] = image_next
        u_ref[1 - par] = image_next - sigma * residual
        sigma_ref[...] = sigma
        return carry

    lax.fori_loop(0, ITERS - 1, step, 0)

    k = ITERS - 1
    par = ITERS % 2
    block_u = u_ref[par]
    stack[5] = block_u
    both = dot_nt(jnp.concatenate([block_u, stack[1]], axis=0), stack[...].reshape(LANES, tile_size), HIGHEST)
    end_col[col] = jnp.where((lane >= width) & (lane < 2 * width), both[width:], both[:width])
    spread("col", end_col, end_col_sem, True)
    spread("col", end_col, end_col_sem, False)
    end_grp[grp] = jnp.sum(end_col[...], axis=0)
    spread("grp", end_grp, end_grp_sem, True)
    spread("grp", end_grp, end_grp_sem, False)
    total = jnp.sum(end_grp[...], axis=0) / node_total
    upper, inverse = factorize(total)
    left, newest, image, coeffs = settle(total, inverse)
    factors_ref[k] = factor_of(upper)
    basis_ref[k] = newest
    now = dot_nn(coeffs, stack[...].reshape(LANES, tile_size), HIGHEST)
    residual = dot_nn(left, block_u - now, HIGHEST)
    found = dot_nn(left, coeffs, HIGHEST)
    coeff_ref[k] = found + jnp.where(lane == row, sigma_ref[:, :LANES], 0.0)
    inner = total[:, 5 * width : 6 * width] - dot_nt(coeffs, coeffs, HIGHEST)
    outer = dot_nt(dot_nn(left, inner, HIGHEST), left, HIGHEST)
    gram = jnp.concatenate([outer] * (LANES // width), axis=1)
    upper, inverse = factorize(gram)
    factors_ref[ITERS] = factor_of(upper)
    basis_ref[ITERS] = dot_nn(inverse[:, :width], residual, HIGHEST)
    proj_ref[...] = jnp.zeros_like(proj_ref)
    for k in range(ITERS):
        for j in range(k):
            proj_ref[k, j] = coeff_ref[k, :, (j + 2) * width : (j + 3) * width]
        proj_ref[k, k] = coeff_ref[k, :, :width]


def deliver(basis, proj, factors, basis_out, proj_out, factors_out, sem):
    pairs = ((basis, basis_out), (proj, proj_out), (factors, factors_out))
    copies = [pltpu.make_async_copy(source, target, sem.at[n]) for n, (source, target) in enumerate(pairs)]
    for copy in copies:
        copy.start()
    for copy in copies:
        copy.wait()


def solution(mesh):
    grp_size, col_size = mesh.shape["grp"], mesh.shape["col"]

    def body(start_block, tile_values, tile_row, tile_col, tile_count):
        width, shard_len = start_block.shape
        slots, tile_size = tile_values.shape[2], tile_values.shape[3]
        assert shard_len == tile_size and LANES // width == 8
        places = LANES // width
        node_total = shard_len * grp_size * col_size
        spots = -(-max(grp_size * col_size, slots) // LANES) * LANES
        vmem = pl.BlockSpec(memory_space=pltpu.VMEM)
        smem = pl.BlockSpec(memory_space=pltpu.SMEM)
        hbm = pl.BlockSpec(memory_space=pl.ANY)
        block = (width, tile_size)
        line = (1, tile_size)
        tiles = (slots + 1, tile_size, tile_size)
        packed = (width // 2, LANES)
        small = (width, LANES)

        def sems(*sizes):
            return pltpu.SemaphoreType.DMA(sizes)

        def pinned(value):
            return pltpu.with_memory_space_constraint(value, pltpu.HBM)

        shapes = (
            jax.ShapeDtypeStruct((ITERS + 1,) + block, F32),
            jax.ShapeDtypeStruct((ITERS, ITERS, width, width), F32),
            jax.ShapeDtypeStruct((ITERS + 1, width, width), F32),
        )
        results = pl.pallas_call(
            functools.partial(kernel, grp_size, col_size, node_total),
            out_shape=shapes,
            in_specs=[hbm, hbm, hbm, hbm, smem],
            out_specs=(vmem, vmem, vmem),
            scratch_shapes=[
                pltpu.VMEM((slots, tile_size, tile_size), F32),
                pltpu.VMEM(tiles, F32),
                pltpu.VMEM(tiles, BF16),
                pltpu.VMEM(tiles, BF16),
                pltpu.VMEM(tiles, BF16),
                pltpu.VMEM(tiles, BF16),
                pltpu.VMEM((1, slots), I32),
                pltpu.VMEM((1, slots), I32),
                pltpu.VMEM((8, spots), I32),
                pltpu.SMEM((8, spots), I32),
                pltpu.VMEM((2,) + block, F32),
                pltpu.VMEM(block, F32),
                pltpu.VMEM((places,) + block, F32),
                pltpu.VMEM((places,) + block, F32),
                pltpu.VMEM((2, col_size) + block, F32),
                pltpu.VMEM((2, grp_size) + block, F32),
                pltpu.VMEM((3 * width, col_size * tile_size), BF16),
                pltpu.VMEM((3 * width, grp_size * tile_size), BF16),
                pltpu.VMEM((col_size,) + block, F32),
                pltpu.VMEM((grp_size,) + block, F32),
                pltpu.VMEM((2, col_size) + block, F32),
                pltpu.VMEM((2, grp_size) + block, F32),
                pltpu.VMEM((col_size,) + line, F32),
                pltpu.VMEM((grp_size,) + line, F32),
                pltpu.VMEM((col_size,) + line, F32),
                pltpu.VMEM((grp_size,) + line, F32),
                pltpu.VMEM(line, F32),
                pltpu.VMEM(block, F32),
                pltpu.VMEM((ITERS,) + small, F32),
                pltpu.VMEM((2, col_size) + packed, F32),
                pltpu.VMEM((2, grp_size) + packed, F32),
                pltpu.VMEM((col_size,) + small, F32),
                pltpu.VMEM((grp_size,) + small, F32),
                sems(slots),
                sems(4),
                sems(2, 2, col_size), sems(2, 2, grp_size),
                sems(2, 2, col_size), sems(2, 2, grp_size),
                sems(2, col_size), sems(2, grp_size),
                sems(2, 2, col_size), sems(2, 2, grp_size),
                sems(2, col_size), sems(2, grp_size),
            ],
            compiler_params=pltpu.CompilerParams(
                collective_id=0, has_side_effects=True, vmem_limit_bytes=40 * 1024 * 1024
            ),
        )(
            pinned(start_block),
            pinned(tile_values.reshape(slots, tile_size, tile_size)),
            pinned(tile_row.reshape(1, slots)),
            pinned(tile_col.reshape(1, slots)),
            tile_count.reshape(1),
        )
        return pl.pallas_call(
            deliver,
            out_shape=shapes,
            in_specs=[vmem] * 3,
            out_specs=[hbm] * 3,
            scratch_shapes=[sems(3)],
        )(*(pltpu.with_memory_space_constraint(value, pltpu.VMEM) for value in results))

    in_specs = (
        P(None, ("grp", "col")),
        P("grp", "col", None, None, None),
        P("grp", "col", None),
        P("grp", "col", None),
        P("grp", "col"),
    )
    out_specs = (P(None, None, ("grp", "col")), P(), P())
    return jax.shard_map(body, mesh=mesh, in_specs=in_specs, out_specs=out_specs, check_vma=False)
```

```python
import functools

import jax
import jax.numpy as jnp
from jax import lax
from jax.experimental import pallas as pl
from jax.experimental.pallas import tpu as pltpu
from jax.sharding import PartitionSpec as P

ITERS = 4
HIGHEST = lax.Precision.HIGHEST
MESH = pl.DeviceIdType.MESH
F32 = jnp.float32
BF16 = jnp.bfloat16
I32 = jnp.int32
LANES = 128
CHUNK = 8
STRIDE = 4


def dot_nt(left, right, precision=None):
    dims = (((1,), (1,)), ((), ()))
    return lax.dot_general(left, right, dims, precision=precision, preferred_element_type=F32)


def dot_nn(left, right, precision=None):
    dims = (((1,), (0,)), ((), ()))
    return lax.dot_general(left, right, dims, precision=precision, preferred_element_type=F32)


def split_two(value):
    high = value.astype(BF16)
    low = (value - high.astype(F32)).astype(BF16)
    return high, low


def factorize(gram):
    width = gram.shape[0]
    shape = gram.shape
    row = lax.broadcasted_iota(I32, shape, 0)
    lane = lax.broadcasted_iota(I32, shape, 1)
    unit = jnp.where(lane == row, 1.0, 0.0).astype(F32)
    work = jnp.where((lane >= width) & (lane < 2 * width), gram, unit)
    diagonal = jnp.ones(shape, F32)
    for base in range(0, width, STRIDE):
        tall = [jnp.broadcast_to(work[:, width + base + i : width + base + i + 1], shape) for i in range(STRIDE)]
        wide = [jnp.broadcast_to(work[base + i : base + i + 1, :], shape) for i in range(STRIDE)]
        cell = {
            (m, i): jnp.broadcast_to(tall[i][base + m : base + m + 1, :], shape)
            for i in range(STRIDE)
            for m in range(i, STRIDE)
        }
        for i in range(STRIDE):
            inverse = 1.0 / cell[i, i]
            diagonal = jnp.where(row == base + i, cell[i, i], diagonal)
            scale = jnp.where(row > base + i, tall[i] * inverse, 0.0)
            work = work - scale * wide[i]
            for m in range(i + 1, STRIDE):
                ratio = cell[m, i] * inverse
                wide[m] = wide[m] - ratio * wide[i]
                tall[m] = tall[m] - scale * cell[m, i]
                for n in range(m, STRIDE):
                    cell[n, m] = cell[n, m] - ratio * cell[n, i]
    work = work / jnp.sqrt(diagonal)
    upper = jnp.where((lane < 2 * width) & (lane >= row + width), work, 0.0)
    inverse = jnp.where(lane <= row, work, 0.0)
    return upper, inverse


def factor_of(upper):
    width = upper.shape[0]
    return upper[:, width : 2 * width].T


def flip(index, distance, size):
    total, bit = 0, 1
    while bit < size:
        total = total + bit * lax.rem(lax.div(index, bit) + lax.div(distance, bit), 2)
        bit *= 2
    return total


def kernel(
    grp_size, col_size, node_total,
    start_ref, tiles_ref, row_ref, col_ref, count_ref,
    basis_ref, proj_ref, factors_ref,
    raw, merged, high, low, high_t, low_t, rows_v, cols_v, table_v, table,
    u_ref, lr_ref, stack, lstack, row_panel, col_panel, row_split, col_split,
    acc_row, acc_col, got_row, got_col, deg_row, deg_col, deg_got_row, deg_got_col,
    degree_ref, sigma_ref, coeff_ref, red_col, red_grp, early, late,
    tile_sem, in_sem, gather_row_sem, gather_col_sem, scatter_row_sem, scatter_col_sem,
    deg_row_sem, deg_col_sem, red_col_sem, red_grp_sem, early_sem, late_sem,
):
    grp = lax.axis_index("grp")
    col = lax.axis_index("col")
    slots, tile_size = raw.shape[0], raw.shape[1]
    width = u_ref.shape[1]
    small = (width, LANES)
    row = lax.broadcasted_iota(I32, small, 0)
    lane = lax.broadcasted_iota(I32, small, 1)

    def other(t):
        dg, dc = lax.div(t, col_size), lax.rem(t, col_size)
        return flip(grp, dg, grp_size), flip(col, dc, col_size)

    loads_of = tile_sem.shape[0]
    share = slots // loads_of

    def load_tile(n):
        at = pl.ds(n * share, share)
        return pltpu.make_async_copy(tiles_ref.at[at], raw.at[at], tile_sem.at[n])

    loads = (
        pltpu.make_async_copy(start_ref, u_ref.at[0], in_sem.at[0]),
        pltpu.make_async_copy(row_ref, rows_v, in_sem.at[1]),
        pltpu.make_async_copy(col_ref, cols_v, in_sem.at[2]),
    )
    for copy in loads:
        copy.start()

    def start_load(s, carry):
        load_tile(s).start()
        return carry

    lax.fori_loop(0, loads_of, start_load, 0)

    barrier = pltpu.get_barrier_semaphore()

    def greet(t, carry):
        pl.semaphore_signal(barrier, inc=1, device_id=other(t), device_id_type=MESH)
        return carry

    everyone = grp_size * col_size
    lax.fori_loop(1, everyone, greet, 0, unroll=everyone <= 32)

    def copy_to(axis, d, source, target, sems):
        size = col_size if axis == "col" else grp_size
        peer = flip(col if axis == "col" else grp, d, size)
        return pltpu.make_async_remote_copy(
            src_ref=source(peer),
            dst_ref=target,
            send_sem=sems.at[0],
            recv_sem=sems.at[1],
            device_id=(grp, peer) if axis == "col" else (peer, col),
            device_id_type=MESH,
        )

    def send(axis, source, target, sems):
        size = col_size if axis == "col" else grp_size

        def visit(d, carry):
            copy_to(axis, size - d, source, target, sems).start()
            return carry

        lax.fori_loop(1, size, visit, 0, unroll=size <= 8)

    def await_all(buf, sems):
        part = buf.at[pl.ds(0, buf.shape[0] - 1)]
        pltpu.make_async_remote_copy(
            src_ref=part, dst_ref=part, send_sem=sems.at[0], recv_sem=sems.at[1],
            device_id=other(1), device_id_type=MESH,
        ).wait()

    def gather_col(par, start):
        if start:
            send("grp", lambda peer: u_ref.at[par], col_panel.at[par, grp], gather_col_sem.at[par])
        else:
            await_all(col_panel.at[par], gather_col_sem.at[par])

    def gather_row(par, start):
        if start:
            send("col", lambda peer: u_ref.at[par], row_panel.at[par, col], gather_row_sem.at[par])
        else:
            await_all(row_panel.at[par], gather_row_sem.at[par])

    def spread(axis, buf, sems, start):
        me = col if axis == "col" else grp
        if start:
            send(axis, lambda peer: buf.at[me], buf.at[me], sems)
        else:
            await_all(buf, sems)

    def spread_all(buf, sems):
        me = grp * col_size + col

        def visit(t, carry):
            pltpu.make_async_remote_copy(
                src_ref=buf.at[me], dst_ref=buf.at[me], send_sem=sems.at[0], recv_sem=sems.at[1],
                device_id=other(everyone - t), device_id_type=MESH,
            ).start()
            return carry

        lax.fori_loop(1, everyone, visit, 0, unroll=everyone <= 32)

    def position(r, q):
        return table[0, r * grp_size + q]

    def send_rows(par, r, d, with_degree):
        copy_to("col", d, lambda peer: acc_row.at[r], got_row.at[par, col], scatter_row_sem.at[par]).start()
        if with_degree:
            copy_to("col", d, lambda peer: deg_row.at[r], deg_got_row.at[col], deg_row_sem).start()

    def halves(panel, par, size, split, with_degree):
        for place in range(size):
            first, second = split_two(panel[par, place])
            at = pl.ds(place * tile_size, tile_size)
            split[:width, at] = first
            if with_degree:
                split[width : 2 * width, at] = jnp.ones((width, tile_size), BF16)
                split[2 * width :, at] = second
            else:
                split[width : 2 * width, at] = second

    def combine(total, rest, with_degree):
        if not with_degree:
            return total[:width] + total[width:] + rest, None
        piece = total[:width] + total[2 * width :] + rest[:width]
        return piece, total[width : width + 1] + rest[width : width + 1]

    def rows_of(r, with_degree):
        places = [position(r, q) for q in range(grp_size)]
        if with_degree:
            left = col_split[...]
            firsts = jnp.concatenate([high[p] for p in places], axis=1)
            seconds = jnp.concatenate([low[p] for p in places], axis=1)
            return combine(dot_nt(left, firsts), dot_nt(left[: 2 * width], seconds), True)
        left = col_split[: 2 * width]
        firsts = jnp.concatenate([high_t[p] for p in places], axis=0)
        seconds = jnp.concatenate([low_t[p] for p in places], axis=0)
        return combine(dot_nn(left, firsts), dot_nn(left[:width], seconds), False)

    def cols_of(q, with_degree):
        piece, degree = 0.0, 0.0
        chunk = CHUNK if col_size % CHUNK == 0 else 1
        for base in range(0, col_size, chunk):
            at = pl.ds(base * tile_size, chunk * tile_size)
            left = row_split[:, at] if with_degree else row_split[: 2 * width, at]
            places = [position(base + r, q) for r in range(chunk)]
            firsts = jnp.concatenate([high[p] for p in places], axis=0)
            seconds = jnp.concatenate([low[p] for p in places], axis=0)
            rest = dot_nn(left[: 2 * width] if with_degree else left[:width], seconds)
            part, extra = combine(dot_nn(left, firsts), rest, with_degree)
            piece = piece + part
            if with_degree:
                degree = degree + extra
        return piece, degree

    def all_rows(par, with_degree):
        def visit(d, carry):
            r = flip(col, d, col_size)
            piece, degree = rows_of(r, with_degree)
            acc_row[r] = piece
            if with_degree:
                deg_row[r] = degree
            return carry

        if col_size <= 8:
            order = list(range(col_size - 1, -1, -1))
            for base in range(0, col_size, 4):
                for d in order[base : base + 4]:
                    visit(d, 0)
                for d in order[base : base + 4]:
                    if d:
                        send_rows(par, flip(col, d, col_size), d, with_degree)
        else:
            def go(d, carry):
                visit(d, 0)
                send_rows(par, flip(col, d, col_size), d, with_degree)
                return carry

            lax.fori_loop(1, col_size, go, 0)
            visit(0, 0)
        got_row[par, col] = acc_row[col]
        if with_degree:
            deg_got_row[col] = deg_row[col]

    def all_cols(par, with_degree):
        for d in range(grp_size - 1, -1, -1):
            q = flip(grp, d, grp_size)
            piece, degree = cols_of(q, with_degree)
            acc_col[q] = piece
            if with_degree:
                deg_col[q] = degree
        send("grp", lambda peer: acc_col.at[peer], got_col.at[par, grp], scatter_col_sem.at[par])
        got_col[par, grp] = acc_col[grp]
        if with_degree:
            send("grp", lambda peer: deg_col.at[peer], deg_got_col.at[grp], deg_col_sem)
            deg_got_col[grp] = deg_col[grp]

    def collect(par, with_degree):
        await_all(got_row.at[par], scatter_row_sem.at[par])
        await_all(got_col.at[par], scatter_col_sem.at[par])
        if with_degree:
            await_all(deg_got_row, deg_row_sem)
            await_all(deg_got_col, deg_col_sem)
            degree_ref[...] = jnp.sum(deg_got_row[...], axis=0) + jnp.sum(deg_got_col[...], axis=0)
        total = jnp.sum(got_row[par], axis=0) + jnp.sum(got_col[par], axis=0)
        return degree_ref[...] * u_ref[par] - total

    loads[0].wait()
    stack[...] = jnp.zeros_like(stack)
    lstack[...] = jnp.zeros_like(lstack)
    start = u_ref[0]
    stack[0] = start
    stack[1] = start
    row_panel[0, col] = start
    col_panel[0, grp] = start
    pl.semaphore_wait(barrier, everyone - 1)
    gather_col(0, True)
    gather_row(0, True)

    loads[1].wait()
    loads[2].wait()
    spots = table.shape[1]
    offset = rows_v[...] - grp * col_size
    pick = lax.div(cols_v[...] - col, col_size)
    place = jnp.clip(offset, 0, col_size - 1) * grp_size + jnp.clip(pick, 0, grp_size - 1)
    square = (slots, slots)
    down = lax.broadcasted_iota(I32, square, 0)
    across = lax.broadcasted_iota(I32, square, 1)
    wide = jnp.broadcast_to(place, square)
    tall = jnp.sum(jnp.where(down == across, wide, 0), axis=1, keepdims=True)
    same = (wide == jnp.broadcast_to(tall, square)) & (down < across)
    before = jnp.max(jnp.where(same, down, -1), axis=0, keepdims=True)
    before = jnp.where(before < 0, slots, before)
    long = (slots, spots)
    depth = lax.broadcasted_iota(I32, long, 0)
    spot = lax.broadcasted_iota(I32, long, 1)
    here = (jnp.broadcast_to(tall, long) == spot) & (depth < count_ref[0])
    last = jnp.max(jnp.where(here, depth, -1), axis=0, keepdims=True)
    table_v[0:1, :] = jnp.where(last < 0, slots, last)
    table_v[1:2, :slots] = before
    move = pltpu.make_async_copy(table_v, table, in_sem.at[3])
    move.start()
    empty = jnp.zeros((tile_size, tile_size), F32)
    merged[slots] = empty
    high[slots] = empty.astype(BF16)
    low[slots] = empty.astype(BF16)
    high_t[slots] = empty.astype(BF16)
    low_t[slots] = empty.astype(BF16)
    move.wait()

    def merge(n, carry):
        load_tile(n).wait()
        for m in range(share):
            s = n * share + m
            value = raw[s] + merged[table[1, s]]
            merged[s] = value
            first, second = split_two(value)
            high[s] = first
            low[s] = second
        return carry

    lax.fori_loop(0, loads_of, merge, 0)

    gather_col(0, False)
    halves(col_panel, 0, grp_size, col_split, True)
    all_rows(0, True)
    gather_row(0, False)
    halves(row_panel, 0, col_size, row_split, True)
    all_cols(0, True)

    def turn(s, carry):
        high_t[s] = high[s].T
        low_t[s] = low[s].T
        return carry

    lax.fori_loop(0, slots, turn, 0, unroll=4)
    applied = collect(0, True)
    lr_ref[...] = applied
    u_ref[1] = applied
    sigma_ref[...] = jnp.zeros_like(sigma_ref)

    half = width // 2

    def fold(value):
        return jnp.where(lane[:half] < LANES // 2, value[:half], value[half:])

    def unfold(packed):
        turned = pltpu.roll(packed, LANES // 2, 1)
        low_lanes = lane[:half] < LANES // 2
        return jnp.concatenate(
            [jnp.where(low_lanes, packed, turned), jnp.where(low_lanes, turned, packed)], axis=0
        )

    def settle(total, inverse):
        left = inverse[:, :width]
        fresh = dot_nn(left, jnp.concatenate([stack[1], lr_ref[...]], axis=1), HIGHEST)
        newest, image = fresh[:, :tile_size], fresh[:, tile_size:]
        pad = jnp.concatenate([inverse, jnp.zeros((LANES - width, LANES), F32)], axis=0)
        mixed = dot_nt(total[:, :width], pad[:, :width], HIGHEST)
        coeffs = jnp.where(lane < width, mixed, jnp.where((lane >= 2 * width) & (lane < 5 * width), total, 0.0))
        stack[0] = newest
        lstack[0] = image
        return left, newest, image, coeffs

    def step(k, carry):
        par = lax.rem(k + 1, 2)
        row_panel[par, col] = u_ref[par]
        col_panel[par, grp] = u_ref[par]
        gather_col(par, True)
        gather_row(par, True)
        block = stack[0:4].reshape(4 * width, tile_size)
        block = jnp.concatenate([block, block], axis=0)
        both = dot_nt(jnp.concatenate([u_ref[par], stack[1]], axis=0), block, HIGHEST)
        gram_lanes = (lax.rem(lane, 4 * width) >= width) & (lax.rem(lane, 4 * width) < 2 * width)
        part = jnp.where(gram_lanes, both[width:], both[:width])
        red_col[par, col] = fold(part)
        spread("col", red_col.at[par], red_col_sem.at[par], True)

        gather_col(par, False)
        halves(col_panel, par, grp_size, col_split, False)
        all_rows(par, False)

        spread("col", red_col.at[par], red_col_sem.at[par], False)
        red_grp[par, grp] = jnp.sum(red_col[par], axis=0)
        spread("grp", red_grp.at[par], red_grp_sem.at[par], True)

        gather_row(par, False)
        halves(row_panel, par, col_size, row_split, False)
        all_cols(par, False)

        spread("grp", red_grp.at[par], red_grp_sem.at[par], False)
        total = jnp.where(lane < LANES // 2, unfold(jnp.sum(red_grp[par], axis=0) / node_total), 0.0)
        upper, inverse = factorize(total)
        left, newest, image, coeffs = settle(total, inverse)
        factors_ref[k] = factor_of(upper)
        basis_ref[k] = newest
        now = dot_nn(coeffs, jnp.concatenate([stack[...].reshape(LANES, tile_size),
                                              lstack[...].reshape(LANES, tile_size)], axis=1), HIGHEST)
        residual = dot_nn(left, u_ref[par] - now[:, :tile_size], HIGHEST)
        known = now[:, tile_size:]
        found = dot_nn(left, coeffs, HIGHEST)
        found = found + jnp.where(lane == row, sigma_ref[:, :LANES], 0.0)
        coeff_ref[k] = found
        mean = jnp.sum(jnp.where(lane == row, found, 0.0), axis=1, keepdims=True)
        mean = jnp.sum(mean, axis=0, keepdims=True) / width
        sigma = jnp.where(k == 0, jnp.broadcast_to(mean, sigma_ref.shape), sigma_ref[...])
        stack[k + 2] = newest
        lstack[k + 2] = image
        stack[0] = residual
        stack[1] = residual

        @pl.when(k == ITERS - 2)
        def _():
            shifted = [lstack[j] - sigma * stack[j] for j in (4, 2, 3)]
            block = jnp.concatenate([shifted[0], residual, shifted[1], shifted[2]] * 2, axis=0)
            early[grp * col_size + col] = fold(dot_nt(residual, block, HIGHEST))
            spread_all(early, early_sem)

        applied = collect(par, False)
        image_next = dot_nn(left, applied - known, HIGHEST)
        lr_ref[...] = image_next
        u_ref[1 - par] = image_next - sigma * residual
        sigma_ref[...] = sigma
        return carry

    lax.fori_loop(0, ITERS - 1, step, 0)

    k = ITERS - 1
    par = ITERS % 2
    quarter = width // 4
    block_u, block_r = u_ref[par], stack[1]
    both = dot_nt(block_u, jnp.concatenate([block_r, block_u] * (LANES // (2 * width)), axis=0), HIGHEST)
    both = fold(both)
    odd = lax.rem(lax.div(lane[:quarter], 2 * width), 2) == 1
    late[grp * col_size + col] = jnp.where(odd, both[quarter:], both[:quarter])
    spread_all(late, late_sem)
    await_all(early, early_sem)
    total = unfold(jnp.sum(early[...], axis=0) / node_total)
    upper, inverse = factorize(total)
    left = inverse[:, :width]
    newest = dot_nn(left, block_r, HIGHEST)
    stack[0] = newest
    basis_ref[k] = newest
    factors_ref[k] = factor_of(upper)
    older = jnp.where((lane >= 2 * width) & (lane < 5 * width), total, 0.0)
    pad = jnp.concatenate([inverse, jnp.zeros((LANES - width, LANES), F32)], axis=0)[:, :width]
    proj_ref[...] = jnp.zeros_like(proj_ref)

    def keep_coeffs(k):
        for j in range(k):
            proj_ref[k, j] = coeff_ref[k, :, (j + 2) * width : (j + 3) * width]
        proj_ref[k, k] = coeff_ref[k, :, :width]

    for n in range(ITERS - 1):
        keep_coeffs(n)
    await_all(late, late_sem)
    packed = jnp.sum(late[...], axis=0) / node_total
    total = jnp.concatenate(
        [packed] + [pltpu.roll(packed, LANES - n * 2 * width, 1) for n in range(1, 4)], axis=0
    )
    coeffs = dot_nt(total[:, :width], pad, HIGHEST) + older
    middle = jnp.zeros((width, LANES), F32)
    beside = jnp.concatenate([middle, coeffs] + [middle] * (LANES // width - 2), axis=0)
    gram = total - dot_nt(coeffs, beside, HIGHEST)
    rest = block_u - dot_nn(coeffs, stack[...].reshape(LANES, tile_size), HIGHEST)
    upper, inverse = factorize(gram)
    basis_ref[ITERS] = dot_nn(inverse[:, :width], rest, HIGHEST)
    factors_ref[ITERS] = dot_nt(left, upper[:, width : 2 * width], HIGHEST)
    coeff_ref[k] = dot_nn(left, coeffs, HIGHEST) + jnp.where(lane == row, sigma_ref[:, :LANES], 0.0)
    keep_coeffs(k)


def deliver(basis, proj, factors, basis_out, proj_out, factors_out, sem):
    pairs = ((basis, basis_out), (proj, proj_out), (factors, factors_out))
    copies = [pltpu.make_async_copy(source, target, sem.at[n]) for n, (source, target) in enumerate(pairs)]
    for copy in copies:
        copy.start()
    for copy in copies:
        copy.wait()


def solution(mesh):
    grp_size, col_size = mesh.shape["grp"], mesh.shape["col"]

    def body(start_block, tile_values, tile_row, tile_col, tile_count):
        width, shard_len = start_block.shape
        slots, tile_size = tile_values.shape[2], tile_values.shape[3]
        assert shard_len == tile_size and LANES // width == 8
        assert grp_size & (grp_size - 1) == 0 and col_size & (col_size - 1) == 0
        places = LANES // width
        node_total = shard_len * grp_size * col_size
        spots = -(-max(grp_size * col_size, slots) // LANES) * LANES
        vmem = pl.BlockSpec(memory_space=pltpu.VMEM)
        smem = pl.BlockSpec(memory_space=pltpu.SMEM)
        hbm = pl.BlockSpec(memory_space=pl.ANY)
        block = (width, tile_size)
        line = (1, tile_size)
        tiles = (slots + 1, tile_size, tile_size)
        packed = (width // 2, LANES)
        small = (width, LANES)

        def sems(*sizes):
            return pltpu.SemaphoreType.DMA(sizes)

        def pinned(value):
            return pltpu.with_memory_space_constraint(value, pltpu.HBM)

        shapes = (
            jax.ShapeDtypeStruct((ITERS + 1,) + block, F32),
            jax.ShapeDtypeStruct((ITERS, ITERS, width, width), F32),
            jax.ShapeDtypeStruct((ITERS + 1, width, width), F32),
        )
        results = pl.pallas_call(
            functools.partial(kernel, grp_size, col_size, node_total),
            out_shape=shapes,
            in_specs=[hbm, hbm, hbm, hbm, smem],
            out_specs=(vmem, vmem, vmem),
            scratch_shapes=[
                pltpu.VMEM((slots, tile_size, tile_size), F32),
                pltpu.VMEM(tiles, F32),
                pltpu.VMEM(tiles, BF16),
                pltpu.VMEM(tiles, BF16),
                pltpu.VMEM(tiles, BF16),
                pltpu.VMEM(tiles, BF16),
                pltpu.VMEM((1, slots), I32),
                pltpu.VMEM((1, slots), I32),
                pltpu.VMEM((8, spots), I32),
                pltpu.SMEM((8, spots), I32),
                pltpu.VMEM((2,) + block, F32),
                pltpu.VMEM(block, F32),
                pltpu.VMEM((places,) + block, F32),
                pltpu.VMEM((places,) + block, F32),
                pltpu.VMEM((2, col_size) + block, F32),
                pltpu.VMEM((2, grp_size) + block, F32),
                pltpu.VMEM((3 * width, col_size * tile_size), BF16),
                pltpu.VMEM((3 * width, grp_size * tile_size), BF16),
                pltpu.VMEM((col_size,) + block, F32),
                pltpu.VMEM((grp_size,) + block, F32),
                pltpu.VMEM((2, col_size) + block, F32),
                pltpu.VMEM((2, grp_size) + block, F32),
                pltpu.VMEM((col_size,) + line, F32),
                pltpu.VMEM((grp_size,) + line, F32),
                pltpu.VMEM((col_size,) + line, F32),
                pltpu.VMEM((grp_size,) + line, F32),
                pltpu.VMEM(line, F32),
                pltpu.VMEM(block, F32),
                pltpu.VMEM((ITERS,) + small, F32),
                pltpu.VMEM((2, col_size) + packed, F32),
                pltpu.VMEM((2, grp_size) + packed, F32),
                pltpu.VMEM((grp_size * col_size,) + packed, F32),
                pltpu.VMEM((grp_size * col_size, width // 4, LANES), F32),
                sems(8 if slots % 8 == 0 else slots),
                sems(4),
                sems(2, 2), sems(2, 2), sems(2, 2), sems(2, 2),
                sems(2), sems(2), sems(2, 2), sems(2, 2), sems(2), sems(2),
            ],
            compiler_params=pltpu.CompilerParams(
                collective_id=0, has_side_effects=True, vmem_limit_bytes=40 * 1024 * 1024
            ),
        )(
            pinned(start_block),
            pinned(tile_values.reshape(slots, tile_size, tile_size)),
            pinned(tile_row.reshape(1, slots)),
            pinned(tile_col.reshape(1, slots)),
            tile_count.reshape(1),
        )
        return pl.pallas_call(
            deliver,
            out_shape=shapes,
            in_specs=[vmem] * 3,
            out_specs=[hbm] * 3,
            scratch_shapes=[sems(3)],
        )(*(pltpu.with_memory_space_constraint(value, pltpu.VMEM) for value in results))

    in_specs = (
        P(None, ("grp", "col")),
        P("grp", "col", None, None, None),
        P("grp", "col", None),
        P("grp", "col", None),
        P("grp", "col"),
    )
    out_specs = (P(None, None, ("grp", "col")), P(), P())
    return jax.shard_map(body, mesh=mesh, in_specs=in_specs, out_specs=out_specs, check_vma=False)
```

```python
import functools

import jax
import jax.numpy as jnp
from jax import lax
from jax.experimental import pallas as pl
from jax.experimental.pallas import tpu as pltpu
from jax.sharding import PartitionSpec as P

ITERS = 4
HIGHEST = lax.Precision.HIGHEST
MESH = pl.DeviceIdType.MESH
F32 = jnp.float32
BF16 = jnp.bfloat16
I32 = jnp.int32
LANES = 128
CHUNK = 8
STRIDE = 4


def dot_nt(left, right, precision=None):
    dims = (((1,), (1,)), ((), ()))
    return lax.dot_general(left, right, dims, precision=precision, preferred_element_type=F32)


def dot_nn(left, right, precision=None):
    dims = (((1,), (0,)), ((), ()))
    return lax.dot_general(left, right, dims, precision=precision, preferred_element_type=F32)


def split_two(value):
    high = value.astype(BF16)
    low = (value - high.astype(F32)).astype(BF16)
    return high, low


def factorize(gram):
    width = gram.shape[0]
    shape = gram.shape
    row = lax.broadcasted_iota(I32, shape, 0)
    lane = lax.broadcasted_iota(I32, shape, 1)
    unit = jnp.where(lane == row, 1.0, 0.0).astype(F32)
    work = jnp.where((lane >= width) & (lane < 2 * width), gram, unit)
    diagonal = jnp.ones(shape, F32)
    for base in range(0, width, STRIDE):
        tall = [jnp.broadcast_to(work[:, width + base + i : width + base + i + 1], shape) for i in range(STRIDE)]
        wide = [jnp.broadcast_to(work[base + i : base + i + 1, :], shape) for i in range(STRIDE)]
        cell = {
            (m, i): jnp.broadcast_to(tall[i][base + m : base + m + 1, :], shape)
            for i in range(STRIDE)
            for m in range(i, STRIDE)
        }
        for i in range(STRIDE):
            inverse = 1.0 / cell[i, i]
            diagonal = jnp.where(row == base + i, cell[i, i], diagonal)
            scale = jnp.where(row > base + i, tall[i] * inverse, 0.0)
            work = work - scale * wide[i]
            for m in range(i + 1, STRIDE):
                ratio = cell[m, i] * inverse
                wide[m] = wide[m] - ratio * wide[i]
                tall[m] = tall[m] - scale * cell[m, i]
                for n in range(m, STRIDE):
                    cell[n, m] = cell[n, m] - ratio * cell[n, i]
    work = work / jnp.sqrt(diagonal)
    upper = jnp.where((lane < 2 * width) & (lane >= row + width), work, 0.0)
    inverse = jnp.where(lane <= row, work, 0.0)
    return upper, inverse


def factor_of(upper):
    width = upper.shape[0]
    return upper[:, width : 2 * width].T


def flip(index, distance, size):
    total, bit = 0, 1
    while bit < size:
        total = total + bit * lax.rem(lax.div(index, bit) + lax.div(distance, bit), 2)
        bit *= 2
    return total


def kernel(
    grp_size, col_size, node_total,
    start_ref, tiles_ref, row_ref, col_ref, count_ref,
    basis_ref, proj_ref, factors_ref,
    raw, merged, high, low, high_t, low_t, rows_v, cols_v, table_v, table,
    u_ref, v_ref, lr_ref, stack, lstack, row_panel, col_panel, row_split, col_split,
    acc_row, acc_col, got_row, got_col, deg_row, deg_col, deg_got_row, deg_got_col,
    degree_ref, sigma_ref, shift_ref, left_ref, upper_ref, coeff_ref, red_col, red_grp, early, late,
    tile_sem, in_sem, gather_row_sem, gather_col_sem, scatter_row_sem, scatter_col_sem,
    deg_row_sem, deg_col_sem, red_col_sem, red_grp_sem, early_sem, late_sem,
):
    grp = lax.axis_index("grp")
    col = lax.axis_index("col")
    slots, tile_size = raw.shape[0], raw.shape[1]
    width = u_ref.shape[1]
    small = (width, LANES)
    row = lax.broadcasted_iota(I32, small, 0)
    lane = lax.broadcasted_iota(I32, small, 1)

    def other(t):
        dg, dc = lax.div(t, col_size), lax.rem(t, col_size)
        return flip(grp, dg, grp_size), flip(col, dc, col_size)

    loads_of = tile_sem.shape[0]
    share = slots // loads_of

    def load_tile(n):
        at = pl.ds(n * share, share)
        return pltpu.make_async_copy(tiles_ref.at[at], raw.at[at], tile_sem.at[n])

    loads = (
        pltpu.make_async_copy(start_ref, u_ref.at[0], in_sem.at[0]),
        pltpu.make_async_copy(row_ref, rows_v, in_sem.at[1]),
        pltpu.make_async_copy(col_ref, cols_v, in_sem.at[2]),
    )
    for copy in loads:
        copy.start()

    def start_load(s, carry):
        load_tile(s).start()
        return carry

    lax.fori_loop(0, loads_of, start_load, 0)

    barrier = pltpu.get_barrier_semaphore()

    def greet(t, carry):
        pl.semaphore_signal(barrier, inc=1, device_id=other(t), device_id_type=MESH)
        return carry

    everyone = grp_size * col_size
    lax.fori_loop(1, everyone, greet, 0, unroll=everyone <= 32)

    def copy_to(axis, d, source, target, send_sem, recv_sem):
        size = col_size if axis == "col" else grp_size
        peer = flip(col if axis == "col" else grp, d, size)
        return pltpu.make_async_remote_copy(
            src_ref=source(peer),
            dst_ref=target,
            send_sem=send_sem,
            recv_sem=recv_sem,
            device_id=(grp, peer) if axis == "col" else (peer, col),
            device_id_type=MESH,
        )

    def send(axis, source, target, sems):
        size = col_size if axis == "col" else grp_size

        def visit(d, carry):
            copy_to(axis, size - d, source, target, sems.at[0], sems.at[1]).start()
            return carry

        lax.fori_loop(1, size, visit, 0, unroll=size <= 8)

    def bytes_of(part, send_sem, recv_sem):
        return pltpu.make_async_remote_copy(
            src_ref=part, dst_ref=part, send_sem=send_sem, recv_sem=recv_sem,
            device_id=other(1), device_id_type=MESH,
        )

    def await_all(buf, sems):
        bytes_of(buf.at[pl.ds(0, buf.shape[0] - 1)], sems.at[0], sems.at[1]).wait()

    col_groups = ((1, grp_size - 1), (grp_size - 1, grp_size))
    row_groups = ((1, 2), (2, 4), (4, col_size))

    def gather(axis, par, panel, sems, groups):
        me = col if axis == "col" else grp
        for n, (low_d, high_d) in reversed(list(enumerate(groups))):

            def visit(i, carry):
                d = high_d - 1 - i
                target = panel.at[par, me]
                copy_to(axis, d, lambda peer: u_ref.at[par], target, sems.at[par, 0], sems.at[par, n + 1]).start()
                return carry

            lax.fori_loop(0, high_d - low_d, visit, 0, unroll=high_d - low_d <= 8)

    def arrive(par, panel, sems, groups, n):
        count = groups[n][1] - groups[n][0]
        bytes_of(panel.at[par, pl.ds(0, count)], sems.at[par, 0], sems.at[par, n + 1]).wait_recv()

    def leave(par, panel, sems):
        count = panel.shape[1] - 1
        bytes_of(panel.at[par, pl.ds(0, count)], sems.at[par, 0], sems.at[par, 1]).wait_send()

    col_side = (col_panel, gather_col_sem, col_groups)
    row_side = (row_panel, gather_row_sem, row_groups)

    def spread(axis, buf, sems, start):
        me = col if axis == "col" else grp
        if start:
            send(axis, lambda peer: buf.at[me], buf.at[me], sems)
        else:
            await_all(buf, sems)

    def spread_all(buf, sems):
        me = grp * col_size + col

        def visit(t, carry):
            pltpu.make_async_remote_copy(
                src_ref=buf.at[me], dst_ref=buf.at[me], send_sem=sems.at[0], recv_sem=sems.at[1],
                device_id=other(everyone - t), device_id_type=MESH,
            ).start()
            return carry

        lax.fori_loop(1, everyone, visit, 0, unroll=everyone <= 32)

    def position(r, q):
        return table[0, r * grp_size + q]

    def send_rows(par, r, d, with_degree):
        sems = scatter_row_sem.at[par]
        copy_to("col", d, lambda peer: acc_row.at[r], got_row.at[par, col], sems.at[0], sems.at[1]).start()
        if with_degree:
            sems = deg_row_sem
            copy_to("col", d, lambda peer: deg_row.at[r], deg_got_row.at[col], sems.at[0], sems.at[1]).start()

    def halves(panel, par, size, split):
        for place in range(size):
            first, second = split_two(panel[par, place])
            at = pl.ds(place * tile_size, tile_size)
            split[:width, at] = first
            split[width : 2 * width, at] = jnp.ones((width, tile_size), BF16)
            split[2 * width :, at] = second

    def combine(total, rest):
        piece = total[:width] + total[2 * width :] + rest[:width]
        return piece, total[width : width + 1] + rest[width : width + 1]

    def rows_of(r):
        places = [position(r, q) for q in range(grp_size)]
        left = col_split[...]
        firsts = jnp.concatenate([high[p] for p in places], axis=1)
        seconds = jnp.concatenate([low[p] for p in places], axis=1)
        return combine(dot_nt(left, firsts), dot_nt(left[: 2 * width], seconds))

    def cols_of(q):
        piece, degree = 0.0, 0.0
        for base in range(0, col_size, CHUNK):
            left = row_split[:, pl.ds(base * tile_size, CHUNK * tile_size)]
            places = [position(base + r, q) for r in range(CHUNK)]
            firsts = jnp.concatenate([high[p] for p in places], axis=0)
            seconds = jnp.concatenate([low[p] for p in places], axis=0)
            part, extra = combine(dot_nn(left, firsts), dot_nn(left[: 2 * width], seconds))
            piece = piece + part
            degree = degree + extra
        return piece, degree

    def first_rows():
        def visit(d):
            r = flip(col, d, col_size)
            piece, degree = rows_of(r)
            acc_row[r] = piece
            deg_row[r] = degree

        def go(base, count):
            for i in range(count):
                visit(base + i)
            for i in range(count):
                send_rows(0, flip(col, base + i, col_size), base + i, True)

        if col_size <= 8:
            go(col_size // 2, col_size // 2)
            go(1, col_size // 2 - 1)
        else:
            def each(d, carry):
                go(d, 1)
                return carry

            lax.fori_loop(1, col_size, each, 0)
        visit(0)
        got_row[0, col] = acc_row[col]
        deg_got_row[col] = deg_row[col]

    def first_cols():
        for d in range(grp_size - 1, -1, -1):
            q = flip(grp, d, grp_size)
            piece, degree = cols_of(q)
            acc_col[q] = piece
            deg_col[q] = degree
        send("grp", lambda peer: acc_col.at[peer], got_col.at[0, grp], scatter_col_sem.at[0])
        got_col[0, grp] = acc_col[grp]
        send("grp", lambda peer: deg_col.at[peer], deg_got_col.at[grp], deg_col_sem)
        deg_got_col[grp] = deg_col[grp]

    def stacked(pieces):
        pairs = [split_two(piece) for piece in pieces]
        return jnp.concatenate([jnp.concatenate(pair, axis=0) for pair in pairs], axis=1)

    def product(left, firsts, seconds):
        total = dot_nn(left, jnp.concatenate(firsts, axis=0))
        rest = dot_nn(left[:width], jnp.concatenate(seconds, axis=0))
        return total[:width] + total[width:] + rest

    def rows_batch(par, ds):
        places = [flip(grp, d, grp_size) for d in ds]
        left = stacked([u_ref[par] if d == 0 else col_panel[par, q] for d, q in zip(ds, places)])

        def visit(r, carry):
            at = [position(r, q) for q in places]
            piece = product(left, [high_t[p] for p in at], [low_t[p] for p in at])
            acc_row[r] = piece if ds[0] == 0 else acc_row[r] + piece
            return carry

        if col_size <= 8:
            for r in range(col_size):
                visit(r, 0)
        else:
            lax.fori_loop(0, col_size, visit, 0)

    def cols_batch(par, base, count):
        places = [flip(col, base + i, col_size) for i in range(count)]
        own = isinstance(base, int) and base == 0
        left = stacked([u_ref[par]] if own else [row_panel[par, r] for r in places])
        for q in range(grp_size):
            at = [position(r, q) for r in places]
            piece = product(left, [high[p] for p in at], [low[p] for p in at])
            acc_col[q] = piece if own else acc_col[q] + piece

    def collect(par, with_degree):
        leave(par, col_panel, gather_col_sem)
        leave(par, row_panel, gather_row_sem)
        await_all(got_row.at[par], scatter_row_sem.at[par])
        await_all(got_col.at[par], scatter_col_sem.at[par])
        if with_degree:
            await_all(deg_got_row, deg_row_sem)
            await_all(deg_got_col, deg_col_sem)
            degree_ref[...] = jnp.sum(deg_got_row[...], axis=0) + jnp.sum(deg_got_col[...], axis=0)
        total = jnp.sum(got_row[par], axis=0) + jnp.sum(got_col[par], axis=0)
        return degree_ref[...] * u_ref[par] - total

    stack[...] = jnp.zeros_like(stack)
    lstack[...] = jnp.zeros_like(lstack)
    loads[1].wait()
    loads[2].wait()
    spots = table.shape[1]
    offset = rows_v[...] - grp * col_size
    pick = lax.div(cols_v[...] - col, col_size)
    place = jnp.clip(offset, 0, col_size - 1) * grp_size + jnp.clip(pick, 0, grp_size - 1)
    square = (slots, slots)
    down = lax.broadcasted_iota(I32, square, 0)
    across = lax.broadcasted_iota(I32, square, 1)
    wide = jnp.broadcast_to(place, square)
    tall = jnp.sum(jnp.where(down == across, wide, 0), axis=1, keepdims=True)
    same = (wide == jnp.broadcast_to(tall, square)) & (down < across)
    before = jnp.max(jnp.where(same, down, -1), axis=0, keepdims=True)
    before = jnp.where(before < 0, slots, before)
    long = (slots, spots)
    depth = lax.broadcasted_iota(I32, long, 0)
    spot = lax.broadcasted_iota(I32, long, 1)
    here = (jnp.broadcast_to(tall, long) == spot) & (depth < count_ref[0])
    last = jnp.max(jnp.where(here, depth, -1), axis=0, keepdims=True)
    table_v[0:1, :] = jnp.where(last < 0, slots, last)
    table_v[1:2, :slots] = before
    move = pltpu.make_async_copy(table_v, table, in_sem.at[3])
    move.start()
    empty = jnp.zeros((tile_size, tile_size), F32)
    merged[slots] = empty
    high[slots] = empty.astype(BF16)
    low[slots] = empty.astype(BF16)
    high_t[slots] = empty.astype(BF16)
    low_t[slots] = empty.astype(BF16)
    loads[0].wait()
    start = u_ref[0]
    stack[0] = start
    stack[1] = start
    row_panel[0, col] = start
    col_panel[0, grp] = start
    pl.semaphore_wait(barrier, everyone - 1)
    gather("grp", 0, *col_side)
    gather("col", 0, *row_side)
    move.wait()

    def merge(n, carry):
        load_tile(n).wait()

        def visit(m, carry):
            s = n * share + m
            value = raw[s] + merged[table[1, s]]
            merged[s] = value
            first, second = split_two(value)
            high[s] = first
            low[s] = second
            return carry

        return lax.fori_loop(0, share, visit, carry)

    lax.fori_loop(0, loads_of, merge, 0)

    for n in range(len(col_groups)):
        arrive(0, *col_side, n)
    halves(col_panel, 0, grp_size, col_split)
    first_rows()
    for n in range(len(row_groups)):
        arrive(0, *row_side, n)
    halves(row_panel, 0, col_size, row_split)
    first_cols()

    def turn(s, carry):
        high_t[s] = high[s].T
        low_t[s] = low[s].T
        return carry

    lax.fori_loop(0, slots, turn, 0, unroll=4)
    applied = collect(0, True)
    lr_ref[...] = applied
    v_ref[...] = applied
    u_ref[1] = applied
    sigma_ref[...] = jnp.zeros_like(sigma_ref)
    left_ref[ITERS] = jnp.where(lane == row, 1.0, 0.0)

    half = width // 2

    def fold(value):
        return jnp.where(lane[:half] < LANES // 2, value[:half], value[half:])

    def unfold(packed):
        turned = pltpu.roll(packed, LANES // 2, 1)
        low_lanes = lane[:half] < LANES // 2
        return jnp.concatenate(
            [jnp.where(low_lanes, packed, turned), jnp.where(low_lanes, turned, packed)], axis=0
        )

    def step(k, carry):
        par = lax.rem(k + 1, 2)
        block_u, block_r = u_ref[par], stack[1]
        gather("grp", par, *col_side)
        block = stack[0:4].reshape(4 * width, tile_size)
        block = jnp.concatenate([block, block], axis=0)
        both = dot_nt(jnp.concatenate([v_ref[...], block_r], axis=0), block, HIGHEST)
        inner = lax.rem(lane, 4 * width)
        red_grp[par, grp] = fold(jnp.where((inner >= width) & (inner < 2 * width), both[width:], both[:width]))
        spread("grp", red_grp.at[par], red_grp_sem.at[par], True)
        gather("col", par, *row_side)

        rows_batch(par, [0])
        cols_batch(par, 0, 1)
        arrive(par, *row_side, 0)
        cols_batch(par, 1, 1)
        arrive(par, *col_side, 0)
        rows_batch(par, list(range(1, grp_size - 1)))
        spread("grp", red_grp.at[par], red_grp_sem.at[par], False)
        red_col[par, col] = jnp.sum(red_grp[par], axis=0)
        spread("col", red_col.at[par], red_col_sem.at[par], True)
        arrive(par, *col_side, 1)
        rows_batch(par, [grp_size - 1])
        send("col", lambda peer: acc_row.at[peer], got_row.at[par, col], scatter_row_sem.at[par])
        got_row[par, col] = acc_row[col]
        arrive(par, *row_side, 1)
        cols_batch(par, 2, 2)
        arrive(par, *row_side, 2)
        if col_size <= 8:
            cols_batch(par, 4, col_size - 4)
        else:
            def visit(n, carry):
                cols_batch(par, 4 * n, 4)
                return carry

            lax.fori_loop(1, col_size // 4, visit, 0)
        send("grp", lambda peer: acc_col.at[peer], got_col.at[par, grp], scatter_col_sem.at[par])
        got_col[par, grp] = acc_col[grp]

        spread("col", red_col.at[par], red_col_sem.at[par], False)
        total = unfold(jnp.sum(red_col[par], axis=0) / node_total)
        former = left_ref[lax.rem(k + ITERS, ITERS + 1)]
        turned = dot_nn(former[:, :width], total, HIGHEST)
        upper, inverse = factorize(total)
        left = inverse[:, :width]
        fresh = dot_nn(left, jnp.concatenate([block_r, lr_ref[...]], axis=1), HIGHEST)
        newest, image = fresh[:, :tile_size], fresh[:, tile_size:]
        pad = jnp.concatenate([inverse, jnp.zeros((LANES - width, LANES), F32)], axis=0)
        mixed = dot_nt(turned[:, :width], pad[:, :width], HIGHEST)
        older = (lane >= 2 * width) & (lane < 4 * width)
        coeffs = jnp.where(lane < width, mixed, jnp.where(older, turned, 0.0))
        stack[0] = newest
        lstack[0] = image
        now = dot_nn(coeffs, jnp.concatenate([stack[...].reshape(LANES, tile_size),
                                              lstack[...].reshape(LANES, tile_size)], axis=1), HIGHEST)
        rest = block_u - now[:, :tile_size]
        residual = dot_nn(left, rest, HIGHEST)
        on_block = jnp.sum(jnp.where(lane == row, total, 0.0), axis=1, keepdims=True)
        on_gram = jnp.sum(jnp.where(lane == row + width, total, 0.0), axis=1, keepdims=True)
        mean = jnp.sum(on_block, axis=0, keepdims=True) / jnp.sum(on_gram, axis=0, keepdims=True)
        before = sigma_ref[...]
        sigma = jnp.where(k == 0, jnp.broadcast_to(mean, sigma_ref.shape), before)
        known = now[:, tile_size:] + sigma * rest
        stack[0] = residual
        stack[1] = residual
        stack[k + 2] = newest
        lstack[k + 2] = image

        @pl.when(k == ITERS - 2)
        def _():
            shifted = [lstack[j] - sigma * stack[j] for j in (4, 2, 3)]
            block = jnp.concatenate([shifted[0], residual, shifted[1], shifted[2]] * 2, axis=0)
            early[grp * col_size + col] = fold(dot_nt(residual, block, HIGHEST))
            spread_all(early, early_sem)

        basis_ref[k] = newest
        left_ref[k] = inverse
        upper_ref[k] = upper
        coeff_ref[k] = coeffs
        sigma_ref[...] = sigma
        shift_ref[k] = before[:, :LANES]

        applied = collect(par, False) - known
        fresh_u = dot_nn(left, applied, HIGHEST)
        v_ref[...] = applied
        u_ref[1 - par] = fresh_u
        lr_ref[...] = fresh_u + sigma * residual
        return carry

    lax.fori_loop(0, ITERS - 1, step, 0)

    k = ITERS - 1
    par = ITERS % 2
    quarter = width // 4
    block_u, block_r = u_ref[par], stack[1]
    both = dot_nt(block_u, jnp.concatenate([block_r, block_u] * (LANES // (2 * width)), axis=0), HIGHEST)
    both = fold(both)
    odd = lax.rem(lax.div(lane[:quarter], 2 * width), 2) == 1
    late[grp * col_size + col] = jnp.where(odd, both[quarter:], both[:quarter])
    spread_all(late, late_sem)
    await_all(early, early_sem)
    total = unfold(jnp.sum(early[...], axis=0) / node_total)
    upper, inverse = factorize(total)
    left = inverse[:, :width]
    newest = dot_nn(left, block_r, HIGHEST)
    stack[0] = newest
    basis_ref[k] = newest
    factors_ref[k] = factor_of(upper)
    older = jnp.where((lane >= 2 * width) & (lane < 5 * width), total, 0.0)
    pad = jnp.concatenate([inverse, jnp.zeros((LANES - width, LANES), F32)], axis=0)[:, :width]
    proj_ref[...] = jnp.zeros_like(proj_ref)

    def keep_coeffs(k, left, coeffs, shift):
        found = dot_nn(left, coeffs, HIGHEST) + jnp.where(lane == row, shift, 0.0)
        for j in range(k):
            proj_ref[k, j] = found[:, (j + 2) * width : (j + 3) * width]
        proj_ref[k, k] = found[:, :width]

    for n in range(ITERS - 1):
        keep_coeffs(n, left_ref[n, :, :width], coeff_ref[n], shift_ref[n])
        factors_ref[n] = factor_of(upper_ref[n])
    await_all(late, late_sem)
    packed = jnp.sum(late[...], axis=0) / node_total
    total = jnp.concatenate(
        [packed] + [pltpu.roll(packed, LANES - n * 2 * width, 1) for n in range(1, 4)], axis=0
    )
    coeffs = dot_nt(total[:, :width], pad, HIGHEST) + older
    middle = jnp.zeros((width, LANES), F32)
    beside = jnp.concatenate([middle, coeffs] + [middle] * (LANES // width - 2), axis=0)
    gram = total - dot_nt(coeffs, beside, HIGHEST)
    rest = block_u - dot_nn(coeffs, stack[...].reshape(LANES, tile_size), HIGHEST)
    upper, inverse = factorize(gram)
    basis_ref[ITERS] = dot_nn(inverse[:, :width], rest, HIGHEST)
    factors_ref[ITERS] = dot_nt(left, upper[:, width : 2 * width], HIGHEST)
    keep_coeffs(k, left, coeffs, sigma_ref[:, :LANES])


def deliver(basis, proj, factors, basis_out, proj_out, factors_out, sem):
    pairs = ((basis, basis_out), (proj, proj_out), (factors, factors_out))
    copies = [pltpu.make_async_copy(source, target, sem.at[n]) for n, (source, target) in enumerate(pairs)]
    for copy in copies:
        copy.start()
    for copy in copies:
        copy.wait()


def solution(mesh):
    grp_size, col_size = mesh.shape["grp"], mesh.shape["col"]

    def body(start_block, tile_values, tile_row, tile_col, tile_count):
        width, shard_len = start_block.shape
        slots, tile_size = tile_values.shape[2], tile_values.shape[3]
        assert shard_len == tile_size and LANES // width == 8
        assert grp_size > 2 and col_size % CHUNK == 0
        assert grp_size & (grp_size - 1) == 0 and col_size & (col_size - 1) == 0
        places = LANES // width
        node_total = shard_len * grp_size * col_size
        spots = -(-max(grp_size * col_size, slots) // LANES) * LANES
        vmem = pl.BlockSpec(memory_space=pltpu.VMEM)
        smem = pl.BlockSpec(memory_space=pltpu.SMEM)
        hbm = pl.BlockSpec(memory_space=pl.ANY)
        block = (width, tile_size)
        line = (1, tile_size)
        tiles = (slots + 1, tile_size, tile_size)
        packed = (width // 2, LANES)
        small = (width, LANES)

        def sems(*sizes):
            return pltpu.SemaphoreType.DMA(sizes)

        def pinned(value):
            return pltpu.with_memory_space_constraint(value, pltpu.HBM)

        shapes = (
            jax.ShapeDtypeStruct((ITERS + 1,) + block, F32),
            jax.ShapeDtypeStruct((ITERS, ITERS, width, width), F32),
            jax.ShapeDtypeStruct((ITERS + 1, width, width), F32),
        )
        results = pl.pallas_call(
            functools.partial(kernel, grp_size, col_size, node_total),
            out_shape=shapes,
            in_specs=[hbm, hbm, hbm, hbm, smem],
            out_specs=(vmem, vmem, vmem),
            scratch_shapes=[
                pltpu.VMEM((slots, tile_size, tile_size), F32),
                pltpu.VMEM(tiles, F32),
                pltpu.VMEM(tiles, BF16),
                pltpu.VMEM(tiles, BF16),
                pltpu.VMEM(tiles, BF16),
                pltpu.VMEM(tiles, BF16),
                pltpu.VMEM((1, slots), I32),
                pltpu.VMEM((1, slots), I32),
                pltpu.VMEM((8, spots), I32),
                pltpu.SMEM((8, spots), I32),
                pltpu.VMEM((2,) + block, F32),
                pltpu.VMEM(block, F32),
                pltpu.VMEM(block, F32),
                pltpu.VMEM((places,) + block, F32),
                pltpu.VMEM((places,) + block, F32),
                pltpu.VMEM((2, col_size) + block, F32),
                pltpu.VMEM((2, grp_size) + block, F32),
                pltpu.VMEM((3 * width, col_size * tile_size), BF16),
                pltpu.VMEM((3 * width, grp_size * tile_size), BF16),
                pltpu.VMEM((col_size,) + block, F32),
                pltpu.VMEM((grp_size,) + block, F32),
                pltpu.VMEM((2, col_size) + block, F32),
                pltpu.VMEM((2, grp_size) + block, F32),
                pltpu.VMEM((col_size,) + line, F32),
                pltpu.VMEM((grp_size,) + line, F32),
                pltpu.VMEM((col_size,) + line, F32),
                pltpu.VMEM((grp_size,) + line, F32),
                pltpu.VMEM(line, F32),
                pltpu.VMEM(block, F32),
                pltpu.VMEM((ITERS,) + small, F32),
                pltpu.VMEM((ITERS + 1,) + small, F32),
                pltpu.VMEM((ITERS,) + small, F32),
                pltpu.VMEM((ITERS,) + small, F32),
                pltpu.VMEM((2, col_size) + packed, F32),
                pltpu.VMEM((2, grp_size) + packed, F32),
                pltpu.VMEM((grp_size * col_size,) + packed, F32),
                pltpu.VMEM((grp_size * col_size, width // 4, LANES), F32),
                sems(8 if slots % 8 == 0 else slots),
                sems(4),
                sems(2, 4), sems(2, 3), sems(2, 2), sems(2, 2),
                sems(2), sems(2), sems(2, 2), sems(2, 2), sems(2), sems(2),
            ],
            compiler_params=pltpu.CompilerParams(
                collective_id=0, has_side_effects=True, vmem_limit_bytes=40 * 1024 * 1024
            ),
        )(
            pinned(start_block),
            pinned(tile_values.reshape(slots, tile_size, tile_size)),
            pinned(tile_row.reshape(1, slots)),
            pinned(tile_col.reshape(1, slots)),
            tile_count.reshape(1),
        )
        return pl.pallas_call(
            deliver,
            out_shape=shapes,
            in_specs=[vmem] * 3,
            out_specs=[hbm] * 3,
            scratch_shapes=[sems(3)],
        )(*(pltpu.with_memory_space_constraint(value, pltpu.VMEM) for value in results))

    in_specs = (
        P(None, ("grp", "col")),
        P("grp", "col", None, None, None),
        P("grp", "col", None),
        P("grp", "col", None),
        P("grp", "col"),
    )
    out_specs = (P(None, None, ("grp", "col")), P(), P())
    return jax.shard_map(body, mesh=mesh, in_specs=in_specs, out_specs=out_specs, check_vma=False)
```

```python
import functools

import jax
import jax.numpy as jnp
from jax import lax
from jax.experimental import pallas as pl
from jax.experimental.pallas import tpu as pltpu
from jax.sharding import PartitionSpec as P

ITERS = 4
HIGHEST = lax.Precision.HIGHEST
MESH = pl.DeviceIdType.MESH
F32 = jnp.float32
BF16 = jnp.bfloat16
I32 = jnp.int32
LANES = 128
CHUNK = 8
STRIDE = 8


def dot_nt(left, right, precision=None):
    dims = (((1,), (1,)), ((), ()))
    return lax.dot_general(left, right, dims, precision=precision, preferred_element_type=F32)


def dot_nn(left, right, precision=None):
    dims = (((1,), (0,)), ((), ()))
    return lax.dot_general(left, right, dims, precision=precision, preferred_element_type=F32)


def split_two(value):
    high = value.astype(BF16)
    low = (value - high.astype(F32)).astype(BF16)
    return high, low


def factorize(gram):
    width = gram.shape[0]
    shape = gram.shape
    row = lax.broadcasted_iota(I32, shape, 0)
    lane = lax.broadcasted_iota(I32, shape, 1)
    unit = jnp.where(lane == row, 1.0, 0.0).astype(F32)
    work = jnp.where((lane >= width) & (lane < 2 * width), gram, unit)
    diagonal = jnp.ones(shape, F32)
    for base in range(0, width, STRIDE):
        tall = [jnp.broadcast_to(work[:, width + base + i : width + base + i + 1], shape) for i in range(STRIDE)]
        wide = [jnp.broadcast_to(work[base + i : base + i + 1, :], shape) for i in range(STRIDE)]
        cell = {
            (m, i): jnp.broadcast_to(tall[i][base + m : base + m + 1, :], shape)
            for i in range(STRIDE)
            for m in range(i, STRIDE)
        }
        for i in range(STRIDE):
            inverse = 1.0 / cell[i, i]
            diagonal = jnp.where(row == base + i, cell[i, i], diagonal)
            scale = jnp.where(row > base + i, tall[i] * inverse, 0.0)
            work = work - scale * wide[i]
            for m in range(i + 1, STRIDE):
                ratio = cell[m, i] * inverse
                wide[m] = wide[m] - ratio * wide[i]
                tall[m] = tall[m] - scale * cell[m, i]
                for n in range(m, STRIDE):
                    cell[n, m] = cell[n, m] - ratio * cell[n, i]
    work = work / jnp.sqrt(diagonal)
    upper = jnp.where((lane < 2 * width) & (lane >= row + width), work, 0.0)
    inverse = jnp.where(lane <= row, work, 0.0)
    return upper, inverse


def factor_of(upper):
    width = upper.shape[0]
    return upper[:, width : 2 * width].T


def flip(index, distance, size):
    total, bit = 0, 1
    while bit < size:
        total = total + bit * lax.rem(lax.div(index, bit) + lax.div(distance, bit), 2)
        bit *= 2
    return total


def kernel(
    grp_size, col_size, node_total,
    start_ref, tiles_ref, row_ref, col_ref, count_ref,
    basis_ref, proj_ref, factors_ref,
    raw, merged, high, low, high_t, low_t, rows_v, cols_v, table_v, table,
    u_ref, lr_ref, stack, lstack, row_panel, col_panel, row_split, col_split,
    acc_row, acc_col, got_row, got_col, deg_row, deg_col, deg_got_row, deg_got_col,
    degree_ref, sigma_ref, shift_ref, left_ref, upper_ref, coeff_ref, red_col, red_grp, early, late,
    tile_sem, in_sem, gather_row_sem, gather_col_sem, scatter_row_sem, scatter_col_sem,
    deg_row_sem, deg_col_sem, red_col_sem, red_grp_sem, early_sem, late_sem,
):
    grp = lax.axis_index("grp")
    col = lax.axis_index("col")
    slots, tile_size = raw.shape[0], raw.shape[1]
    width = u_ref.shape[1]
    small = (width, LANES)
    row = lax.broadcasted_iota(I32, small, 0)
    lane = lax.broadcasted_iota(I32, small, 1)

    def other(t):
        dg, dc = lax.div(t, col_size), lax.rem(t, col_size)
        return flip(grp, dg, grp_size), flip(col, dc, col_size)

    loads_of = tile_sem.shape[0]
    share = slots // loads_of

    def load_tile(n):
        at = pl.ds(n * share, share)
        return pltpu.make_async_copy(tiles_ref.at[at], raw.at[at], tile_sem.at[n])

    loads = (
        pltpu.make_async_copy(start_ref, u_ref.at[0], in_sem.at[0]),
        pltpu.make_async_copy(row_ref, rows_v, in_sem.at[1]),
        pltpu.make_async_copy(col_ref, cols_v, in_sem.at[2]),
    )
    for copy in loads:
        copy.start()

    def start_load(s, carry):
        load_tile(s).start()
        return carry

    lax.fori_loop(0, loads_of, start_load, 0)

    barrier = pltpu.get_barrier_semaphore()

    def greet(t, carry):
        pl.semaphore_signal(barrier, inc=1, device_id=other(t), device_id_type=MESH)
        return carry

    everyone = grp_size * col_size
    lax.fori_loop(1, everyone, greet, 0, unroll=everyone <= 32)

    def copy_to(axis, d, source, target, send_sem, recv_sem):
        size = col_size if axis == "col" else grp_size
        peer = flip(col if axis == "col" else grp, d, size)
        return pltpu.make_async_remote_copy(
            src_ref=source(peer),
            dst_ref=target,
            send_sem=send_sem,
            recv_sem=recv_sem,
            device_id=(grp, peer) if axis == "col" else (peer, col),
            device_id_type=MESH,
        )

    def send(axis, source, target, sems):
        size = col_size if axis == "col" else grp_size

        def visit(d, carry):
            copy_to(axis, size - d, source, target, sems.at[0], sems.at[1]).start()
            return carry

        lax.fori_loop(1, size, visit, 0, unroll=size <= 8)

    def bytes_of(part, send_sem, recv_sem):
        return pltpu.make_async_remote_copy(
            src_ref=part, dst_ref=part, send_sem=send_sem, recv_sem=recv_sem,
            device_id=other(1), device_id_type=MESH,
        )

    def await_all(buf, sems):
        bytes_of(buf.at[pl.ds(0, buf.shape[0] - 1)], sems.at[0], sems.at[1]).wait()

    col_groups = ((1, grp_size - 1), (grp_size - 1, grp_size))
    row_groups = ((1, 2), (2, 4), (4, col_size))

    def gather(axis, par, panel, sems, groups):
        me = col if axis == "col" else grp
        for n, (low_d, high_d) in reversed(list(enumerate(groups))):

            def visit(i, carry):
                d = high_d - 1 - i
                target = panel.at[par, me]
                copy_to(axis, d, lambda peer: u_ref.at[par], target, sems.at[par, 0], sems.at[par, n + 1]).start()
                return carry

            lax.fori_loop(0, high_d - low_d, visit, 0, unroll=high_d - low_d <= 8)

    def arrive(par, panel, sems, groups, n):
        count = groups[n][1] - groups[n][0]
        bytes_of(panel.at[par, pl.ds(0, count)], sems.at[par, 0], sems.at[par, n + 1]).wait_recv()

    def leave(par, panel, sems):
        count = panel.shape[1] - 1
        bytes_of(panel.at[par, pl.ds(0, count)], sems.at[par, 0], sems.at[par, 1]).wait_send()

    col_side = (col_panel, gather_col_sem, col_groups)
    row_side = (row_panel, gather_row_sem, row_groups)

    def spread(axis, buf, sems, start):
        me = col if axis == "col" else grp
        if start:
            send(axis, lambda peer: buf.at[me], buf.at[me], sems)
        else:
            await_all(buf, sems)

    def spread_all(buf, sems):
        me = grp * col_size + col

        def visit(t, carry):
            pltpu.make_async_remote_copy(
                src_ref=buf.at[me], dst_ref=buf.at[me], send_sem=sems.at[0], recv_sem=sems.at[1],
                device_id=other(everyone - t), device_id_type=MESH,
            ).start()
            return carry

        lax.fori_loop(1, everyone, visit, 0, unroll=everyone <= 32)

    def position(r, q):
        return table[0, r * grp_size + q]

    def send_rows(par, r, d, with_degree):
        sems = scatter_row_sem.at[par]
        copy_to("col", d, lambda peer: acc_row.at[r], got_row.at[par, col], sems.at[0], sems.at[1]).start()
        if with_degree:
            sems = deg_row_sem
            copy_to("col", d, lambda peer: deg_row.at[r], deg_got_row.at[col], sems.at[0], sems.at[1]).start()

    def halves(panel, par, size, split):
        for place in range(size):
            first, second = split_two(panel[par, place])
            at = pl.ds(place * tile_size, tile_size)
            split[:width, at] = first
            split[width : 2 * width, at] = jnp.ones((width, tile_size), BF16)
            split[2 * width :, at] = second

    def combine(total, rest):
        piece = total[:width] + total[2 * width :] + rest[:width]
        return piece, total[width : width + 1] + rest[width : width + 1]

    def rows_of(r):
        places = [position(r, q) for q in range(grp_size)]
        left = col_split[...]
        firsts = jnp.concatenate([high[p] for p in places], axis=1)
        seconds = jnp.concatenate([low[p] for p in places], axis=1)
        return combine(dot_nt(left, firsts), dot_nt(left[: 2 * width], seconds))

    def cols_of(q):
        piece, degree = 0.0, 0.0
        for base in range(0, col_size, CHUNK):
            left = row_split[:, pl.ds(base * tile_size, CHUNK * tile_size)]
            places = [position(base + r, q) for r in range(CHUNK)]
            firsts = jnp.concatenate([high[p] for p in places], axis=0)
            seconds = jnp.concatenate([low[p] for p in places], axis=0)
            part, extra = combine(dot_nn(left, firsts), dot_nn(left[: 2 * width], seconds))
            piece = piece + part
            degree = degree + extra
        return piece, degree

    def first_rows():
        def visit(d):
            r = flip(col, d, col_size)
            piece, degree = rows_of(r)
            acc_row[r] = piece
            deg_row[r] = degree

        def go(ds):
            for d in ds:
                visit(d)
            for d in ds:
                if not isinstance(d, int) or d:
                    send_rows(0, flip(col, d, col_size), d, True)

        if col_size <= 8:
            go(range(col_size // 2, col_size))
            go(range(col_size // 2))
        else:
            def each(d, carry):
                go([d])
                return carry

            lax.fori_loop(1, col_size, each, 0)
            visit(0)
        got_row[0, col] = acc_row[col]
        deg_got_row[col] = deg_row[col]

    def first_cols():
        for d in range(grp_size - 1, -1, -1):
            q = flip(grp, d, grp_size)
            piece, degree = cols_of(q)
            acc_col[q] = piece
            deg_col[q] = degree
        send("grp", lambda peer: acc_col.at[peer], got_col.at[0, grp], scatter_col_sem.at[0])
        got_col[0, grp] = acc_col[grp]
        send("grp", lambda peer: deg_col.at[peer], deg_got_col.at[grp], deg_col_sem)
        deg_got_col[grp] = deg_col[grp]

    def stacked(pieces):
        pairs = [split_two(piece) for piece in pieces]
        return jnp.concatenate([jnp.concatenate(pair, axis=0) for pair in pairs], axis=1)

    def product(left, firsts, seconds):
        total = dot_nn(left, jnp.concatenate(firsts, axis=0))
        rest = dot_nn(left[:width], jnp.concatenate(seconds, axis=0))
        return total[:width] + total[width:] + rest

    def rows_batch(par, ds):
        places = [flip(grp, d, grp_size) for d in ds]
        left = stacked([u_ref[par] if d == 0 else col_panel[par, q] for d, q in zip(ds, places)])

        def visit(r, carry):
            at = [position(r, q) for q in places]
            piece = product(left, [high_t[p] for p in at], [low_t[p] for p in at])
            acc_row[r] = piece if ds[0] == 0 else acc_row[r] + piece
            return carry

        if col_size <= 8:
            for r in range(col_size):
                visit(r, 0)
        else:
            lax.fori_loop(0, col_size, visit, 0)

    def cols_batch(par, base, count):
        places = [flip(col, base + i, col_size) for i in range(count)]
        own = isinstance(base, int) and base == 0
        left = stacked([u_ref[par]] if own else [row_panel[par, r] for r in places])
        for q in range(grp_size):
            at = [position(r, q) for r in places]
            piece = product(left, [high[p] for p in at], [low[p] for p in at])
            acc_col[q] = piece if own else acc_col[q] + piece

    def collect(par, with_degree):
        leave(par, col_panel, gather_col_sem)
        leave(par, row_panel, gather_row_sem)
        await_all(got_row.at[par], scatter_row_sem.at[par])
        await_all(got_col.at[par], scatter_col_sem.at[par])
        if with_degree:
            await_all(deg_got_row, deg_row_sem)
            await_all(deg_got_col, deg_col_sem)
            degree_ref[...] = jnp.sum(deg_got_row[...], axis=0) + jnp.sum(deg_got_col[...], axis=0)
        total = jnp.sum(got_row[par], axis=0) + jnp.sum(got_col[par], axis=0)
        return degree_ref[...] * u_ref[par] - total

    stack[...] = jnp.zeros_like(stack)
    lstack[...] = jnp.zeros_like(lstack)
    loads[1].wait()
    loads[2].wait()
    spots = table.shape[1]
    offset = rows_v[...] - grp * col_size
    pick = lax.div(cols_v[...] - col, col_size)
    place = jnp.clip(offset, 0, col_size - 1) * grp_size + jnp.clip(pick, 0, grp_size - 1)
    square = (slots, slots)
    down = lax.broadcasted_iota(I32, square, 0)
    across = lax.broadcasted_iota(I32, square, 1)
    wide = jnp.broadcast_to(place, square)
    tall = jnp.sum(jnp.where(down == across, wide, 0), axis=1, keepdims=True)
    same = (wide == jnp.broadcast_to(tall, square)) & (down < across)
    before = jnp.max(jnp.where(same, down, -1), axis=0, keepdims=True)
    before = jnp.where(before < 0, slots, before)
    long = (slots, spots)
    depth = lax.broadcasted_iota(I32, long, 0)
    spot = lax.broadcasted_iota(I32, long, 1)
    here = (jnp.broadcast_to(tall, long) == spot) & (depth < count_ref[0])
    last = jnp.max(jnp.where(here, depth, -1), axis=0, keepdims=True)
    table_v[0:1, :] = jnp.where(last < 0, slots, last)
    table_v[1:2, :slots] = before
    move = pltpu.make_async_copy(table_v, table, in_sem.at[3])
    move.start()
    empty = jnp.zeros((tile_size, tile_size), F32)
    merged[slots] = empty
    high[slots] = empty.astype(BF16)
    low[slots] = empty.astype(BF16)
    high_t[slots] = empty.astype(BF16)
    low_t[slots] = empty.astype(BF16)
    loads[0].wait()
    start = u_ref[0]
    stack[0] = start
    stack[1] = start
    row_panel[0, col] = start
    col_panel[0, grp] = start
    pl.semaphore_wait(barrier, everyone - 1)
    gather("grp", 0, *col_side)
    gather("col", 0, *row_side)
    move.wait()

    def merge(n, carry):
        load_tile(n).wait()

        def visit(m, carry):
            s = n * share + m
            value = raw[s] + merged[table[1, s]]
            merged[s] = value
            first, second = split_two(value)
            high[s] = first
            low[s] = second
            return carry

        return lax.fori_loop(0, share, visit, carry)

    lax.fori_loop(0, loads_of, merge, 0)

    for n in range(len(col_groups)):
        arrive(0, *col_side, n)
    halves(col_panel, 0, grp_size, col_split)
    first_rows()
    for n in range(len(row_groups)):
        arrive(0, *row_side, n)
    halves(row_panel, 0, col_size, row_split)
    first_cols()

    def turn(s, carry):
        high_t[s] = high[s].T
        low_t[s] = low[s].T
        return carry

    lax.fori_loop(0, slots, turn, 0, unroll=4)
    applied = collect(0, True)
    lr_ref[...] = applied
    u_ref[1] = applied
    sigma_ref[...] = jnp.zeros_like(sigma_ref)
    left_ref[ITERS] = jnp.where(lane == row, 1.0, 0.0)

    half = width // 2

    def fold(value):
        return jnp.where(lane[:half] < LANES // 2, value[:half], value[half:])

    def unfold(packed):
        turned = pltpu.roll(packed, LANES // 2, 1)
        low_lanes = lane[:half] < LANES // 2
        return jnp.concatenate(
            [jnp.where(low_lanes, packed, turned), jnp.where(low_lanes, turned, packed)], axis=0
        )

    def inner_products(par, block_v):
        block = stack[0:4].reshape(4 * width, tile_size)
        block = jnp.concatenate([block, block], axis=0)
        both = dot_nt(jnp.concatenate([block_v, stack[1]], axis=0), block, HIGHEST)
        inner = lax.rem(lane, 4 * width)
        red_grp[par, grp] = fold(jnp.where((inner >= width) & (inner < 2 * width), both[width:], both[:width]))

    inner_products(1, applied)

    def step(k, carry):
        par = lax.rem(k + 1, 2)
        block_u, block_r = u_ref[par], stack[1]
        gather("grp", par, *col_side)
        spread("grp", red_grp.at[par], red_grp_sem.at[par], True)
        gather("col", par, *row_side)

        rows_batch(par, [0])
        cols_batch(par, 0, 1)
        arrive(par, *col_side, 0)
        spread("grp", red_grp.at[par], red_grp_sem.at[par], False)
        red_col[par, col] = jnp.sum(red_grp[par], axis=0)
        spread("col", red_col.at[par], red_col_sem.at[par], True)
        arrive(par, *col_side, 1)
        rows_batch(par, list(range(1, grp_size - 1)))
        rows_batch(par, [grp_size - 1])
        send("col", lambda peer: acc_row.at[peer], got_row.at[par, col], scatter_row_sem.at[par])
        got_row[par, col] = acc_row[col]
        arrive(par, *row_side, 0)
        arrive(par, *row_side, 1)
        cols_batch(par, 1, 3)
        arrive(par, *row_side, 2)
        if col_size <= 8:
            cols_batch(par, 4, col_size - 4)
        else:
            def visit(n, carry):
                cols_batch(par, 4 * n, 4)
                return carry

            lax.fori_loop(1, col_size // 4, visit, 0)
        send("grp", lambda peer: acc_col.at[peer], got_col.at[par, grp], scatter_col_sem.at[par])
        got_col[par, grp] = acc_col[grp]

        spread("col", red_col.at[par], red_col_sem.at[par], False)
        total = unfold(jnp.sum(red_col[par], axis=0) / node_total)
        former = left_ref[lax.rem(k + ITERS, ITERS + 1)]
        turned = dot_nn(former[:, :width], total, HIGHEST)
        upper, inverse = factorize(total)
        left = inverse[:, :width]
        fresh = dot_nn(left, jnp.concatenate([block_r, lr_ref[...]], axis=1), HIGHEST)
        newest, image = fresh[:, :tile_size], fresh[:, tile_size:]
        pad = jnp.concatenate([inverse, jnp.zeros((LANES - width, LANES), F32)], axis=0)
        mixed = dot_nt(turned[:, :width], pad[:, :width], HIGHEST)
        older = (lane >= 2 * width) & (lane < 4 * width)
        coeffs = jnp.where(lane < width, mixed, jnp.where(older, turned, 0.0))
        stack[0] = newest
        lstack[0] = image
        now = dot_nn(coeffs, jnp.concatenate([stack[...].reshape(LANES, tile_size),
                                              lstack[...].reshape(LANES, tile_size)], axis=1), HIGHEST)
        rest = block_u - now[:, :tile_size]
        residual = dot_nn(left, rest, HIGHEST)
        on_block = jnp.sum(jnp.where(lane == row, turned, 0.0), axis=1, keepdims=True)
        on_gram = jnp.sum(jnp.where(lane == row + width, total, 0.0), axis=1, keepdims=True)
        mean = jnp.sum(on_block, axis=0, keepdims=True) / jnp.sum(on_gram, axis=0, keepdims=True)
        before = sigma_ref[...]
        sigma = before + jnp.broadcast_to(mean, sigma_ref.shape)
        known = now[:, tile_size:] + sigma * rest
        stack[0] = residual
        stack[1] = residual
        stack[k + 2] = newest
        lstack[k + 2] = image

        @pl.when(k == ITERS - 2)
        def _():
            shifted = [lstack[j] - sigma * stack[j] for j in (4, 2, 3)]
            block = jnp.concatenate([shifted[0], residual, shifted[1], shifted[2]] * 2, axis=0)
            early[grp * col_size + col] = fold(dot_nt(residual, block, HIGHEST))
            spread_all(early, early_sem)

        basis_ref[k] = newest
        left_ref[k] = inverse
        upper_ref[k] = upper
        coeff_ref[k] = coeffs
        sigma_ref[...] = sigma
        shift_ref[k] = before[:, :LANES]

        applied = collect(par, False) - known
        fresh_u = dot_nn(left, applied, HIGHEST)
        inner_products(1 - par, applied)
        u_ref[1 - par] = fresh_u
        lr_ref[...] = fresh_u + sigma * residual
        return carry

    lax.fori_loop(0, ITERS - 1, step, 0)

    k = ITERS - 1
    par = ITERS % 2
    quarter = width // 4
    block_u, block_r = u_ref[par], stack[1]
    both = dot_nt(block_u, jnp.concatenate([block_r, block_u] * (LANES // (2 * width)), axis=0), HIGHEST)
    both = fold(both)
    odd = lax.rem(lax.div(lane[:quarter], 2 * width), 2) == 1
    late[grp * col_size + col] = jnp.where(odd, both[quarter:], both[:quarter])
    spread_all(late, late_sem)
    await_all(early, early_sem)
    total = unfold(jnp.sum(early[...], axis=0) / node_total)
    upper, inverse = factorize(total)
    left = inverse[:, :width]
    newest = dot_nn(left, block_r, HIGHEST)
    stack[0] = newest
    basis_ref[k] = newest
    factors_ref[k] = factor_of(upper)
    older = jnp.where((lane >= 2 * width) & (lane < 5 * width), total, 0.0)
    pad = jnp.concatenate([inverse, jnp.zeros((LANES - width, LANES), F32)], axis=0)[:, :width]
    proj_ref[...] = jnp.zeros_like(proj_ref)

    def keep_coeffs(k, left, coeffs, shift):
        found = dot_nn(left, coeffs, HIGHEST) + jnp.where(lane == row, shift, 0.0)
        for j in range(k):
            proj_ref[k, j] = found[:, (j + 2) * width : (j + 3) * width]
        proj_ref[k, k] = found[:, :width]

    for n in range(ITERS - 1):
        keep_coeffs(n, left_ref[n, :, :width], coeff_ref[n], shift_ref[n])
        factors_ref[n] = factor_of(upper_ref[n])
    await_all(late, late_sem)
    packed = jnp.sum(late[...], axis=0) / node_total
    total = jnp.concatenate(
        [packed] + [pltpu.roll(packed, LANES - n * 2 * width, 1) for n in range(1, 4)], axis=0
    )
    coeffs = dot_nt(total[:, :width], pad, HIGHEST) + older
    middle = jnp.zeros((width, LANES), F32)
    beside = jnp.concatenate([middle, coeffs] + [middle] * (LANES // width - 2), axis=0)
    gram = total - dot_nt(coeffs, beside, HIGHEST)
    rest = block_u - dot_nn(coeffs, stack[...].reshape(LANES, tile_size), HIGHEST)
    upper, inverse = factorize(gram)
    basis_ref[ITERS] = dot_nn(inverse[:, :width], rest, HIGHEST)
    factors_ref[ITERS] = dot_nt(left, upper[:, width : 2 * width], HIGHEST)
    keep_coeffs(k, left, coeffs, sigma_ref[:, :LANES])


def deliver(basis, proj, factors, basis_out, proj_out, factors_out, sem):
    pairs = ((basis, basis_out), (proj, proj_out), (factors, factors_out))
    copies = [pltpu.make_async_copy(source, target, sem.at[n]) for n, (source, target) in enumerate(pairs)]
    for copy in copies:
        copy.start()
    for copy in copies:
        copy.wait()


def solution(mesh):
    grp_size, col_size = mesh.shape["grp"], mesh.shape["col"]

    def body(start_block, tile_values, tile_row, tile_col, tile_count):
        width, shard_len = start_block.shape
        slots, tile_size = tile_values.shape[2], tile_values.shape[3]
        assert shard_len == tile_size and LANES // width == 8
        assert grp_size > 2 and col_size % CHUNK == 0
        assert grp_size & (grp_size - 1) == 0 and col_size & (col_size - 1) == 0
        places = LANES // width
        node_total = shard_len * grp_size * col_size
        spots = -(-max(grp_size * col_size, slots) // LANES) * LANES
        vmem = pl.BlockSpec(memory_space=pltpu.VMEM)
        smem = pl.BlockSpec(memory_space=pltpu.SMEM)
        hbm = pl.BlockSpec(memory_space=pl.ANY)
        block = (width, tile_size)
        line = (1, tile_size)
        tiles = (slots + 1, tile_size, tile_size)
        packed = (width // 2, LANES)
        small = (width, LANES)

        def sems(*sizes):
            return pltpu.SemaphoreType.DMA(sizes)

        def pinned(value):
            return pltpu.with_memory_space_constraint(value, pltpu.HBM)

        shapes = (
            jax.ShapeDtypeStruct((ITERS + 1,) + block, F32),
            jax.ShapeDtypeStruct((ITERS, ITERS, width, width), F32),
            jax.ShapeDtypeStruct((ITERS + 1, width, width), F32),
        )
        results = pl.pallas_call(
            functools.partial(kernel, grp_size, col_size, node_total),
            out_shape=shapes,
            in_specs=[hbm, hbm, hbm, hbm, smem],
            out_specs=(vmem, vmem, vmem),
            scratch_shapes=[
                pltpu.VMEM((slots, tile_size, tile_size), F32),
                pltpu.VMEM(tiles, F32),
                pltpu.VMEM(tiles, BF16),
                pltpu.VMEM(tiles, BF16),
                pltpu.VMEM(tiles, BF16),
                pltpu.VMEM(tiles, BF16),
                pltpu.VMEM((1, slots), I32),
                pltpu.VMEM((1, slots), I32),
                pltpu.VMEM((8, spots), I32),
                pltpu.SMEM((8, spots), I32),
                pltpu.VMEM((2,) + block, F32),
                pltpu.VMEM(block, F32),
                pltpu.VMEM((places,) + block, F32),
                pltpu.VMEM((places,) + block, F32),
                pltpu.VMEM((2, col_size) + block, F32),
                pltpu.VMEM((2, grp_size) + block, F32),
                pltpu.VMEM((3 * width, col_size * tile_size), BF16),
                pltpu.VMEM((3 * width, grp_size * tile_size), BF16),
                pltpu.VMEM((col_size,) + block, F32),
                pltpu.VMEM((grp_size,) + block, F32),
                pltpu.VMEM((2, col_size) + block, F32),
                pltpu.VMEM((2, grp_size) + block, F32),
                pltpu.VMEM((col_size,) + line, F32),
                pltpu.VMEM((grp_size,) + line, F32),
                pltpu.VMEM((col_size,) + line, F32),
                pltpu.VMEM((grp_size,) + line, F32),
                pltpu.VMEM(line, F32),
                pltpu.VMEM(block, F32),
                pltpu.VMEM((ITERS,) + small, F32),
                pltpu.VMEM((ITERS + 1,) + small, F32),
                pltpu.VMEM((ITERS,) + small, F32),
                pltpu.VMEM((ITERS,) + small, F32),
                pltpu.VMEM((2, col_size) + packed, F32),
                pltpu.VMEM((2, grp_size) + packed, F32),
                pltpu.VMEM((grp_size * col_size,) + packed, F32),
                pltpu.VMEM((grp_size * col_size, width // 4, LANES), F32),
                sems(8 if slots % 8 == 0 else slots),
                sems(4),
                sems(2, 4), sems(2, 3), sems(2, 2), sems(2, 2),
                sems(2), sems(2), sems(2, 2), sems(2, 2), sems(2), sems(2),
            ],
            compiler_params=pltpu.CompilerParams(
                collective_id=0, has_side_effects=True, vmem_limit_bytes=40 * 1024 * 1024
            ),
        )(
            pinned(start_block),
            pinned(tile_values.reshape(slots, tile_size, tile_size)),
            pinned(tile_row.reshape(1, slots)),
            pinned(tile_col.reshape(1, slots)),
            tile_count.reshape(1),
        )
        return pl.pallas_call(
            deliver,
            out_shape=shapes,
            in_specs=[vmem] * 3,
            out_specs=[hbm] * 3,
            scratch_shapes=[sems(3)],
        )(*(pltpu.with_memory_space_constraint(value, pltpu.VMEM) for value in results))

    in_specs = (
        P(None, ("grp", "col")),
        P("grp", "col", None, None, None),
        P("grp", "col", None),
        P("grp", "col", None),
        P("grp", "col"),
    )
    out_specs = (P(None, None, ("grp", "col")), P(), P())
    return jax.shard_map(body, mesh=mesh, in_specs=in_specs, out_specs=out_specs, check_vma=False)
```

```python
import functools

import jax
import jax.numpy as jnp
from jax import lax
from jax.experimental import pallas as pl
from jax.experimental.pallas import tpu as pltpu
from jax.sharding import PartitionSpec as P

ITERS = 4
HIGHEST = lax.Precision.HIGHEST
MESH = pl.DeviceIdType.MESH
F32 = jnp.float32
BF16 = jnp.bfloat16
I32 = jnp.int32
LANES = 128
CHUNK = 8
STRIDE = 8
UNROLL = 4


def dot_nt(left, right, precision=None):
    dims = (((1,), (1,)), ((), ()))
    return lax.dot_general(left, right, dims, precision=precision, preferred_element_type=F32)


def dot_nn(left, right, precision=None):
    dims = (((1,), (0,)), ((), ()))
    return lax.dot_general(left, right, dims, precision=precision, preferred_element_type=F32)


def split_two(value):
    high = value.astype(BF16)
    low = (value - high.astype(F32)).astype(BF16)
    return high, low


def factorize(gram):
    width = gram.shape[0]
    shape = gram.shape
    row = lax.broadcasted_iota(I32, shape, 0)
    lane = lax.broadcasted_iota(I32, shape, 1)
    unit = jnp.where(lane == row, 1.0, 0.0).astype(F32)
    work = jnp.where((lane >= width) & (lane < 2 * width), gram, unit)
    diagonal = jnp.ones(shape, F32)
    for base in range(0, width, STRIDE):
        tall = [jnp.broadcast_to(work[:, width + base + i : width + base + i + 1], shape) for i in range(STRIDE)]
        wide = [jnp.broadcast_to(work[base + i : base + i + 1, :], shape) for i in range(STRIDE)]
        cell = {
            (m, i): jnp.broadcast_to(tall[i][base + m : base + m + 1, :], shape)
            for i in range(STRIDE)
            for m in range(i, STRIDE)
        }
        for i in range(STRIDE):
            inverse = 1.0 / cell[i, i]
            diagonal = jnp.where(row == base + i, cell[i, i], diagonal)
            scale = jnp.where(row > base + i, tall[i] * inverse, 0.0)
            work = work - scale * wide[i]
            for m in range(i + 1, STRIDE):
                ratio = cell[m, i] * inverse
                wide[m] = wide[m] - ratio * wide[i]
                tall[m] = tall[m] - scale * cell[m, i]
                for n in range(m, STRIDE):
                    cell[n, m] = cell[n, m] - ratio * cell[n, i]
    work = work / jnp.sqrt(diagonal)
    upper = jnp.where((lane < 2 * width) & (lane >= row + width), work, 0.0)
    inverse = jnp.where(lane <= row, work, 0.0)
    return upper, inverse


def factor_of(upper):
    width = upper.shape[0]
    return upper[:, width : 2 * width].T


def flip(index, distance, size):
    total, bit = 0, 1
    while bit < size:
        total = total + bit * lax.rem(lax.div(index, bit) + lax.div(distance, bit), 2)
        bit *= 2
    return total


def kernel(
    grp_size, col_size, node_total,
    start_ref, tiles_ref, row_ref, col_ref, count_ref,
    basis_ref, proj_ref, factors_ref,
    raw, merged, high, low, high_t, low_t, rows_v, cols_v, table_v, table,
    u_ref, lr_ref, stack, lstack, row_panel, col_panel, row_split, col_split,
    acc_row, acc_col, got_row, got_col, deg_row, deg_col, deg_got_row, deg_got_col,
    degree_ref, sigma_ref, shift_ref, left_ref, upper_ref, coeff_ref, red_col, red_grp, early_grp, early_col, late,
    tile_sem, in_sem, gather_row_sem, gather_col_sem, scatter_row_sem, scatter_col_sem,
    deg_row_sem, deg_col_sem, red_col_sem, red_grp_sem, early_grp_sem, early_col_sem, late_sem,
):
    grp = lax.axis_index("grp")
    col = lax.axis_index("col")
    slots, tile_size = raw.shape[0], raw.shape[1]
    width = u_ref.shape[1]
    small = (width, LANES)
    row = lax.broadcasted_iota(I32, small, 0)
    lane = lax.broadcasted_iota(I32, small, 1)

    def other(t):
        dg, dc = lax.div(t, col_size), lax.rem(t, col_size)
        return flip(grp, dg, grp_size), flip(col, dc, col_size)

    loads_of = tile_sem.shape[0]
    share = slots // loads_of

    def load_tile(n):
        at = pl.ds(n * share, share)
        return pltpu.make_async_copy(tiles_ref.at[at], raw.at[at], tile_sem.at[n])

    loads = (
        pltpu.make_async_copy(start_ref, u_ref.at[0], in_sem.at[0]),
        pltpu.make_async_copy(row_ref, rows_v, in_sem.at[1]),
        pltpu.make_async_copy(col_ref, cols_v, in_sem.at[2]),
    )
    for copy in loads:
        copy.start()

    def start_load(s, carry):
        load_tile(s).start()
        return carry

    lax.fori_loop(0, loads_of, start_load, 0)

    barrier = pltpu.get_barrier_semaphore()

    def greet(t, carry):
        pl.semaphore_signal(barrier, inc=1, device_id=other(t), device_id_type=MESH)
        return carry

    everyone = grp_size * col_size
    lax.fori_loop(1, everyone, greet, 0, unroll=everyone <= 32)

    def copy_to(axis, d, source, target, send_sem, recv_sem):
        size = col_size if axis == "col" else grp_size
        peer = flip(col if axis == "col" else grp, d, size)
        return pltpu.make_async_remote_copy(
            src_ref=source(peer),
            dst_ref=target,
            send_sem=send_sem,
            recv_sem=recv_sem,
            device_id=(grp, peer) if axis == "col" else (peer, col),
            device_id_type=MESH,
        )

    def send(axis, source, target, sems):
        size = col_size if axis == "col" else grp_size

        def visit(d, carry):
            copy_to(axis, size - d, source, target, sems.at[0], sems.at[1]).start()
            return carry

        lax.fori_loop(1, size, visit, 0, unroll=size <= 8)

    def bytes_of(part, send_sem, recv_sem):
        return pltpu.make_async_remote_copy(
            src_ref=part, dst_ref=part, send_sem=send_sem, recv_sem=recv_sem,
            device_id=other(1), device_id_type=MESH,
        )

    def await_all(buf, sems):
        bytes_of(buf.at[pl.ds(0, buf.shape[0] - 1)], sems.at[0], sems.at[1]).wait()

    col_groups = ((1, grp_size - 1), (grp_size - 1, grp_size))
    row_groups = ((1, 2), (2, 4), (4, col_size))

    def gather(axis, par, panel, sems, groups):
        me = col if axis == "col" else grp
        for n, (low_d, high_d) in reversed(list(enumerate(groups))):

            def visit(i, carry):
                d = high_d - 1 - i
                target = panel.at[par, me]
                copy_to(axis, d, lambda peer: u_ref.at[par], target, sems.at[par, 0], sems.at[par, n + 1]).start()
                return carry

            lax.fori_loop(0, high_d - low_d, visit, 0, unroll=high_d - low_d <= 8)

    def arrive(par, panel, sems, groups, n):
        count = groups[n][1] - groups[n][0]
        bytes_of(panel.at[par, pl.ds(0, count)], sems.at[par, 0], sems.at[par, n + 1]).wait_recv()

    def leave(par, panel, sems):
        count = panel.shape[1] - 1
        bytes_of(panel.at[par, pl.ds(0, count)], sems.at[par, 0], sems.at[par, 1]).wait_send()

    col_side = (col_panel, gather_col_sem, col_groups)
    row_side = (row_panel, gather_row_sem, row_groups)

    def spread(axis, buf, sems, start):
        me = col if axis == "col" else grp
        if start:
            send(axis, lambda peer: buf.at[me], buf.at[me], sems)
        else:
            await_all(buf, sems)

    def spread_all(buf, sems):
        me = grp * col_size + col

        def visit(t, carry):
            pltpu.make_async_remote_copy(
                src_ref=buf.at[me], dst_ref=buf.at[me], send_sem=sems.at[0], recv_sem=sems.at[1],
                device_id=other(everyone - t), device_id_type=MESH,
            ).start()
            return carry

        lax.fori_loop(1, everyone, visit, 0, unroll=everyone <= 32)

    def position(r, q):
        return table[0, r * grp_size + q]

    def send_rows(par, r, d, with_degree):
        sems = scatter_row_sem.at[par]
        copy_to("col", d, lambda peer: acc_row.at[r], got_row.at[par, col], sems.at[0], sems.at[1]).start()
        if with_degree:
            sems = deg_row_sem
            copy_to("col", d, lambda peer: deg_row.at[r], deg_got_row.at[col], sems.at[0], sems.at[1]).start()

    def halves(panel, par, size, split):
        for place in range(size):
            first, second = split_two(panel[par, place])
            at = pl.ds(place * tile_size, tile_size)
            split[:width, at] = first
            split[width : 2 * width, at] = jnp.ones((width, tile_size), BF16)
            split[2 * width :, at] = second

    def combine(total, rest):
        piece = total[:width] + total[2 * width :] + rest[:width]
        return piece, total[width : width + 1] + rest[width : width + 1]

    def rows_of(r):
        places = [position(r, q) for q in range(grp_size)]
        left = col_split[...]
        firsts = jnp.concatenate([high_t[p] for p in places], axis=0)
        seconds = jnp.concatenate([low[p] for p in places], axis=1)
        return combine(dot_nn(left, firsts), dot_nt(left[: 2 * width], seconds))

    def cols_of(q):
        piece, degree = 0.0, 0.0
        for base in range(0, col_size, CHUNK):
            left = row_split[:, pl.ds(base * tile_size, CHUNK * tile_size)]
            places = [position(base + r, q) for r in range(CHUNK)]
            firsts = jnp.concatenate([high[p] for p in places], axis=0)
            seconds = jnp.concatenate([low[p] for p in places], axis=0)
            part, extra = combine(dot_nn(left, firsts), dot_nn(left[: 2 * width], seconds))
            piece = piece + part
            degree = degree + extra
        return piece, degree

    def first_rows():
        def visit(d):
            r = flip(col, d, col_size)
            piece, degree = rows_of(r)
            acc_row[r] = piece
            deg_row[r] = degree

        def go(ds):
            for d in ds:
                visit(d)
            for d in ds:
                if not isinstance(d, int) or d:
                    send_rows(0, flip(col, d, col_size), d, True)

        if col_size <= 8:
            go(range(col_size // 2, col_size))
            go(range(col_size // 2))
        else:
            def each(d, carry):
                go([d])
                return carry

            lax.fori_loop(1, col_size, each, 0)
            visit(0)
        got_row[0, col] = acc_row[col]
        deg_got_row[col] = deg_row[col]

    def first_cols():
        for d in range(grp_size - 1, -1, -1):
            q = flip(grp, d, grp_size)
            piece, degree = cols_of(q)
            acc_col[q] = piece
            deg_col[q] = degree
        send("grp", lambda peer: acc_col.at[peer], got_col.at[0, grp], scatter_col_sem.at[0])
        got_col[0, grp] = acc_col[grp]
        send("grp", lambda peer: deg_col.at[peer], deg_got_col.at[grp], deg_col_sem)
        deg_got_col[grp] = deg_col[grp]

    def stacked(pieces):
        pairs = [split_two(piece) for piece in pieces]
        return jnp.concatenate([jnp.concatenate(pair, axis=0) for pair in pairs], axis=1)

    def product(left, firsts, seconds):
        total = dot_nn(left, jnp.concatenate(firsts, axis=0))
        rest = dot_nn(left[:width], jnp.concatenate(seconds, axis=0))
        return total[:width] + total[width:] + rest

    def rows_batch(par, ds):
        places = [flip(grp, d, grp_size) for d in ds]
        left = stacked([u_ref[par] if d == 0 else col_panel[par, q] for d, q in zip(ds, places)])

        def visit(r, carry):
            at = [position(r, q) for q in places]
            piece = product(left, [high_t[p] for p in at], [low_t[p] for p in at])
            acc_row[r] = piece if ds[0] == 0 else acc_row[r] + piece
            return carry

        if col_size <= 8:
            for r in range(col_size):
                visit(r, 0)
        else:
            lax.fori_loop(0, col_size, visit, 0)

    def cols_batch(par, base, count):
        places = [flip(col, base + i, col_size) for i in range(count)]
        own = isinstance(base, int) and base == 0
        left = stacked([u_ref[par]] if own else [row_panel[par, r] for r in places])
        for q in range(grp_size):
            at = [position(r, q) for r in places]
            piece = product(left, [high[p] for p in at], [low[p] for p in at])
            acc_col[q] = piece if own else acc_col[q] + piece

    def collect(par, with_degree):
        leave(par, col_panel, gather_col_sem)
        leave(par, row_panel, gather_row_sem)
        await_all(got_row.at[par], scatter_row_sem.at[par])
        await_all(got_col.at[par], scatter_col_sem.at[par])
        if with_degree:
            await_all(deg_got_row, deg_row_sem)
            await_all(deg_got_col, deg_col_sem)
            degree_ref[...] = jnp.sum(deg_got_row[...], axis=0) + jnp.sum(deg_got_col[...], axis=0)
        total = jnp.sum(got_row[par], axis=0) + jnp.sum(got_col[par], axis=0)
        return degree_ref[...] * u_ref[par] - total

    stack[...] = jnp.zeros_like(stack)
    lstack[...] = jnp.zeros_like(lstack)
    loads[1].wait()
    loads[2].wait()
    spots = table.shape[1]
    offset = rows_v[...] - grp * col_size
    pick = lax.div(cols_v[...] - col, col_size)
    place = jnp.clip(offset, 0, col_size - 1) * grp_size + jnp.clip(pick, 0, grp_size - 1)
    square = (slots, slots)
    down = lax.broadcasted_iota(I32, square, 0)
    across = lax.broadcasted_iota(I32, square, 1)
    wide = jnp.broadcast_to(place, square)
    tall = jnp.sum(jnp.where(down == across, wide, 0), axis=1, keepdims=True)
    same = (wide == jnp.broadcast_to(tall, square)) & (down < across)
    before = jnp.max(jnp.where(same, down, -1), axis=0, keepdims=True)
    before = jnp.where(before < 0, slots, before)
    long = (slots, spots)
    depth = lax.broadcasted_iota(I32, long, 0)
    spot = lax.broadcasted_iota(I32, long, 1)
    here = (jnp.broadcast_to(tall, long) == spot) & (depth < count_ref[0])
    last = jnp.max(jnp.where(here, depth, -1), axis=0, keepdims=True)
    table_v[0:1, :] = jnp.where(last < 0, slots, last)
    table_v[1:2, :slots] = before
    move = pltpu.make_async_copy(table_v, table, in_sem.at[3])
    move.start()
    empty = jnp.zeros((tile_size, tile_size), F32)
    merged[slots] = empty
    high[slots] = empty.astype(BF16)
    low[slots] = empty.astype(BF16)
    high_t[slots] = empty.astype(BF16)
    low_t[slots] = empty.astype(BF16)
    loads[0].wait()
    start = u_ref[0]
    stack[0] = start
    stack[1] = start
    row_panel[0, col] = start
    col_panel[0, grp] = start
    pl.semaphore_wait(barrier, everyone - 1)
    gather("grp", 0, *col_side)
    gather("col", 0, *row_side)
    move.wait()

    def merge(n, carry):
        load_tile(n).wait()

        def visit(m, carry):
            s = n * share + m
            value = raw[s] + merged[table[1, s]]
            merged[s] = value
            first, second = split_two(value)
            high[s] = first
            high_t[s] = first.T
            low[s] = second
            return carry

        return lax.fori_loop(0, share, visit, carry, unroll=UNROLL)

    lax.fori_loop(0, loads_of, merge, 0)

    for n in range(len(col_groups)):
        arrive(0, *col_side, n)
    halves(col_panel, 0, grp_size, col_split)
    first_rows()
    for n in range(len(row_groups)):
        arrive(0, *row_side, n)
    halves(row_panel, 0, col_size, row_split)
    first_cols()

    def turn(s, carry):
        low_t[s] = low[s].T
        return carry

    lax.fori_loop(0, slots, turn, 0, unroll=4)
    applied = collect(0, True)
    lr_ref[...] = applied
    u_ref[1] = applied
    sigma_ref[...] = jnp.zeros_like(sigma_ref)
    left_ref[ITERS] = jnp.where(lane == row, 1.0, 0.0)

    half = width // 2

    def fold(value):
        return jnp.where(lane[:half] < LANES // 2, value[:half], value[half:])

    def unfold(packed):
        turned = pltpu.roll(packed, LANES // 2, 1)
        low_lanes = lane[:half] < LANES // 2
        return jnp.concatenate(
            [jnp.where(low_lanes, packed, turned), jnp.where(low_lanes, turned, packed)], axis=0
        )

    def inner_products(par, block_v):
        block = stack[0:4].reshape(4 * width, tile_size)
        block = jnp.concatenate([block, block], axis=0)
        both = dot_nt(jnp.concatenate([block_v, stack[1]], axis=0), block, HIGHEST)
        inner = lax.rem(lane, 4 * width)
        red_grp[par, grp] = fold(jnp.where((inner >= width) & (inner < 2 * width), both[width:], both[:width]))

    gather("grp", 1, *col_side)
    inner_products(1, applied)

    def step(k, carry):
        par = lax.rem(k + 1, 2)
        block_u, block_r = u_ref[par], stack[1]
        spread("grp", red_grp.at[par], red_grp_sem.at[par], True)
        gather("col", par, *row_side)

        rows_batch(par, [0])
        cols_batch(par, 0, 1)
        arrive(par, *col_side, 0)
        rows_batch(par, list(range(1, grp_size - 1)))
        spread("grp", red_grp.at[par], red_grp_sem.at[par], False)
        red_col[par, col] = jnp.sum(red_grp[par], axis=0)
        spread("col", red_col.at[par], red_col_sem.at[par], True)
        arrive(par, *col_side, 1)
        rows_batch(par, [grp_size - 1])
        send("col", lambda peer: acc_row.at[peer], got_row.at[par, col], scatter_row_sem.at[par])
        got_row[par, col] = acc_row[col]
        arrive(par, *row_side, 0)
        arrive(par, *row_side, 1)
        cols_batch(par, 1, 3)
        arrive(par, *row_side, 2)
        if col_size <= 8:
            cols_batch(par, 4, col_size - 4)
        else:
            def visit(n, carry):
                cols_batch(par, 4 * n, 4)
                return carry

            lax.fori_loop(1, col_size // 4, visit, 0)
        send("grp", lambda peer: acc_col.at[peer], got_col.at[par, grp], scatter_col_sem.at[par])
        got_col[par, grp] = acc_col[grp]

        spread("col", red_col.at[par], red_col_sem.at[par], False)
        total = unfold(jnp.sum(red_col[par], axis=0) / node_total)
        former = left_ref[lax.rem(k + ITERS, ITERS + 1)]
        turned = dot_nn(former[:, :width], total, HIGHEST)
        upper, inverse = factorize(total)
        left = inverse[:, :width]
        fresh = dot_nn(left, jnp.concatenate([block_r, lr_ref[...]], axis=1), HIGHEST)
        newest, image = fresh[:, :tile_size], fresh[:, tile_size:]
        pad = jnp.concatenate([inverse, jnp.zeros((LANES - width, LANES), F32)], axis=0)
        mixed = dot_nt(turned[:, :width], pad[:, :width], HIGHEST)
        older = (lane >= 2 * width) & (lane < 4 * width)
        coeffs = jnp.where(lane < width, mixed, jnp.where(older, turned, 0.0))
        stack[0] = newest
        lstack[0] = image
        now = dot_nn(coeffs, jnp.concatenate([stack[...].reshape(LANES, tile_size),
                                              lstack[...].reshape(LANES, tile_size)], axis=1), HIGHEST)
        rest = block_u - now[:, :tile_size]
        residual = dot_nn(left, rest, HIGHEST)
        on_block = jnp.sum(jnp.where(lane == row, turned, 0.0), axis=1, keepdims=True)
        on_gram = jnp.sum(jnp.where(lane == row + width, total, 0.0), axis=1, keepdims=True)
        mean = jnp.sum(on_block, axis=0, keepdims=True) / jnp.sum(on_gram, axis=0, keepdims=True)
        before = sigma_ref[...]
        sigma = before + jnp.broadcast_to(mean, sigma_ref.shape)
        known = now[:, tile_size:] + sigma * rest
        stack[0] = residual
        stack[1] = residual
        stack[k + 2] = newest
        lstack[k + 2] = image

        @pl.when(k == ITERS - 2)
        def _():
            shifted = [lstack[j] - sigma * stack[j] for j in (4, 2, 3)]
            block = jnp.concatenate([shifted[0], residual, shifted[1], shifted[2]] * 2, axis=0)
            early_grp[grp] = fold(dot_nt(residual, block, HIGHEST))
            spread("grp", early_grp, early_grp_sem, True)

        basis_ref[k] = newest
        left_ref[k] = inverse
        upper_ref[k] = upper
        coeff_ref[k] = coeffs
        sigma_ref[...] = sigma
        shift_ref[k] = before[:, :LANES]

        applied = collect(par, False) - known
        fresh_u = dot_nn(left, applied, HIGHEST)
        u_ref[1 - par] = fresh_u

        @pl.when(k < ITERS - 2)
        def _():
            gather("grp", 1 - par, *col_side)

        inner_products(1 - par, applied)
        lr_ref[...] = fresh_u + sigma * residual
        return carry

    lax.fori_loop(0, ITERS - 1, step, 0)

    k = ITERS - 1
    par = ITERS % 2
    quarter = width // 4
    block_u, block_r = u_ref[par], stack[1]
    both = dot_nt(block_u, jnp.concatenate([block_r, block_u] * (LANES // (2 * width)), axis=0), HIGHEST)
    both = fold(both)
    odd = lax.rem(lax.div(lane[:quarter], 2 * width), 2) == 1
    late[grp * col_size + col] = jnp.where(odd, both[quarter:], both[:quarter])
    spread_all(late, late_sem)
    spread("grp", early_grp, early_grp_sem, False)
    early_col[col] = jnp.sum(early_grp[...], axis=0)
    spread("col", early_col, early_col_sem, True)
    proj_ref[...] = jnp.zeros_like(proj_ref)

    def keep_coeffs(k, left, coeffs, shift):
        found = dot_nn(left, coeffs, HIGHEST) + jnp.where(lane == row, shift, 0.0)
        for j in range(k):
            proj_ref[k, j] = found[:, (j + 2) * width : (j + 3) * width]
        proj_ref[k, k] = found[:, :width]

    for n in range(ITERS - 1):
        keep_coeffs(n, left_ref[n, :, :width], coeff_ref[n], shift_ref[n])
        factors_ref[n] = factor_of(upper_ref[n])
    spread("col", early_col, early_col_sem, False)
    total = unfold(jnp.sum(early_col[...], axis=0) / node_total)
    upper, inverse = factorize(total)
    left = inverse[:, :width]
    newest = dot_nn(left, block_r, HIGHEST)
    stack[0] = newest
    basis_ref[k] = newest
    factors_ref[k] = factor_of(upper)
    older = jnp.where((lane >= 2 * width) & (lane < 5 * width), total, 0.0)
    pad = jnp.concatenate([inverse, jnp.zeros((LANES - width, LANES), F32)], axis=0)[:, :width]
    await_all(late, late_sem)
    packed = jnp.sum(late[...], axis=0) / node_total
    total = jnp.concatenate(
        [packed] + [pltpu.roll(packed, LANES - n * 2 * width, 1) for n in range(1, 4)], axis=0
    )
    coeffs = dot_nt(total[:, :width], pad, HIGHEST) + older
    middle = jnp.zeros((width, LANES), F32)
    beside = jnp.concatenate([middle, coeffs] + [middle] * (LANES // width - 2), axis=0)
    gram = total - dot_nt(coeffs, beside, HIGHEST)
    rest = block_u - dot_nn(coeffs, stack[...].reshape(LANES, tile_size), HIGHEST)
    upper, inverse = factorize(gram)
    basis_ref[ITERS] = dot_nn(inverse[:, :width], rest, HIGHEST)
    factors_ref[ITERS] = dot_nt(left, upper[:, width : 2 * width], HIGHEST)
    keep_coeffs(k, left, coeffs, sigma_ref[:, :LANES])


def deliver(basis, proj, factors, basis_out, proj_out, factors_out, sem):
    pairs = ((basis, basis_out), (proj, proj_out), (factors, factors_out))
    copies = [pltpu.make_async_copy(source, target, sem.at[n]) for n, (source, target) in enumerate(pairs)]
    for copy in copies:
        copy.start()
    for copy in copies:
        copy.wait()


def solution(mesh):
    grp_size, col_size = mesh.shape["grp"], mesh.shape["col"]

    def body(start_block, tile_values, tile_row, tile_col, tile_count):
        width, shard_len = start_block.shape
        slots, tile_size = tile_values.shape[2], tile_values.shape[3]
        assert shard_len == tile_size and LANES // width == 8
        assert grp_size > 2 and col_size % CHUNK == 0
        assert grp_size & (grp_size - 1) == 0 and col_size & (col_size - 1) == 0
        places = LANES // width
        node_total = shard_len * grp_size * col_size
        spots = -(-max(grp_size * col_size, slots) // LANES) * LANES
        vmem = pl.BlockSpec(memory_space=pltpu.VMEM)
        smem = pl.BlockSpec(memory_space=pltpu.SMEM)
        hbm = pl.BlockSpec(memory_space=pl.ANY)
        block = (width, tile_size)
        line = (1, tile_size)
        tiles = (slots + 1, tile_size, tile_size)
        packed = (width // 2, LANES)
        small = (width, LANES)

        def sems(*sizes):
            return pltpu.SemaphoreType.DMA(sizes)

        def pinned(value):
            return pltpu.with_memory_space_constraint(value, pltpu.HBM)

        shapes = (
            jax.ShapeDtypeStruct((ITERS + 1,) + block, F32),
            jax.ShapeDtypeStruct((ITERS, ITERS, width, width), F32),
            jax.ShapeDtypeStruct((ITERS + 1, width, width), F32),
        )
        results = pl.pallas_call(
            functools.partial(kernel, grp_size, col_size, node_total),
            out_shape=shapes,
            in_specs=[hbm, hbm, hbm, hbm, smem],
            out_specs=(vmem, vmem, vmem),
            scratch_shapes=[
                pltpu.VMEM((slots, tile_size, tile_size), F32),
                pltpu.VMEM(tiles, F32),
                pltpu.VMEM(tiles, BF16),
                pltpu.VMEM(tiles, BF16),
                pltpu.VMEM(tiles, BF16),
                pltpu.VMEM(tiles, BF16),
                pltpu.VMEM((1, slots), I32),
                pltpu.VMEM((1, slots), I32),
                pltpu.VMEM((8, spots), I32),
                pltpu.SMEM((8, spots), I32),
                pltpu.VMEM((2,) + block, F32),
                pltpu.VMEM(block, F32),
                pltpu.VMEM((places,) + block, F32),
                pltpu.VMEM((places,) + block, F32),
                pltpu.VMEM((2, col_size) + block, F32),
                pltpu.VMEM((2, grp_size) + block, F32),
                pltpu.VMEM((3 * width, col_size * tile_size), BF16),
                pltpu.VMEM((3 * width, grp_size * tile_size), BF16),
                pltpu.VMEM((col_size,) + block, F32),
                pltpu.VMEM((grp_size,) + block, F32),
                pltpu.VMEM((2, col_size) + block, F32),
                pltpu.VMEM((2, grp_size) + block, F32),
                pltpu.VMEM((col_size,) + line, F32),
                pltpu.VMEM((grp_size,) + line, F32),
                pltpu.VMEM((col_size,) + line, F32),
                pltpu.VMEM((grp_size,) + line, F32),
                pltpu.VMEM(line, F32),
                pltpu.VMEM(block, F32),
                pltpu.VMEM((ITERS,) + small, F32),
                pltpu.VMEM((ITERS + 1,) + small, F32),
                pltpu.VMEM((ITERS,) + small, F32),
                pltpu.VMEM((ITERS,) + small, F32),
                pltpu.VMEM((2, col_size) + packed, F32),
                pltpu.VMEM((2, grp_size) + packed, F32),
                pltpu.VMEM((grp_size,) + packed, F32),
                pltpu.VMEM((col_size,) + packed, F32),
                pltpu.VMEM((grp_size * col_size, width // 4, LANES), F32),
                sems(8 if slots % 8 == 0 else slots),
                sems(4),
                sems(2, 4), sems(2, 3), sems(2, 2), sems(2, 2),
                sems(2), sems(2), sems(2, 2), sems(2, 2), sems(2), sems(2), sems(2),
            ],
            compiler_params=pltpu.CompilerParams(
                collective_id=0, has_side_effects=True, vmem_limit_bytes=40 * 1024 * 1024
            ),
        )(
            pinned(start_block),
            pinned(tile_values.reshape(slots, tile_size, tile_size)),
            pinned(tile_row.reshape(1, slots)),
            pinned(tile_col.reshape(1, slots)),
            tile_count.reshape(1),
        )
        return pl.pallas_call(
            deliver,
            out_shape=shapes,
            in_specs=[vmem] * 3,
            out_specs=[hbm] * 3,
            scratch_shapes=[sems(3)],
        )(*(pltpu.with_memory_space_constraint(value, pltpu.VMEM) for value in results))

    in_specs = (
        P(None, ("grp", "col")),
        P("grp", "col", None, None, None),
        P("grp", "col", None),
        P("grp", "col", None),
        P("grp", "col"),
    )
    out_specs = (P(None, None, ("grp", "col")), P(), P())
    return jax.shard_map(body, mesh=mesh, in_specs=in_specs, out_specs=out_specs, check_vma=False)
```

```python
import functools

import jax
import jax.numpy as jnp
from jax import lax
from jax.experimental import pallas as pl
from jax.experimental.pallas import tpu as pltpu
from jax.sharding import PartitionSpec as P

ITERS = 4
HIGHEST = lax.Precision.HIGHEST
MESH = pl.DeviceIdType.MESH
F32 = jnp.float32
BF16 = jnp.bfloat16
I32 = jnp.int32
LANES = 128
CHUNK = 8
STRIDE = 8
UNROLL = 4


def dot_nt(left, right, precision=None):
    dims = (((1,), (1,)), ((), ()))
    return lax.dot_general(left, right, dims, precision=precision, preferred_element_type=F32)


def dot_nn(left, right, precision=None):
    dims = (((1,), (0,)), ((), ()))
    return lax.dot_general(left, right, dims, precision=precision, preferred_element_type=F32)


def split_two(value):
    high = value.astype(BF16)
    low = (value - high.astype(F32)).astype(BF16)
    return high, low


def factorize(gram):
    width = gram.shape[0]
    shape = gram.shape
    row = lax.broadcasted_iota(I32, shape, 0)
    lane = lax.broadcasted_iota(I32, shape, 1)
    unit = jnp.where(lane == row, 1.0, 0.0).astype(F32)
    work = jnp.where((lane >= width) & (lane < 2 * width), gram, unit)
    diagonal = jnp.ones(shape, F32)
    for base in range(0, width, STRIDE):
        tall = [jnp.broadcast_to(work[:, width + base + i : width + base + i + 1], shape) for i in range(STRIDE)]
        wide = [jnp.broadcast_to(work[base + i : base + i + 1, :], shape) for i in range(STRIDE)]
        cell = {
            (m, i): jnp.broadcast_to(tall[i][base + m : base + m + 1, :], shape)
            for i in range(STRIDE)
            for m in range(i, STRIDE)
        }
        for i in range(STRIDE):
            inverse = 1.0 / cell[i, i]
            diagonal = jnp.where(row == base + i, cell[i, i], diagonal)
            scale = jnp.where(row > base + i, tall[i] * inverse, 0.0)
            work = work - scale * wide[i]
            for m in range(i + 1, STRIDE):
                ratio = cell[m, i] * inverse
                wide[m] = wide[m] - ratio * wide[i]
                tall[m] = tall[m] - scale * cell[m, i]
                for n in range(m, STRIDE):
                    cell[n, m] = cell[n, m] - ratio * cell[n, i]
    work = work / jnp.sqrt(diagonal)
    upper = jnp.where((lane < 2 * width) & (lane >= row + width), work, 0.0)
    inverse = jnp.where(lane <= row, work, 0.0)
    return upper, inverse


def factor_of(upper):
    width = upper.shape[0]
    return upper[:, width : 2 * width].T


def flip(index, distance, size):
    total, bit = 0, 1
    while bit < size:
        total = total + bit * lax.rem(lax.div(index, bit) + lax.div(distance, bit), 2)
        bit *= 2
    return total


def kernel(
    grp_size, col_size, node_total,
    start_ref, tiles_ref, row_ref, col_ref, count_ref,
    basis_ref, proj_ref, factors_ref,
    raw, merged, high, low, high_t, low_t, rows_v, cols_v, table_v, table,
    u_ref, lr_ref, stack, lstack, row_panel, col_panel, row_split, col_split,
    acc_row, acc_col, got_row, got_col, deg_row, deg_col, deg_got_row, deg_got_col,
    degree_ref, sigma_ref, shift_ref, left_ref, upper_ref, coeff_ref, red_col, red_grp, early_grp, early_col, late,
    tile_sem, in_sem, gather_row_sem, gather_col_sem, scatter_row_sem, scatter_col_sem,
    deg_row_sem, deg_col_sem, red_col_sem, red_grp_sem, early_grp_sem, early_col_sem, late_sem,
):
    grp = lax.axis_index("grp")
    col = lax.axis_index("col")
    slots, tile_size = raw.shape[0], raw.shape[1]
    width = u_ref.shape[1]
    small = (width, LANES)
    row = lax.broadcasted_iota(I32, small, 0)
    lane = lax.broadcasted_iota(I32, small, 1)

    def other(t):
        dg, dc = lax.div(t, col_size), lax.rem(t, col_size)
        return flip(grp, dg, grp_size), flip(col, dc, col_size)

    loads_of = tile_sem.shape[0]
    share = slots // loads_of

    def load_tile(n):
        at = pl.ds(n * share, share)
        return pltpu.make_async_copy(tiles_ref.at[at], raw.at[at], tile_sem.at[n])

    loads = (
        pltpu.make_async_copy(start_ref, u_ref.at[0], in_sem.at[0]),
        pltpu.make_async_copy(row_ref, rows_v, in_sem.at[1]),
        pltpu.make_async_copy(col_ref, cols_v, in_sem.at[2]),
    )
    for copy in loads:
        copy.start()

    def start_load(s, carry):
        load_tile(s).start()
        return carry

    lax.fori_loop(0, loads_of, start_load, 0)

    barrier = pltpu.get_barrier_semaphore()

    def greet(t, carry):
        pl.semaphore_signal(barrier, inc=1, device_id=other(t), device_id_type=MESH)
        return carry

    everyone = grp_size * col_size
    lax.fori_loop(1, everyone, greet, 0, unroll=everyone <= 32)

    def copy_to(axis, d, source, target, send_sem, recv_sem):
        size = col_size if axis == "col" else grp_size
        peer = flip(col if axis == "col" else grp, d, size)
        return pltpu.make_async_remote_copy(
            src_ref=source(peer),
            dst_ref=target,
            send_sem=send_sem,
            recv_sem=recv_sem,
            device_id=(grp, peer) if axis == "col" else (peer, col),
            device_id_type=MESH,
        )

    def send(axis, source, target, sems):
        size = col_size if axis == "col" else grp_size

        def visit(d, carry):
            copy_to(axis, size - d, source, target, sems.at[0], sems.at[1]).start()
            return carry

        lax.fori_loop(1, size, visit, 0, unroll=size <= 8)

    def bytes_of(part, send_sem, recv_sem):
        return pltpu.make_async_remote_copy(
            src_ref=part, dst_ref=part, send_sem=send_sem, recv_sem=recv_sem,
            device_id=other(1), device_id_type=MESH,
        )

    def await_all(buf, sems):
        bytes_of(buf.at[pl.ds(0, buf.shape[0] - 1)], sems.at[0], sems.at[1]).wait()

    col_groups = ((1, grp_size - 1), (grp_size - 1, grp_size))
    row_groups = ((1, 4), (4, 6), (6, col_size))

    def gather(axis, par, panel, sems, groups):
        me = col if axis == "col" else grp
        for n, (low_d, high_d) in enumerate(groups):

            def visit(i, carry):
                d = low_d + i
                target = panel.at[par, me]
                copy_to(axis, d, lambda peer: u_ref.at[par], target, sems.at[par, 0], sems.at[par, n + 1]).start()
                return carry

            lax.fori_loop(0, high_d - low_d, visit, 0, unroll=high_d - low_d <= 8)

    def arrive(par, panel, sems, groups, n):
        count = groups[n][1] - groups[n][0]
        bytes_of(panel.at[par, pl.ds(0, count)], sems.at[par, 0], sems.at[par, n + 1]).wait_recv()

    def leave(par, panel, sems):
        count = panel.shape[1] - 1
        bytes_of(panel.at[par, pl.ds(0, count)], sems.at[par, 0], sems.at[par, 1]).wait_send()

    col_side = (col_panel, gather_col_sem, col_groups)
    row_side = (row_panel, gather_row_sem, row_groups)

    def spread(axis, buf, sems, start):
        me = col if axis == "col" else grp
        if start:
            send(axis, lambda peer: buf.at[me], buf.at[me], sems)
        else:
            await_all(buf, sems)

    def spread_all(buf, sems):
        me = grp * col_size + col

        def visit(t, carry):
            pltpu.make_async_remote_copy(
                src_ref=buf.at[me], dst_ref=buf.at[me], send_sem=sems.at[0], recv_sem=sems.at[1],
                device_id=other(everyone - t), device_id_type=MESH,
            ).start()
            return carry

        lax.fori_loop(1, everyone, visit, 0, unroll=everyone <= 32)

    def position(r, q):
        return table[0, r * grp_size + q]

    def send_rows(par, r, d, with_degree):
        sems = scatter_row_sem.at[par]
        copy_to("col", d, lambda peer: acc_row.at[r], got_row.at[par, col], sems.at[0], sems.at[1]).start()
        if with_degree:
            sems = deg_row_sem
            copy_to("col", d, lambda peer: deg_row.at[r], deg_got_row.at[col], sems.at[0], sems.at[1]).start()

    def halves(panel, par, size, split):
        for place in range(size):
            first, second = split_two(panel[par, place])
            at = pl.ds(place * tile_size, tile_size)
            split[:width, at] = first
            split[width : 2 * width, at] = jnp.ones((width, tile_size), BF16)
            split[2 * width :, at] = second

    def combine(total, rest):
        piece = total[:width] + total[2 * width :] + rest[:width]
        return piece, total[width : width + 1] + rest[width : width + 1]

    def rows_of(r):
        places = [position(r, q) for q in range(grp_size)]
        left = col_split[...]
        firsts = jnp.concatenate([high_t[p] for p in places], axis=0)
        seconds = jnp.concatenate([low[p] for p in places], axis=1)
        return combine(dot_nn(left, firsts), dot_nt(left[: 2 * width], seconds))

    def cols_of(q):
        piece, degree = 0.0, 0.0
        for base in range(0, col_size, CHUNK):
            left = row_split[:, pl.ds(base * tile_size, CHUNK * tile_size)]
            places = [position(base + r, q) for r in range(CHUNK)]
            firsts = jnp.concatenate([high[p] for p in places], axis=0)
            seconds = jnp.concatenate([low[p] for p in places], axis=0)
            part, extra = combine(dot_nn(left, firsts), dot_nn(left[: 2 * width], seconds))
            piece = piece + part
            degree = degree + extra
        return piece, degree

    def first_rows():
        def visit(d):
            r = flip(col, d, col_size)
            piece, degree = rows_of(r)
            acc_row[r] = piece
            deg_row[r] = degree

        def go(ds):
            for d in ds:
                visit(d)
            for d in ds:
                if not isinstance(d, int) or d:
                    send_rows(0, flip(col, d, col_size), d, True)

        if col_size <= 8:
            go(range(col_size // 2, col_size))
            go(range(col_size // 2))
        else:
            def each(d, carry):
                go([d])
                return carry

            lax.fori_loop(1, col_size, each, 0)
            visit(0)
        got_row[0, col] = acc_row[col]
        deg_got_row[col] = deg_row[col]

    def first_cols():
        for d in range(grp_size - 1, -1, -1):
            q = flip(grp, d, grp_size)
            piece, degree = cols_of(q)
            acc_col[q] = piece
            deg_col[q] = degree
        send("grp", lambda peer: acc_col.at[peer], got_col.at[0, grp], scatter_col_sem.at[0])
        got_col[0, grp] = acc_col[grp]
        send("grp", lambda peer: deg_col.at[peer], deg_got_col.at[grp], deg_col_sem)
        deg_got_col[grp] = deg_col[grp]

    def stacked(pieces):
        pairs = [split_two(piece) for piece in pieces]
        return jnp.concatenate([jnp.concatenate(pair, axis=0) for pair in pairs], axis=1)

    def product(left, firsts, seconds):
        total = dot_nn(left, jnp.concatenate(firsts, axis=0))
        rest = dot_nn(left[:width], jnp.concatenate(seconds, axis=0))
        return total[:width] + total[width:] + rest

    def rows_batch(par, ds):
        places = [flip(grp, d, grp_size) for d in ds]
        left = stacked([u_ref[par] if d == 0 else col_panel[par, q] for d, q in zip(ds, places)])

        def visit(r, carry):
            at = [position(r, q) for q in places]
            piece = product(left, [high_t[p] for p in at], [low_t[p] for p in at])
            acc_row[r] = piece if ds[0] == 0 else acc_row[r] + piece
            return carry

        if col_size <= 8:
            for r in range(col_size):
                visit(r, 0)
        else:
            lax.fori_loop(0, col_size, visit, 0)

    def cols_batch(par, base, count):
        places = [flip(col, base + i, col_size) for i in range(count)]
        own = isinstance(base, int) and base == 0
        left = stacked([u_ref[par]] if own else [row_panel[par, r] for r in places])
        for q in range(grp_size):
            at = [position(r, q) for r in places]
            piece = product(left, [high[p] for p in at], [low[p] for p in at])
            acc_col[q] = piece if own else acc_col[q] + piece

    def collect(par, with_degree):
        leave(par, col_panel, gather_col_sem)
        leave(par, row_panel, gather_row_sem)
        await_all(got_row.at[par], scatter_row_sem.at[par])
        await_all(got_col.at[par], scatter_col_sem.at[par])
        if with_degree:
            await_all(deg_got_row, deg_row_sem)
            await_all(deg_got_col, deg_col_sem)
            degree_ref[...] = jnp.sum(deg_got_row[...], axis=0) + jnp.sum(deg_got_col[...], axis=0)
        total = jnp.sum(got_row[par], axis=0) + jnp.sum(got_col[par], axis=0)
        return degree_ref[...] * u_ref[par] - total

    stack[...] = jnp.zeros_like(stack)
    lstack[...] = jnp.zeros_like(lstack)
    loads[1].wait()
    loads[2].wait()
    spots = table.shape[1]
    offset = rows_v[...] - grp * col_size
    pick = lax.div(cols_v[...] - col, col_size)
    place = jnp.clip(offset, 0, col_size - 1) * grp_size + jnp.clip(pick, 0, grp_size - 1)
    square = (slots, slots)
    down = lax.broadcasted_iota(I32, square, 0)
    across = lax.broadcasted_iota(I32, square, 1)
    wide = jnp.broadcast_to(place, square)
    tall = jnp.sum(jnp.where(down == across, wide, 0), axis=1, keepdims=True)
    same = (wide == jnp.broadcast_to(tall, square)) & (down < across)
    before = jnp.max(jnp.where(same, down, -1), axis=0, keepdims=True)
    before = jnp.where(before < 0, slots, before)
    long = (slots, spots)
    depth = lax.broadcasted_iota(I32, long, 0)
    spot = lax.broadcasted_iota(I32, long, 1)
    here = (jnp.broadcast_to(tall, long) == spot) & (depth < count_ref[0])
    last = jnp.max(jnp.where(here, depth, -1), axis=0, keepdims=True)
    table_v[0:1, :] = jnp.where(last < 0, slots, last)
    table_v[1:2, :slots] = before
    move = pltpu.make_async_copy(table_v, table, in_sem.at[3])
    move.start()
    empty = jnp.zeros((tile_size, tile_size), F32)
    merged[slots] = empty
    high[slots] = empty.astype(BF16)
    low[slots] = empty.astype(BF16)
    high_t[slots] = empty.astype(BF16)
    low_t[slots] = empty.astype(BF16)
    loads[0].wait()
    start = u_ref[0]
    stack[0] = start
    stack[1] = start
    row_panel[0, col] = start
    col_panel[0, grp] = start
    pl.semaphore_wait(barrier, everyone - 1)
    gather("grp", 0, *col_side)
    gather("col", 0, *row_side)
    move.wait()

    def merge(n, carry):
        load_tile(n).wait()

        def visit(m, carry):
            s = n * share + m
            value = raw[s] + merged[table[1, s]]
            merged[s] = value
            first, second = split_two(value)
            high[s] = first
            high_t[s] = first.T
            low[s] = second
            return carry

        return lax.fori_loop(0, share, visit, carry, unroll=UNROLL)

    lax.fori_loop(0, loads_of, merge, 0)

    for n in range(len(col_groups)):
        arrive(0, *col_side, n)
    halves(col_panel, 0, grp_size, col_split)
    first_rows()
    for n in range(len(row_groups)):
        arrive(0, *row_side, n)
    halves(row_panel, 0, col_size, row_split)
    first_cols()

    def turn(s, carry):
        low_t[s] = low[s].T
        return carry

    lax.fori_loop(0, slots, turn, 0, unroll=4)
    applied = collect(0, True)
    lr_ref[...] = applied
    u_ref[1] = applied
    sigma_ref[...] = jnp.zeros_like(sigma_ref)
    left_ref[ITERS] = jnp.where(lane == row, 1.0, 0.0)

    half = width // 2

    def fold(value):
        return jnp.where(lane[:half] < LANES // 2, value[:half], value[half:])

    def unfold(packed):
        turned = pltpu.roll(packed, LANES // 2, 1)
        low_lanes = lane[:half] < LANES // 2
        return jnp.concatenate(
            [jnp.where(low_lanes, packed, turned), jnp.where(low_lanes, turned, packed)], axis=0
        )

    def inner_products(par, block_v):
        block = stack[0:4].reshape(4 * width, tile_size)
        block = jnp.concatenate([block, block], axis=0)
        both = dot_nt(jnp.concatenate([block_v, stack[1]], axis=0), block, HIGHEST)
        inner = lax.rem(lane, 4 * width)
        red_grp[par, grp] = fold(jnp.where((inner >= width) & (inner < 2 * width), both[width:], both[:width]))

    gather("grp", 1, *col_side)
    gather("col", 1, *row_side)
    inner_products(1, applied)

    def step(k, carry):
        par = lax.rem(k + 1, 2)
        block_u, block_r = u_ref[par], stack[1]
        spread("grp", red_grp.at[par], red_grp_sem.at[par], True)

        rows_batch(par, [0])
        cols_batch(par, 0, 1)
        arrive(par, *col_side, 0)
        rows_batch(par, list(range(1, grp_size - 1)))
        spread("grp", red_grp.at[par], red_grp_sem.at[par], False)
        red_col[par, col] = jnp.sum(red_grp[par], axis=0)
        spread("col", red_col.at[par], red_col_sem.at[par], True)
        arrive(par, *col_side, 1)
        rows_batch(par, [grp_size - 1])
        send("col", lambda peer: acc_row.at[peer], got_row.at[par, col], scatter_row_sem.at[par])
        got_row[par, col] = acc_row[col]
        arrive(par, *row_side, 0)
        cols_batch(par, 1, 3)
        arrive(par, *row_side, 1)
        cols_batch(par, 4, 2)
        arrive(par, *row_side, 2)
        cols_batch(par, 6, 2)

        def visit(n, carry):
            cols_batch(par, 4 * n, 4)
            return carry

        if col_size > 8:
            lax.fori_loop(2, col_size // 4, visit, 0)
        send("grp", lambda peer: acc_col.at[peer], got_col.at[par, grp], scatter_col_sem.at[par])
        got_col[par, grp] = acc_col[grp]

        spread("col", red_col.at[par], red_col_sem.at[par], False)
        total = unfold(jnp.sum(red_col[par], axis=0) / node_total)
        former = left_ref[lax.rem(k + ITERS, ITERS + 1)]
        turned = dot_nn(former[:, :width], total, HIGHEST)
        upper, inverse = factorize(total)
        left = inverse[:, :width]
        fresh = dot_nn(left, jnp.concatenate([block_r, lr_ref[...]], axis=1), HIGHEST)
        newest, image = fresh[:, :tile_size], fresh[:, tile_size:]
        pad = jnp.concatenate([inverse, jnp.zeros((LANES - width, LANES), F32)], axis=0)
        mixed = dot_nt(turned[:, :width], pad[:, :width], HIGHEST)
        older = (lane >= 2 * width) & (lane < 4 * width)
        coeffs = jnp.where(lane < width, mixed, jnp.where(older, turned, 0.0))
        stack[0] = newest
        lstack[0] = image
        now = dot_nn(coeffs, jnp.concatenate([stack[...].reshape(LANES, tile_size),
                                              lstack[...].reshape(LANES, tile_size)], axis=1), HIGHEST)
        rest = block_u - now[:, :tile_size]
        residual = dot_nn(left, rest, HIGHEST)
        on_block = jnp.sum(jnp.where(lane == row, turned, 0.0), axis=1, keepdims=True)
        on_gram = jnp.sum(jnp.where(lane == row + width, total, 0.0), axis=1, keepdims=True)
        mean = jnp.sum(on_block, axis=0, keepdims=True) / jnp.sum(on_gram, axis=0, keepdims=True)
        before = sigma_ref[...]
        sigma = before + jnp.broadcast_to(mean, sigma_ref.shape)
        known = now[:, tile_size:] + sigma * rest
        stack[0] = residual
        stack[1] = residual
        stack[k + 2] = newest
        lstack[k + 2] = image

        @pl.when(k == ITERS - 2)
        def _():
            shifted = [lstack[j] - sigma * stack[j] for j in (4, 2, 3)]
            block = jnp.concatenate([shifted[0], residual, shifted[1], shifted[2]] * 2, axis=0)
            early_grp[grp] = fold(dot_nt(residual, block, HIGHEST))
            spread("grp", early_grp, early_grp_sem, True)

        basis_ref[k] = newest
        left_ref[k] = inverse
        upper_ref[k] = upper
        coeff_ref[k] = coeffs
        sigma_ref[...] = sigma
        shift_ref[k] = before[:, :LANES]

        applied = collect(par, False) - known
        fresh_u = dot_nn(left, applied, HIGHEST)
        u_ref[1 - par] = fresh_u

        @pl.when(k < ITERS - 2)
        def _():
            gather("grp", 1 - par, *col_side)
            gather("col", 1 - par, *row_side)

        inner_products(1 - par, applied)
        lr_ref[...] = fresh_u + sigma * residual
        return carry

    lax.fori_loop(0, ITERS - 1, step, 0)

    k = ITERS - 1
    par = ITERS % 2
    quarter = width // 4
    block_u, block_r = u_ref[par], stack[1]
    both = dot_nt(block_u, jnp.concatenate([block_r, block_u] * (LANES // (2 * width)), axis=0), HIGHEST)
    both = fold(both)
    odd = lax.rem(lax.div(lane[:quarter], 2 * width), 2) == 1
    late[grp * col_size + col] = jnp.where(odd, both[quarter:], both[:quarter])
    spread_all(late, late_sem)
    spread("grp", early_grp, early_grp_sem, False)
    early_col[col] = jnp.sum(early_grp[...], axis=0)
    spread("col", early_col, early_col_sem, True)
    proj_ref[...] = jnp.zeros_like(proj_ref)

    def keep_coeffs(k, left, coeffs, shift):
        found = dot_nn(left, coeffs, HIGHEST) + jnp.where(lane == row, shift, 0.0)
        for j in range(k):
            proj_ref[k, j] = found[:, (j + 2) * width : (j + 3) * width]
        proj_ref[k, k] = found[:, :width]

    for n in range(ITERS - 1):
        keep_coeffs(n, left_ref[n, :, :width], coeff_ref[n], shift_ref[n])
        factors_ref[n] = factor_of(upper_ref[n])
    spread("col", early_col, early_col_sem, False)
    total = unfold(jnp.sum(early_col[...], axis=0) / node_total)
    upper, inverse = factorize(total)
    left = inverse[:, :width]
    newest = dot_nn(left, block_r, HIGHEST)
    stack[0] = newest
    basis_ref[k] = newest
    factors_ref[k] = factor_of(upper)
    older = jnp.where((lane >= 2 * width) & (lane < 5 * width), total, 0.0)
    pad = jnp.concatenate([inverse, jnp.zeros((LANES - width, LANES), F32)], axis=0)[:, :width]
    await_all(late, late_sem)
    packed = jnp.sum(late[...], axis=0) / node_total
    total = jnp.concatenate(
        [packed] + [pltpu.roll(packed, LANES - n * 2 * width, 1) for n in range(1, 4)], axis=0
    )
    coeffs = dot_nt(total[:, :width], pad, HIGHEST) + older
    middle = jnp.zeros((width, LANES), F32)
    beside = jnp.concatenate([middle, coeffs] + [middle] * (LANES // width - 2), axis=0)
    gram = total - dot_nt(coeffs, beside, HIGHEST)
    rest = block_u - dot_nn(coeffs, stack[...].reshape(LANES, tile_size), HIGHEST)
    upper, inverse = factorize(gram)
    basis_ref[ITERS] = dot_nn(inverse[:, :width], rest, HIGHEST)
    factors_ref[ITERS] = dot_nt(left, upper[:, width : 2 * width], HIGHEST)
    keep_coeffs(k, left, coeffs, sigma_ref[:, :LANES])


def deliver(basis, proj, factors, basis_out, proj_out, factors_out, sem):
    pairs = ((basis, basis_out), (proj, proj_out), (factors, factors_out))
    copies = [pltpu.make_async_copy(source, target, sem.at[n]) for n, (source, target) in enumerate(pairs)]
    for copy in copies:
        copy.start()
    for copy in copies:
        copy.wait()


def solution(mesh):
    grp_size, col_size = mesh.shape["grp"], mesh.shape["col"]

    def body(start_block, tile_values, tile_row, tile_col, tile_count):
        width, shard_len = start_block.shape
        slots, tile_size = tile_values.shape[2], tile_values.shape[3]
        assert shard_len == tile_size and LANES // width == 8
        assert grp_size > 2 and col_size % CHUNK == 0
        assert grp_size & (grp_size - 1) == 0 and col_size & (col_size - 1) == 0
        places = LANES // width
        node_total = shard_len * grp_size * col_size
        spots = -(-max(grp_size * col_size, slots) // LANES) * LANES
        vmem = pl.BlockSpec(memory_space=pltpu.VMEM)
        smem = pl.BlockSpec(memory_space=pltpu.SMEM)
        hbm = pl.BlockSpec(memory_space=pl.ANY)
        block = (width, tile_size)
        line = (1, tile_size)
        tiles = (slots + 1, tile_size, tile_size)
        packed = (width // 2, LANES)
        small = (width, LANES)

        def sems(*sizes):
            return pltpu.SemaphoreType.DMA(sizes)

        def pinned(value):
            return pltpu.with_memory_space_constraint(value, pltpu.HBM)

        shapes = (
            jax.ShapeDtypeStruct((ITERS + 1,) + block, F32),
            jax.ShapeDtypeStruct((ITERS, ITERS, width, width), F32),
            jax.ShapeDtypeStruct((ITERS + 1, width, width), F32),
        )
        results = pl.pallas_call(
            functools.partial(kernel, grp_size, col_size, node_total),
            out_shape=shapes,
            in_specs=[hbm, hbm, hbm, hbm, smem],
            out_specs=(vmem, vmem, vmem),
            scratch_shapes=[
                pltpu.VMEM((slots, tile_size, tile_size), F32),
                pltpu.VMEM(tiles, F32),
                pltpu.VMEM(tiles, BF16),
                pltpu.VMEM(tiles, BF16),
                pltpu.VMEM(tiles, BF16),
                pltpu.VMEM(tiles, BF16),
                pltpu.VMEM((1, slots), I32),
                pltpu.VMEM((1, slots), I32),
                pltpu.VMEM((8, spots), I32),
                pltpu.SMEM((8, spots), I32),
                pltpu.VMEM((2,) + block, F32),
                pltpu.VMEM(block, F32),
                pltpu.VMEM((places,) + block, F32),
                pltpu.VMEM((places,) + block, F32),
                pltpu.VMEM((2, col_size) + block, F32),
                pltpu.VMEM((2, grp_size) + block, F32),
                pltpu.VMEM((3 * width, col_size * tile_size), BF16),
                pltpu.VMEM((3 * width, grp_size * tile_size), BF16),
                pltpu.VMEM((col_size,) + block, F32),
                pltpu.VMEM((grp_size,) + block, F32),
                pltpu.VMEM((2, col_size) + block, F32),
                pltpu.VMEM((2, grp_size) + block, F32),
                pltpu.VMEM((col_size,) + line, F32),
                pltpu.VMEM((grp_size,) + line, F32),
                pltpu.VMEM((col_size,) + line, F32),
                pltpu.VMEM((grp_size,) + line, F32),
                pltpu.VMEM(line, F32),
                pltpu.VMEM(block, F32),
                pltpu.VMEM((ITERS,) + small, F32),
                pltpu.VMEM((ITERS + 1,) + small, F32),
                pltpu.VMEM((ITERS,) + small, F32),
                pltpu.VMEM((ITERS,) + small, F32),
                pltpu.VMEM((2, col_size) + packed, F32),
                pltpu.VMEM((2, grp_size) + packed, F32),
                pltpu.VMEM((grp_size,) + packed, F32),
                pltpu.VMEM((col_size,) + packed, F32),
                pltpu.VMEM((grp_size * col_size, width // 4, LANES), F32),
                sems(8 if slots % 8 == 0 else slots),
                sems(4),
                sems(2, 4), sems(2, 3), sems(2, 2), sems(2, 2),
                sems(2), sems(2), sems(2, 2), sems(2, 2), sems(2), sems(2), sems(2),
            ],
            compiler_params=pltpu.CompilerParams(
                collective_id=0, has_side_effects=True, vmem_limit_bytes=40 * 1024 * 1024
            ),
        )(
            pinned(start_block),
            pinned(tile_values.reshape(slots, tile_size, tile_size)),
            pinned(tile_row.reshape(1, slots)),
            pinned(tile_col.reshape(1, slots)),
            tile_count.reshape(1),
        )
        return pl.pallas_call(
            deliver,
            out_shape=shapes,
            in_specs=[vmem] * 3,
            out_specs=[hbm] * 3,
            scratch_shapes=[sems(3)],
        )(*(pltpu.with_memory_space_constraint(value, pltpu.VMEM) for value in results))

    in_specs = (
        P(None, ("grp", "col")),
        P("grp", "col", None, None, None),
        P("grp", "col", None),
        P("grp", "col", None),
        P("grp", "col"),
    )
    out_specs = (P(None, None, ("grp", "col")), P(), P())
    return jax.shard_map(body, mesh=mesh, in_specs=in_specs, out_specs=out_specs, check_vma=False)
```

```python
import functools

import jax
import jax.numpy as jnp
from jax import lax
from jax.experimental import pallas as pl
from jax.experimental.pallas import tpu as pltpu
from jax.sharding import PartitionSpec as P

ITERS = 4
HIGHEST = lax.Precision.HIGHEST
MESH = pl.DeviceIdType.MESH
F32 = jnp.float32
BF16 = jnp.bfloat16
I32 = jnp.int32
LANES = 128
CHUNK = 8
STRIDE = 8
UNROLL = 4


def dot_nt(left, right, precision=None):
    dims = (((1,), (1,)), ((), ()))
    return lax.dot_general(left, right, dims, precision=precision, preferred_element_type=F32)


def dot_nn(left, right, precision=None):
    dims = (((1,), (0,)), ((), ()))
    return lax.dot_general(left, right, dims, precision=precision, preferred_element_type=F32)


def split_two(value):
    high = value.astype(BF16)
    low = (value - high.astype(F32)).astype(BF16)
    return high, low


def factorize(gram):
    width = gram.shape[0]
    shape = gram.shape
    row = lax.broadcasted_iota(I32, shape, 0)
    lane = lax.broadcasted_iota(I32, shape, 1)
    unit = jnp.where(lane == row, 1.0, 0.0).astype(F32)
    work = jnp.where((lane >= width) & (lane < 2 * width), gram, unit)
    diagonal = jnp.ones(shape, F32)
    for base in range(0, width, STRIDE):
        tall = [jnp.broadcast_to(work[:, width + base + i : width + base + i + 1], shape) for i in range(STRIDE)]
        wide = [jnp.broadcast_to(work[base + i : base + i + 1, :], shape) for i in range(STRIDE)]
        cell = {
            (m, i): jnp.broadcast_to(tall[i][base + m : base + m + 1, :], shape)
            for i in range(STRIDE)
            for m in range(i, STRIDE)
        }
        for i in range(STRIDE):
            inverse = 1.0 / cell[i, i]
            diagonal = jnp.where(row == base + i, cell[i, i], diagonal)
            scale = jnp.where(row > base + i, tall[i] * inverse, 0.0)
            work = work - scale * wide[i]
            for m in range(i + 1, STRIDE):
                ratio = cell[m, i] * inverse
                wide[m] = wide[m] - ratio * wide[i]
                tall[m] = tall[m] - scale * cell[m, i]
                for n in range(m, STRIDE):
                    cell[n, m] = cell[n, m] - ratio * cell[n, i]
    work = work / jnp.sqrt(diagonal)
    upper = jnp.where((lane < 2 * width) & (lane >= row + width), work, 0.0)
    inverse = jnp.where(lane <= row, work, 0.0)
    return upper, inverse


def factor_of(upper):
    width = upper.shape[0]
    return upper[:, width : 2 * width].T


def flip(index, distance, size):
    total, bit = 0, 1
    while bit < size:
        total = total + bit * lax.rem(lax.div(index, bit) + lax.div(distance, bit), 2)
        bit *= 2
    return total


def kernel(
    grp_size, col_size, node_total,
    start_ref, tiles_ref, row_ref, col_ref, count_ref,
    basis_ref, proj_ref, factors_ref,
    raw, merged, high, low, high_t, low_t, rows_v, cols_v, table_v, table,
    u_ref, lr_ref, stack, lstack, row_panel, col_panel,
    acc_row, acc_col, got_row, got_col, deg_row, deg_col, deg_got_row, deg_got_col,
    degree_ref, sigma_ref, shift_ref, left_ref, upper_ref, coeff_ref, red_col, red_grp, early_grp, early_col, late,
    tile_sem, in_sem, gather_row_sem, gather_col_sem, scatter_row_sem, scatter_col_sem,
    deg_row_sem, deg_col_sem, red_col_sem, red_grp_sem, early_grp_sem, early_col_sem, late_sem,
):
    grp = lax.axis_index("grp")
    col = lax.axis_index("col")
    slots, tile_size = raw.shape[0], raw.shape[1]
    width = u_ref.shape[1]
    small = (width, LANES)
    row = lax.broadcasted_iota(I32, small, 0)
    lane = lax.broadcasted_iota(I32, small, 1)

    def other(t):
        dg, dc = lax.div(t, col_size), lax.rem(t, col_size)
        return flip(grp, dg, grp_size), flip(col, dc, col_size)

    loads_of = tile_sem.shape[0]
    share = slots // loads_of

    def load_tile(n):
        at = pl.ds(n * share, share)
        return pltpu.make_async_copy(tiles_ref.at[at], raw.at[at], tile_sem.at[n])

    loads = (
        pltpu.make_async_copy(start_ref, u_ref.at[0], in_sem.at[0]),
        pltpu.make_async_copy(row_ref, rows_v, in_sem.at[1]),
        pltpu.make_async_copy(col_ref, cols_v, in_sem.at[2]),
    )
    for copy in loads:
        copy.start()

    def start_load(s, carry):
        load_tile(s).start()
        return carry

    lax.fori_loop(0, loads_of, start_load, 0)

    barrier = pltpu.get_barrier_semaphore()

    def greet(t, carry):
        pl.semaphore_signal(barrier, inc=1, device_id=other(t), device_id_type=MESH)
        return carry

    everyone = grp_size * col_size
    lax.fori_loop(1, everyone, greet, 0, unroll=everyone <= 32)

    def copy_to(axis, d, source, target, send_sem, recv_sem):
        size = col_size if axis == "col" else grp_size
        peer = flip(col if axis == "col" else grp, d, size)
        return pltpu.make_async_remote_copy(
            src_ref=source(peer),
            dst_ref=target,
            send_sem=send_sem,
            recv_sem=recv_sem,
            device_id=(grp, peer) if axis == "col" else (peer, col),
            device_id_type=MESH,
        )

    def send(axis, source, target, sems):
        size = col_size if axis == "col" else grp_size

        def visit(d, carry):
            copy_to(axis, size - d, source, target, sems.at[0], sems.at[1]).start()
            return carry

        lax.fori_loop(1, size, visit, 0, unroll=size <= 8)

    def bytes_of(part, send_sem, recv_sem):
        return pltpu.make_async_remote_copy(
            src_ref=part, dst_ref=part, send_sem=send_sem, recv_sem=recv_sem,
            device_id=other(1), device_id_type=MESH,
        )

    def await_all(buf, sems):
        bytes_of(buf.at[pl.ds(0, buf.shape[0] - 1)], sems.at[0], sems.at[1]).wait()

    col_groups = ((1, grp_size - 1), (grp_size - 1, grp_size))
    row_groups = ((1, 4), (4, 6), (6, col_size))

    def gather(axis, par, panel, sems, groups):
        me = col if axis == "col" else grp
        for n, (low_d, high_d) in enumerate(groups):

            def visit(i, carry):
                d = low_d + i
                target = panel.at[par, me]
                copy_to(axis, d, lambda peer: u_ref.at[par], target, sems.at[par, 0], sems.at[par, n + 1]).start()
                return carry

            lax.fori_loop(0, high_d - low_d, visit, 0, unroll=high_d - low_d <= 8)

    def arrive(par, panel, sems, groups, n):
        count = groups[n][1] - groups[n][0]
        bytes_of(panel.at[par, pl.ds(0, count)], sems.at[par, 0], sems.at[par, n + 1]).wait_recv()

    def leave(par, panel, sems):
        count = panel.shape[1] - 1
        bytes_of(panel.at[par, pl.ds(0, count)], sems.at[par, 0], sems.at[par, 1]).wait_send()

    col_side = (col_panel, gather_col_sem, col_groups)
    row_side = (row_panel, gather_row_sem, row_groups)

    def spread(axis, buf, sems, start):
        me = col if axis == "col" else grp
        if start:
            send(axis, lambda peer: buf.at[me], buf.at[me], sems)
        else:
            await_all(buf, sems)

    def spread_all(buf, sems):
        me = grp * col_size + col

        def visit(t, carry):
            pltpu.make_async_remote_copy(
                src_ref=buf.at[me], dst_ref=buf.at[me], send_sem=sems.at[0], recv_sem=sems.at[1],
                device_id=other(everyone - t), device_id_type=MESH,
            ).start()
            return carry

        lax.fori_loop(1, everyone, visit, 0, unroll=everyone <= 32)

    def position(r, q):
        return table[0, r * grp_size + q]

    def send_rows(par, r, d, with_degree):
        sems = scatter_row_sem.at[par]
        copy_to("col", d, lambda peer: acc_row.at[r], got_row.at[par, col], sems.at[0], sems.at[1]).start()
        if with_degree:
            sems = deg_row_sem
            copy_to("col", d, lambda peer: deg_row.at[r], deg_got_row.at[col], sems.at[0], sems.at[1]).start()

    def combine(total, rest):
        piece = total[:width] + total[2 * width :] + rest[:width]
        return piece, total[width : width + 1] + rest[width : width + 1]

    def with_ones(pieces):
        ones = jnp.ones((width, tile_size), BF16)
        parts = [split_two(piece) for piece in pieces]
        return jnp.concatenate([jnp.concatenate([a, ones, b], axis=0) for a, b in parts], axis=1)

    def rows_of(r, left, places):
        at = [position(r, q) for q in places]
        firsts = jnp.concatenate([high_t[p] for p in at], axis=0)
        seconds = jnp.concatenate([low[p] for p in at], axis=1)
        return combine(dot_nn(left, firsts), dot_nt(left[: 2 * width], seconds))

    def cols_of(q, left, places):
        at = [position(r, q) for r in places]
        firsts = jnp.concatenate([high[p] for p in at], axis=0)
        seconds = jnp.concatenate([low[p] for p in at], axis=0)
        return combine(dot_nn(left, firsts), dot_nn(left[: 2 * width], seconds))

    def first_own():
        left = with_ones([u_ref[0]])

        def visit(r, carry):
            acc_row[r], deg_row[r] = rows_of(r, left, [grp])
            return carry

        lax.fori_loop(0, col_size, visit, 0, unroll=min(col_size, 8))
        for q in range(grp_size):
            acc_col[q], deg_col[q] = cols_of(q, left, [col])

    def first_rows():
        places = [flip(grp, d, grp_size) for d in range(1, grp_size)]
        left = with_ones([col_panel[0, q] for q in places])

        def visit(d):
            r = flip(col, d, col_size)
            piece, degree = rows_of(r, left, places)
            acc_row[r] = acc_row[r] + piece
            deg_row[r] = deg_row[r] + degree

        def go(ds):
            for d in ds:
                visit(d)
            for d in ds:
                if not isinstance(d, int) or d:
                    send_rows(0, flip(col, d, col_size), d, True)

        if col_size <= 8:
            go(range(col_size // 2, col_size))
            go(range(col_size // 2))
        else:
            def each(d, carry):
                go([d])
                return carry

            lax.fori_loop(1, col_size, each, 0)
            visit(0)
        got_row[0, col] = acc_row[col]
        deg_got_row[col] = deg_row[col]

    def first_cols():
        def batch(places):
            left = with_ones([row_panel[0, r] for r in places])
            for q in range(grp_size):
                piece, degree = cols_of(q, left, places)
                acc_col[q] = acc_col[q] + piece
                deg_col[q] = deg_col[q] + degree

        def visit(n, carry):
            batch([flip(col, n * CHUNK + i, col_size) for i in range(CHUNK)])
            return carry

        batch([flip(col, i, col_size) for i in range(1, CHUNK)])
        if col_size > CHUNK:
            lax.fori_loop(1, col_size // CHUNK, visit, 0)
        send("grp", lambda peer: acc_col.at[peer], got_col.at[0, grp], scatter_col_sem.at[0])
        got_col[0, grp] = acc_col[grp]
        send("grp", lambda peer: deg_col.at[peer], deg_got_col.at[grp], deg_col_sem)
        deg_got_col[grp] = deg_col[grp]

    def stacked(pieces):
        pairs = [split_two(piece) for piece in pieces]
        return jnp.concatenate([jnp.concatenate(pair, axis=0) for pair in pairs], axis=1)

    def product(left, firsts, seconds):
        total = dot_nn(left, jnp.concatenate(firsts, axis=0))
        rest = dot_nn(left[:width], jnp.concatenate(seconds, axis=0))
        return total[:width] + total[width:] + rest

    def rows_batch(par, ds):
        places = [flip(grp, d, grp_size) for d in ds]
        left = stacked([u_ref[par] if d == 0 else col_panel[par, q] for d, q in zip(ds, places)])

        def visit(r, carry):
            at = [position(r, q) for q in places]
            piece = product(left, [high_t[p] for p in at], [low_t[p] for p in at])
            acc_row[r] = piece if ds[0] == 0 else acc_row[r] + piece
            return carry

        if col_size <= 8:
            for r in range(col_size):
                visit(r, 0)
        else:
            lax.fori_loop(0, col_size, visit, 0)

    def cols_batch(par, base, count):
        places = [flip(col, base + i, col_size) for i in range(count)]
        own = isinstance(base, int) and base == 0
        left = stacked([u_ref[par]] if own else [row_panel[par, r] for r in places])
        for q in range(grp_size):
            at = [position(r, q) for r in places]
            piece = product(left, [high[p] for p in at], [low[p] for p in at])
            acc_col[q] = piece if own else acc_col[q] + piece

    def collect(par, with_degree):
        leave(par, col_panel, gather_col_sem)
        leave(par, row_panel, gather_row_sem)
        await_all(got_row.at[par], scatter_row_sem.at[par])
        await_all(got_col.at[par], scatter_col_sem.at[par])
        if with_degree:
            await_all(deg_got_row, deg_row_sem)
            await_all(deg_got_col, deg_col_sem)
            degree_ref[...] = jnp.sum(deg_got_row[...], axis=0) + jnp.sum(deg_got_col[...], axis=0)
        total = jnp.sum(got_row[par], axis=0) + jnp.sum(got_col[par], axis=0)
        return degree_ref[...] * u_ref[par] - total

    stack[...] = jnp.zeros_like(stack)
    lstack[...] = jnp.zeros_like(lstack)
    loads[1].wait()
    loads[2].wait()
    spots = table.shape[1]
    offset = rows_v[...] - grp * col_size
    pick = lax.div(cols_v[...] - col, col_size)
    place = jnp.clip(offset, 0, col_size - 1) * grp_size + jnp.clip(pick, 0, grp_size - 1)
    square = (slots, slots)
    down = lax.broadcasted_iota(I32, square, 0)
    across = lax.broadcasted_iota(I32, square, 1)
    wide = jnp.broadcast_to(place, square)
    tall = jnp.sum(jnp.where(down == across, wide, 0), axis=1, keepdims=True)
    same = (wide == jnp.broadcast_to(tall, square)) & (down < across)
    before = jnp.max(jnp.where(same, down, -1), axis=0, keepdims=True)
    before = jnp.where(before < 0, slots, before)
    long = (slots, spots)
    depth = lax.broadcasted_iota(I32, long, 0)
    spot = lax.broadcasted_iota(I32, long, 1)
    here = (jnp.broadcast_to(tall, long) == spot) & (depth < count_ref[0])
    last = jnp.max(jnp.where(here, depth, -1), axis=0, keepdims=True)
    table_v[0:1, :] = jnp.where(last < 0, slots, last)
    table_v[1:2, :slots] = before
    move = pltpu.make_async_copy(table_v, table, in_sem.at[3])
    move.start()
    empty = jnp.zeros((tile_size, tile_size), F32)
    merged[slots] = empty
    high[slots] = empty.astype(BF16)
    low[slots] = empty.astype(BF16)
    high_t[slots] = empty.astype(BF16)
    low_t[slots] = empty.astype(BF16)
    loads[0].wait()
    start = u_ref[0]
    stack[0] = start
    stack[1] = start
    pl.semaphore_wait(barrier, everyone - 1)
    gather("grp", 0, *col_side)
    gather("col", 0, *row_side)
    move.wait()

    def merge(n, carry):
        load_tile(n).wait()

        def visit(m, carry):
            s = n * share + m
            value = raw[s] + merged[table[1, s]]
            merged[s] = value
            first, second = split_two(value)
            high[s] = first
            high_t[s] = first.T
            low[s] = second
            return carry

        return lax.fori_loop(0, share, visit, carry, unroll=UNROLL)

    lax.fori_loop(0, loads_of, merge, 0)

    first_own()
    for n in range(len(col_groups)):
        arrive(0, *col_side, n)
    first_rows()
    for n in range(len(row_groups)):
        arrive(0, *row_side, n)
    first_cols()

    def turn(s, carry):
        low_t[s] = low[s].T
        return carry

    lax.fori_loop(0, slots, turn, 0, unroll=4)
    applied = collect(0, True)
    lr_ref[...] = applied
    u_ref[1] = applied
    sigma_ref[...] = jnp.zeros_like(sigma_ref)
    left_ref[ITERS] = jnp.where(lane == row, 1.0, 0.0)

    half = width // 2

    def fold(value):
        return jnp.where(lane[:half] < LANES // 2, value[:half], value[half:])

    def unfold(packed):
        turned = pltpu.roll(packed, LANES // 2, 1)
        low_lanes = lane[:half] < LANES // 2
        return jnp.concatenate(
            [jnp.where(low_lanes, packed, turned), jnp.where(low_lanes, turned, packed)], axis=0
        )

    def inner_products(par, block_v):
        block = stack[0:4].reshape(4 * width, tile_size)
        block = jnp.concatenate([block, block], axis=0)
        both = dot_nt(jnp.concatenate([block_v, stack[1]], axis=0), block, HIGHEST)
        inner = lax.rem(lane, 4 * width)
        red_grp[par, grp] = fold(jnp.where((inner >= width) & (inner < 2 * width), both[width:], both[:width]))

    def depart(par):
        spread("grp", red_grp.at[par], red_grp_sem.at[par], True)
        gather("grp", par, *col_side)
        gather("col", par, *row_side)

    inner_products(1, applied)
    depart(1)

    def step(k, carry):
        par = lax.rem(k + 1, 2)
        block_u, block_r = u_ref[par], stack[1]
        rows_batch(par, [0])
        cols_batch(par, 0, 1)
        arrive(par, *col_side, 0)
        spread("grp", red_grp.at[par], red_grp_sem.at[par], False)
        red_col[par, col] = jnp.sum(red_grp[par], axis=0)
        spread("col", red_col.at[par], red_col_sem.at[par], True)
        rows_batch(par, list(range(1, grp_size - 1)))
        arrive(par, *col_side, 1)
        rows_batch(par, [grp_size - 1])
        send("col", lambda peer: acc_row.at[peer], got_row.at[par, col], scatter_row_sem.at[par])
        got_row[par, col] = acc_row[col]
        arrive(par, *row_side, 0)
        cols_batch(par, 1, 3)
        arrive(par, *row_side, 1)
        cols_batch(par, 4, 2)
        arrive(par, *row_side, 2)
        cols_batch(par, 6, 2)

        def visit(n, carry):
            cols_batch(par, 4 * n, 4)
            return carry

        if col_size > 8:
            lax.fori_loop(2, col_size // 4, visit, 0)
        send("grp", lambda peer: acc_col.at[peer], got_col.at[par, grp], scatter_col_sem.at[par])
        got_col[par, grp] = acc_col[grp]

        spread("col", red_col.at[par], red_col_sem.at[par], False)
        total = unfold(jnp.sum(red_col[par], axis=0) / node_total)
        former = left_ref[lax.rem(k + ITERS, ITERS + 1)]
        turned = dot_nn(former[:, :width], total, HIGHEST)
        upper, inverse = factorize(total)
        left = inverse[:, :width]
        fresh = dot_nn(left, jnp.concatenate([block_r, lr_ref[...]], axis=1), HIGHEST)
        newest, image = fresh[:, :tile_size], fresh[:, tile_size:]
        pad = jnp.concatenate([inverse, jnp.zeros((LANES - width, LANES), F32)], axis=0)
        mixed = dot_nt(turned[:, :width], pad[:, :width], HIGHEST)
        older = (lane >= 2 * width) & (lane < 4 * width)
        coeffs = jnp.where(lane < width, mixed, jnp.where(older, turned, 0.0))
        stack[0] = newest
        lstack[0] = image
        now = dot_nn(coeffs, jnp.concatenate([stack[...].reshape(LANES, tile_size),
                                              lstack[...].reshape(LANES, tile_size)], axis=1), HIGHEST)
        rest = block_u - now[:, :tile_size]
        residual = dot_nn(left, rest, HIGHEST)
        on_block = jnp.sum(jnp.where(lane == row, turned, 0.0), axis=1, keepdims=True)
        on_gram = jnp.sum(jnp.where(lane == row + width, total, 0.0), axis=1, keepdims=True)
        mean = jnp.sum(on_block, axis=0, keepdims=True) / jnp.sum(on_gram, axis=0, keepdims=True)
        before = sigma_ref[...]
        sigma = before + jnp.broadcast_to(mean, sigma_ref.shape)
        known = now[:, tile_size:] + sigma * rest
        stack[0] = residual
        stack[1] = residual
        stack[k + 2] = newest
        lstack[k + 2] = image

        @pl.when(k == ITERS - 2)
        def _():
            shifted = [lstack[j] - sigma * stack[j] for j in (4, 2, 3)]
            block = jnp.concatenate([shifted[0], residual, shifted[1], shifted[2]] * 2, axis=0)
            early_grp[grp] = fold(dot_nt(residual, block, HIGHEST))
            spread("grp", early_grp, early_grp_sem, True)

        basis_ref[k] = newest
        left_ref[k] = inverse
        upper_ref[k] = upper
        coeff_ref[k] = coeffs
        sigma_ref[...] = sigma
        shift_ref[k] = before[:, :LANES]

        applied = collect(par, False) - known

        def renew():
            block_u = dot_nn(left, applied, HIGHEST)
            u_ref[1 - par] = block_u
            return block_u

        @pl.when(k < ITERS - 2)
        def _():
            lr_ref[...] = renew() + sigma * residual
            inner_products(1 - par, applied)
            depart(1 - par)

        @pl.when(k == ITERS - 2)
        def _():
            renew()

        return carry

    lax.fori_loop(0, ITERS - 1, step, 0)

    k = ITERS - 1
    par = ITERS % 2
    quarter = width // 4
    block_u, block_r = u_ref[par], stack[1]
    both = dot_nt(block_u, jnp.concatenate([block_r, block_u] * (LANES // (2 * width)), axis=0), HIGHEST)
    both = fold(both)
    odd = lax.rem(lax.div(lane[:quarter], 2 * width), 2) == 1
    late[grp * col_size + col] = jnp.where(odd, both[quarter:], both[:quarter])
    spread_all(late, late_sem)
    spread("grp", early_grp, early_grp_sem, False)
    early_col[col] = jnp.sum(early_grp[...], axis=0)
    spread("col", early_col, early_col_sem, True)
    proj_ref[...] = jnp.zeros_like(proj_ref)

    def keep_coeffs(k, left, coeffs, shift):
        found = dot_nn(left, coeffs, HIGHEST) + jnp.where(lane == row, shift, 0.0)
        for j in range(k):
            proj_ref[k, j] = found[:, (j + 2) * width : (j + 3) * width]
        proj_ref[k, k] = found[:, :width]

    for n in range(ITERS - 1):
        keep_coeffs(n, left_ref[n, :, :width], coeff_ref[n], shift_ref[n])
        factors_ref[n] = factor_of(upper_ref[n])
    spread("col", early_col, early_col_sem, False)
    total = unfold(jnp.sum(early_col[...], axis=0) / node_total)
    upper, inverse = factorize(total)
    left = inverse[:, :width]
    newest = dot_nn(left, block_r, HIGHEST)
    stack[0] = newest
    basis_ref[k] = newest
    factors_ref[k] = factor_of(upper)
    older = jnp.where((lane >= 2 * width) & (lane < 5 * width), total, 0.0)
    pad = jnp.concatenate([inverse, jnp.zeros((LANES - width, LANES), F32)], axis=0)[:, :width]
    await_all(late, late_sem)
    packed = jnp.sum(late[...], axis=0) / node_total
    total = jnp.concatenate(
        [packed] + [pltpu.roll(packed, LANES - n * 2 * width, 1) for n in range(1, 4)], axis=0
    )
    coeffs = dot_nt(total[:, :width], pad, HIGHEST) + older
    middle = jnp.zeros((width, LANES), F32)
    beside = jnp.concatenate([middle, coeffs] + [middle] * (LANES // width - 2), axis=0)
    gram = total - dot_nt(coeffs, beside, HIGHEST)
    rest = block_u - dot_nn(coeffs, stack[...].reshape(LANES, tile_size), HIGHEST)
    upper, inverse = factorize(gram)
    basis_ref[ITERS] = dot_nn(inverse[:, :width], rest, HIGHEST)
    factors_ref[ITERS] = dot_nt(left, upper[:, width : 2 * width], HIGHEST)
    keep_coeffs(k, left, coeffs, sigma_ref[:, :LANES])


def deliver(basis, proj, factors, basis_out, proj_out, factors_out, sem):
    pairs = ((basis, basis_out), (proj, proj_out), (factors, factors_out))
    copies = [pltpu.make_async_copy(source, target, sem.at[n]) for n, (source, target) in enumerate(pairs)]
    for copy in copies:
        copy.start()
    for copy in copies:
        copy.wait()


def solution(mesh):
    grp_size, col_size = mesh.shape["grp"], mesh.shape["col"]

    def body(start_block, tile_values, tile_row, tile_col, tile_count):
        width, shard_len = start_block.shape
        slots, tile_size = tile_values.shape[2], tile_values.shape[3]
        assert shard_len == tile_size and LANES // width == 8
        assert grp_size > 2 and col_size % CHUNK == 0
        assert grp_size & (grp_size - 1) == 0 and col_size & (col_size - 1) == 0
        places = LANES // width
        node_total = shard_len * grp_size * col_size
        spots = -(-max(grp_size * col_size, slots) // LANES) * LANES
        vmem = pl.BlockSpec(memory_space=pltpu.VMEM)
        smem = pl.BlockSpec(memory_space=pltpu.SMEM)
        hbm = pl.BlockSpec(memory_space=pl.ANY)
        block = (width, tile_size)
        line = (1, tile_size)
        tiles = (slots + 1, tile_size, tile_size)
        packed = (width // 2, LANES)
        small = (width, LANES)

        def sems(*sizes):
            return pltpu.SemaphoreType.DMA(sizes)

        def pinned(value):
            return pltpu.with_memory_space_constraint(value, pltpu.HBM)

        shapes = (
            jax.ShapeDtypeStruct((ITERS + 1,) + block, F32),
            jax.ShapeDtypeStruct((ITERS, ITERS, width, width), F32),
            jax.ShapeDtypeStruct((ITERS + 1, width, width), F32),
        )
        results = pl.pallas_call(
            functools.partial(kernel, grp_size, col_size, node_total),
            out_shape=shapes,
            in_specs=[hbm, hbm, hbm, hbm, smem],
            out_specs=(vmem, vmem, vmem),
            scratch_shapes=[
                pltpu.VMEM((slots, tile_size, tile_size), F32),
                pltpu.VMEM(tiles, F32),
                pltpu.VMEM(tiles, BF16),
                pltpu.VMEM(tiles, BF16),
                pltpu.VMEM(tiles, BF16),
                pltpu.VMEM(tiles, BF16),
                pltpu.VMEM((1, slots), I32),
                pltpu.VMEM((1, slots), I32),
                pltpu.VMEM((8, spots), I32),
                pltpu.SMEM((8, spots), I32),
                pltpu.VMEM((2,) + block, F32),
                pltpu.VMEM(block, F32),
                pltpu.VMEM((places,) + block, F32),
                pltpu.VMEM((places,) + block, F32),
                pltpu.VMEM((2, col_size) + block, F32),
                pltpu.VMEM((2, grp_size) + block, F32),
                pltpu.VMEM((col_size,) + block, F32),
                pltpu.VMEM((grp_size,) + block, F32),
                pltpu.VMEM((2, col_size) + block, F32),
                pltpu.VMEM((2, grp_size) + block, F32),
                pltpu.VMEM((col_size,) + line, F32),
                pltpu.VMEM((grp_size,) + line, F32),
                pltpu.VMEM((col_size,) + line, F32),
                pltpu.VMEM((grp_size,) + line, F32),
                pltpu.VMEM(line, F32),
                pltpu.VMEM(block, F32),
                pltpu.VMEM((ITERS,) + small, F32),
                pltpu.VMEM((ITERS + 1,) + small, F32),
                pltpu.VMEM((ITERS,) + small, F32),
                pltpu.VMEM((ITERS,) + small, F32),
                pltpu.VMEM((2, col_size) + packed, F32),
                pltpu.VMEM((2, grp_size) + packed, F32),
                pltpu.VMEM((grp_size,) + packed, F32),
                pltpu.VMEM((col_size,) + packed, F32),
                pltpu.VMEM((grp_size * col_size, width // 4, LANES), F32),
                sems(8 if slots % 8 == 0 else slots),
                sems(4),
                sems(2, 4), sems(2, 3), sems(2, 2), sems(2, 2),
                sems(2), sems(2), sems(2, 2), sems(2, 2), sems(2), sems(2), sems(2),
            ],
            compiler_params=pltpu.CompilerParams(
                collective_id=0, has_side_effects=True, vmem_limit_bytes=40 * 1024 * 1024
            ),
        )(
            pinned(start_block),
            pinned(tile_values.reshape(slots, tile_size, tile_size)),
            pinned(tile_row.reshape(1, slots)),
            pinned(tile_col.reshape(1, slots)),
            tile_count.reshape(1),
        )
        return pl.pallas_call(
            deliver,
            out_shape=shapes,
            in_specs=[vmem] * 3,
            out_specs=[hbm] * 3,
            scratch_shapes=[sems(3)],
        )(*(pltpu.with_memory_space_constraint(value, pltpu.VMEM) for value in results))

    in_specs = (
        P(None, ("grp", "col")),
        P("grp", "col", None, None, None),
        P("grp", "col", None),
        P("grp", "col", None),
        P("grp", "col"),
    )
    out_specs = (P(None, None, ("grp", "col")), P(), P())
    return jax.shard_map(body, mesh=mesh, in_specs=in_specs, out_specs=out_specs, check_vma=False)
```

```python
import functools

import jax
import jax.numpy as jnp
from jax import lax
from jax.experimental import pallas as pl
from jax.experimental.pallas import tpu as pltpu
from jax.sharding import PartitionSpec as P

ITERS = 4
HIGHEST = lax.Precision.HIGHEST
MESH = pl.DeviceIdType.MESH
F32 = jnp.float32
BF16 = jnp.bfloat16
I32 = jnp.int32
LANES = 128
CHUNK = 8
STRIDE = 8
UNROLL = 4


def dot_nt(left, right, precision=None):
    dims = (((1,), (1,)), ((), ()))
    return lax.dot_general(left, right, dims, precision=precision, preferred_element_type=F32)


def dot_nn(left, right, precision=None):
    dims = (((1,), (0,)), ((), ()))
    return lax.dot_general(left, right, dims, precision=precision, preferred_element_type=F32)


def split_two(value):
    high = value.astype(BF16)
    low = (value - high.astype(F32)).astype(BF16)
    return high, low


def factorize(gram):
    width = gram.shape[0]
    shape = gram.shape
    row = lax.broadcasted_iota(I32, shape, 0)
    lane = lax.broadcasted_iota(I32, shape, 1)
    unit = jnp.where(lane == row, 1.0, 0.0).astype(F32)
    work = jnp.where((lane >= width) & (lane < 2 * width), gram, unit)
    diagonal = jnp.ones(shape, F32)
    for base in range(0, width, STRIDE):
        tall = [jnp.broadcast_to(work[:, width + base + i : width + base + i + 1], shape) for i in range(STRIDE)]
        wide = [jnp.broadcast_to(work[base + i : base + i + 1, :], shape) for i in range(STRIDE)]
        cell = {
            (m, i): jnp.broadcast_to(tall[i][base + m : base + m + 1, :], shape)
            for i in range(STRIDE)
            for m in range(i, STRIDE)
        }
        for i in range(STRIDE):
            inverse = 1.0 / cell[i, i]
            diagonal = jnp.where(row == base + i, cell[i, i], diagonal)
            scale = jnp.where(row > base + i, tall[i] * inverse, 0.0)
            work = work - scale * wide[i]
            for m in range(i + 1, STRIDE):
                ratio = cell[m, i] * inverse
                wide[m] = wide[m] - ratio * wide[i]
                tall[m] = tall[m] - scale * cell[m, i]
                for n in range(m, STRIDE):
                    cell[n, m] = cell[n, m] - ratio * cell[n, i]
    work = work / jnp.sqrt(diagonal)
    upper = jnp.where((lane < 2 * width) & (lane >= row + width), work, 0.0)
    inverse = jnp.where(lane <= row, work, 0.0)
    return upper, inverse


def factor_of(upper):
    width = upper.shape[0]
    return upper[:, width : 2 * width].T


def flip(index, distance, size):
    total, bit = 0, 1
    while bit < size:
        total = total + bit * lax.rem(lax.div(index, bit) + lax.div(distance, bit), 2)
        bit *= 2
    return total


def kernel(
    grp_size, col_size, node_total,
    start_ref, tiles_ref, row_ref, col_ref, count_ref,
    basis_ref, proj_ref, factors_ref,
    raw, merged, high, low, high_t, low_t, rows_v, cols_v, table_v, table,
    u_ref, lr_ref, stack, lstack, row_panel, col_panel,
    acc_row, acc_col, got_row, got_col, deg_row, deg_col, deg_got_row, deg_got_col,
    degree_ref, sigma_ref, shift_ref, left_ref, upper_ref, coeff_ref, red_col, red_grp, early_grp, early_col, late,
    tile_sem, in_sem, gather_row_sem, gather_col_sem, scatter_row_sem, scatter_col_sem,
    deg_row_sem, deg_col_sem, red_col_sem, red_grp_sem, early_grp_sem, early_col_sem, late_sem,
):
    grp = lax.axis_index("grp")
    col = lax.axis_index("col")
    slots, tile_size = raw.shape[0], raw.shape[1]
    width = u_ref.shape[1]
    small = (width, LANES)
    row = lax.broadcasted_iota(I32, small, 0)
    lane = lax.broadcasted_iota(I32, small, 1)

    def other(t):
        dg, dc = lax.div(t, col_size), lax.rem(t, col_size)
        return flip(grp, dg, grp_size), flip(col, dc, col_size)

    loads_of = tile_sem.shape[0]
    share = slots // loads_of

    def load_tile(n):
        at = pl.ds(n * share, share)
        return pltpu.make_async_copy(tiles_ref.at[at], raw.at[at], tile_sem.at[n])

    loads = (
        pltpu.make_async_copy(start_ref, u_ref.at[0], in_sem.at[0]),
        pltpu.make_async_copy(row_ref, rows_v, in_sem.at[1]),
        pltpu.make_async_copy(col_ref, cols_v, in_sem.at[2]),
    )
    for copy in loads:
        copy.start()

    def start_load(s, carry):
        load_tile(s).start()
        return carry

    lax.fori_loop(0, loads_of, start_load, 0)

    barrier = pltpu.get_barrier_semaphore()

    def greet(t, carry):
        pl.semaphore_signal(barrier, inc=1, device_id=other(t), device_id_type=MESH)
        return carry

    everyone = grp_size * col_size
    lax.fori_loop(1, everyone, greet, 0, unroll=everyone <= 32)

    def copy_to(axis, d, source, target, send_sem, recv_sem):
        size = col_size if axis == "col" else grp_size
        peer = flip(col if axis == "col" else grp, d, size)
        return pltpu.make_async_remote_copy(
            src_ref=source(peer),
            dst_ref=target,
            send_sem=send_sem,
            recv_sem=recv_sem,
            device_id=(grp, peer) if axis == "col" else (peer, col),
            device_id_type=MESH,
        )

    def send(axis, source, target, sems):
        size = col_size if axis == "col" else grp_size

        def visit(d, carry):
            copy_to(axis, size - d, source, target, sems.at[0], sems.at[1]).start()
            return carry

        lax.fori_loop(1, size, visit, 0, unroll=size <= 8)

    def bytes_of(part, send_sem, recv_sem):
        return pltpu.make_async_remote_copy(
            src_ref=part, dst_ref=part, send_sem=send_sem, recv_sem=recv_sem,
            device_id=other(1), device_id_type=MESH,
        )

    def await_all(buf, sems):
        bytes_of(buf.at[pl.ds(0, buf.shape[0] - 1)], sems.at[0], sems.at[1]).wait()

    col_groups = ((1, grp_size - 1), (grp_size - 1, grp_size))
    row_groups = ((1, 4), (4, 6), (6, col_size))

    def gather(axis, par, panel, sems, groups):
        me = col if axis == "col" else grp
        for n, (low_d, high_d) in enumerate(groups):

            def visit(i, carry):
                d = low_d + i
                target = panel.at[par, me]
                copy_to(axis, d, lambda peer: u_ref.at[par], target, sems.at[par, 0], sems.at[par, n + 1]).start()
                return carry

            lax.fori_loop(0, high_d - low_d, visit, 0, unroll=high_d - low_d <= 8)

    def arrive(par, panel, sems, groups, n):
        count = groups[n][1] - groups[n][0]
        bytes_of(panel.at[par, pl.ds(0, count)], sems.at[par, 0], sems.at[par, n + 1]).wait_recv()

    def leave(par, panel, sems):
        count = panel.shape[1] - 1
        bytes_of(panel.at[par, pl.ds(0, count)], sems.at[par, 0], sems.at[par, 1]).wait_send()

    col_side = (col_panel, gather_col_sem, col_groups)
    row_side = (row_panel, gather_row_sem, row_groups)

    def spread(axis, buf, sems, start):
        me = col if axis == "col" else grp
        if start:
            send(axis, lambda peer: buf.at[me], buf.at[me], sems)
        else:
            await_all(buf, sems)

    def spread_all(buf, sems):
        me = grp * col_size + col

        def visit(t, carry):
            pltpu.make_async_remote_copy(
                src_ref=buf.at[me], dst_ref=buf.at[me], send_sem=sems.at[0], recv_sem=sems.at[1],
                device_id=other(everyone - t), device_id_type=MESH,
            ).start()
            return carry

        lax.fori_loop(1, everyone, visit, 0, unroll=everyone <= 32)

    def position(r, q):
        return table[0, r * grp_size + q]

    def send_rows(par, r, d, with_degree):
        sems = scatter_row_sem.at[par]
        copy_to("col", d, lambda peer: acc_row.at[r], got_row.at[par, col], sems.at[0], sems.at[1]).start()
        if with_degree:
            sems = deg_row_sem
            copy_to("col", d, lambda peer: deg_row.at[r], deg_got_row.at[col], sems.at[0], sems.at[1]).start()

    def combine(total, rest):
        piece = total[:width] + total[2 * width :] + rest[:width]
        return piece, total[width : width + 1] + rest[width : width + 1]

    def with_ones(pieces):
        ones = jnp.ones((width, tile_size), BF16)
        parts = [split_two(piece) for piece in pieces]
        return jnp.concatenate([jnp.concatenate([a, ones, b], axis=0) for a, b in parts], axis=1)

    def rows_of(r, left, places):
        at = [position(r, q) for q in places]
        firsts = jnp.concatenate([high_t[p] for p in at], axis=0)
        seconds = jnp.concatenate([low[p] for p in at], axis=1)
        return combine(dot_nn(left, firsts), dot_nt(left[: 2 * width], seconds))

    def cols_of(q, left, places):
        at = [position(r, q) for r in places]
        firsts = jnp.concatenate([high[p] for p in at], axis=0)
        seconds = jnp.concatenate([low[p] for p in at], axis=0)
        return combine(dot_nn(left, firsts), dot_nn(left[: 2 * width], seconds))

    def first_own():
        left = with_ones([u_ref[0]])

        def visit(r, carry):
            acc_row[r], deg_row[r] = rows_of(r, left, [grp])
            return carry

        lax.fori_loop(0, col_size, visit, 0, unroll=min(col_size, 8))
        for q in range(grp_size):
            acc_col[q], deg_col[q] = cols_of(q, left, [col])

    def first_rows():
        places = [flip(grp, d, grp_size) for d in range(1, grp_size)]
        left = with_ones([col_panel[0, q] for q in places])

        def visit(d):
            r = flip(col, d, col_size)
            piece, degree = rows_of(r, left, places)
            acc_row[r] = acc_row[r] + piece
            deg_row[r] = deg_row[r] + degree

        def go(ds):
            for d in ds:
                visit(d)
            for d in ds:
                if not isinstance(d, int) or d:
                    send_rows(0, flip(col, d, col_size), d, True)

        if col_size <= 8:
            go(range(col_size // 2, col_size))
            go(range(col_size // 2))
        else:
            def each(d, carry):
                go([d])
                return carry

            lax.fori_loop(1, col_size, each, 0)
            visit(0)
        got_row[0, col] = acc_row[col]
        deg_got_row[col] = deg_row[col]

    def first_cols():
        def batch(places):
            left = with_ones([row_panel[0, r] for r in places])
            for q in range(grp_size):
                piece, degree = cols_of(q, left, places)
                acc_col[q] = acc_col[q] + piece
                deg_col[q] = deg_col[q] + degree

        def visit(n, carry):
            batch([flip(col, n * CHUNK + i, col_size) for i in range(CHUNK)])
            return carry

        batch([flip(col, i, col_size) for i in range(1, CHUNK)])
        if col_size > CHUNK:
            lax.fori_loop(1, col_size // CHUNK, visit, 0)
        send("grp", lambda peer: acc_col.at[peer], got_col.at[0, grp], scatter_col_sem.at[0])
        got_col[0, grp] = acc_col[grp]
        send("grp", lambda peer: deg_col.at[peer], deg_got_col.at[grp], deg_col_sem)
        deg_got_col[grp] = deg_col[grp]

    def stacked(pieces):
        pairs = [split_two(piece) for piece in pieces]
        return jnp.concatenate([jnp.concatenate(pair, axis=0) for pair in pairs], axis=1)

    def product(left, firsts, seconds):
        total = dot_nn(left, jnp.concatenate(firsts, axis=0))
        rest = dot_nn(left[:width], jnp.concatenate(seconds, axis=0))
        return total[:width] + total[width:] + rest

    def rows_batch(par, ds):
        places = [flip(grp, d, grp_size) for d in ds]
        left = stacked([u_ref[par] if d == 0 else col_panel[par, q] for d, q in zip(ds, places)])

        def visit(r, carry):
            at = [position(r, q) for q in places]
            piece = product(left, [high_t[p] for p in at], [low_t[p] for p in at])
            acc_row[r] = piece if ds[0] == 0 else acc_row[r] + piece
            return carry

        if col_size <= 8:
            for r in range(col_size):
                visit(r, 0)
        else:
            lax.fori_loop(0, col_size, visit, 0)

    def cols_batch(par, base, count):
        places = [flip(col, base + i, col_size) for i in range(count)]
        own = isinstance(base, int) and base == 0
        left = stacked([u_ref[par]] if own else [row_panel[par, r] for r in places])
        for q in range(grp_size):
            at = [position(r, q) for r in places]
            piece = product(left, [high[p] for p in at], [low[p] for p in at])
            acc_col[q] = piece if own else acc_col[q] + piece

    def collect(par, with_degree):
        leave(par, col_panel, gather_col_sem)
        leave(par, row_panel, gather_row_sem)
        await_all(got_row.at[par], scatter_row_sem.at[par])
        await_all(got_col.at[par], scatter_col_sem.at[par])
        if with_degree:
            await_all(deg_got_row, deg_row_sem)
            await_all(deg_got_col, deg_col_sem)
            degree_ref[...] = jnp.sum(deg_got_row[...], axis=0) + jnp.sum(deg_got_col[...], axis=0)
        total = jnp.sum(got_row[par], axis=0) + jnp.sum(got_col[par], axis=0)
        return degree_ref[...] * u_ref[par] - total

    stack[...] = jnp.zeros_like(stack)
    lstack[...] = jnp.zeros_like(lstack)
    loads[1].wait()
    loads[2].wait()
    spots = table.shape[1]
    offset = rows_v[...] - grp * col_size
    pick = lax.div(cols_v[...] - col, col_size)
    place = jnp.clip(offset, 0, col_size - 1) * grp_size + jnp.clip(pick, 0, grp_size - 1)
    square = (slots, slots)
    down = lax.broadcasted_iota(I32, square, 0)
    across = lax.broadcasted_iota(I32, square, 1)
    wide = jnp.broadcast_to(place, square)
    tall = jnp.sum(jnp.where(down == across, wide, 0), axis=1, keepdims=True)
    same = (wide == jnp.broadcast_to(tall, square)) & (down < across)
    before = jnp.max(jnp.where(same, down, -1), axis=0, keepdims=True)
    before = jnp.where(before < 0, slots, before)
    long = (slots, spots)
    depth = lax.broadcasted_iota(I32, long, 0)
    spot = lax.broadcasted_iota(I32, long, 1)
    here = (jnp.broadcast_to(tall, long) == spot) & (depth < count_ref[0])
    last = jnp.max(jnp.where(here, depth, -1), axis=0, keepdims=True)
    table_v[0:1, :] = jnp.where(last < 0, slots, last)
    table_v[1:2, :slots] = before
    move = pltpu.make_async_copy(table_v, table, in_sem.at[3])
    move.start()
    empty = jnp.zeros((tile_size, tile_size), F32)
    merged[slots] = empty
    high[slots] = empty.astype(BF16)
    low[slots] = empty.astype(BF16)
    high_t[slots] = empty.astype(BF16)
    low_t[slots] = empty.astype(BF16)
    loads[0].wait()
    start = u_ref[0]
    stack[0] = start
    stack[1] = start
    pl.semaphore_wait(barrier, everyone - 1)
    gather("grp", 0, *col_side)
    gather("col", 0, *row_side)
    move.wait()

    def merge(n, carry):
        load_tile(n).wait()

        def visit(m, carry):
            s = n * share + m
            value = raw[s] + merged[table[1, s]]
            merged[s] = value
            first, second = split_two(value)
            high[s] = first
            high_t[s] = first.T
            low[s] = second
            return carry

        return lax.fori_loop(0, share, visit, carry, unroll=UNROLL)

    lax.fori_loop(0, loads_of, merge, 0)

    first_own()
    for n in range(len(col_groups)):
        arrive(0, *col_side, n)
    first_rows()
    for n in range(len(row_groups)):
        arrive(0, *row_side, n)
    first_cols()

    def turn(s, carry):
        low_t[s] = low[s].T
        return carry

    lax.fori_loop(0, slots, turn, 0, unroll=4)
    applied = collect(0, True)
    lr_ref[...] = applied
    u_ref[1] = applied
    sigma_ref[...] = jnp.zeros_like(sigma_ref)
    left_ref[ITERS] = jnp.where(lane == row, 1.0, 0.0)

    half = width // 2

    def fold(value):
        return jnp.where(lane[:half] < LANES // 2, value[:half], value[half:])

    def unfold(packed):
        turned = pltpu.roll(packed, LANES // 2, 1)
        low_lanes = lane[:half] < LANES // 2
        return jnp.concatenate(
            [jnp.where(low_lanes, packed, turned), jnp.where(low_lanes, turned, packed)], axis=0
        )

    def inner_products(par, block_v):
        block = stack[0:4].reshape(4 * width, tile_size)
        block = jnp.concatenate([block, block], axis=0)
        both = dot_nt(jnp.concatenate([block_v, stack[1]], axis=0), block, HIGHEST)
        inner = lax.rem(lane, 4 * width)
        red_grp[par, grp] = fold(jnp.where((inner >= width) & (inner < 2 * width), both[width:], both[:width]))
        spread("grp", red_grp.at[par], red_grp_sem.at[par], True)

    def depart(par):
        gather("grp", par, *col_side)
        gather("col", par, *row_side)

    depart(1)
    inner_products(1, applied)

    def step(k, carry):
        par = lax.rem(k + 1, 2)
        block_u, block_r = u_ref[par], stack[1]
        rows_batch(par, [0])
        cols_batch(par, 0, 1)
        arrive(par, *col_side, 0)
        rows_batch(par, list(range(1, grp_size - 1)))
        spread("grp", red_grp.at[par], red_grp_sem.at[par], False)
        red_col[par, col] = jnp.sum(red_grp[par], axis=0)
        spread("col", red_col.at[par], red_col_sem.at[par], True)
        arrive(par, *col_side, 1)
        rows_batch(par, [grp_size - 1])
        send("col", lambda peer: acc_row.at[peer], got_row.at[par, col], scatter_row_sem.at[par])
        got_row[par, col] = acc_row[col]
        arrive(par, *row_side, 0)
        cols_batch(par, 1, 3)
        arrive(par, *row_side, 1)
        cols_batch(par, 4, 2)
        arrive(par, *row_side, 2)
        cols_batch(par, 6, 2)

        def visit(n, carry):
            cols_batch(par, 4 * n, 4)
            return carry

        if col_size > 8:
            lax.fori_loop(2, col_size // 4, visit, 0)
        send("grp", lambda peer: acc_col.at[peer], got_col.at[par, grp], scatter_col_sem.at[par])
        got_col[par, grp] = acc_col[grp]

        spread("col", red_col.at[par], red_col_sem.at[par], False)
        total = unfold(jnp.sum(red_col[par], axis=0) / node_total)
        former = left_ref[lax.rem(k + ITERS, ITERS + 1)]
        turned = dot_nn(former[:, :width], total, HIGHEST)
        upper, inverse = factorize(total)
        left = inverse[:, :width]
        fresh = dot_nn(left, jnp.concatenate([block_r, lr_ref[...]], axis=1), HIGHEST)
        newest, image = fresh[:, :tile_size], fresh[:, tile_size:]
        pad = jnp.concatenate([inverse, jnp.zeros((LANES - width, LANES), F32)], axis=0)
        mixed = dot_nt(turned[:, :width], pad[:, :width], HIGHEST)
        older = (lane >= 2 * width) & (lane < 4 * width)
        coeffs = jnp.where(lane < width, mixed, jnp.where(older, turned, 0.0))
        stack[0] = newest
        lstack[0] = image
        now = dot_nn(coeffs, jnp.concatenate([stack[...].reshape(LANES, tile_size),
                                              lstack[...].reshape(LANES, tile_size)], axis=1), HIGHEST)
        rest = block_u - now[:, :tile_size]
        residual = dot_nn(left, rest, HIGHEST)
        on_block = jnp.sum(jnp.where(lane == row, turned, 0.0), axis=1, keepdims=True)
        on_gram = jnp.sum(jnp.where(lane == row + width, total, 0.0), axis=1, keepdims=True)
        mean = jnp.sum(on_block, axis=0, keepdims=True) / jnp.sum(on_gram, axis=0, keepdims=True)
        before = sigma_ref[...]
        sigma = before + jnp.broadcast_to(mean, sigma_ref.shape)
        known = now[:, tile_size:] + sigma * rest
        stack[0] = residual
        stack[1] = residual
        stack[k + 2] = newest
        lstack[k + 2] = image

        @pl.when(k == ITERS - 2)
        def _():
            shifted = [lstack[j] - sigma * stack[j] for j in (4, 2, 3)]
            block = jnp.concatenate([shifted[0], residual, shifted[1], shifted[2]] * 2, axis=0)
            early_grp[grp] = fold(dot_nt(residual, block, HIGHEST))
            spread("grp", early_grp, early_grp_sem, True)

        basis_ref[k] = newest
        left_ref[k] = inverse
        upper_ref[k] = upper
        coeff_ref[k] = coeffs
        sigma_ref[...] = sigma
        shift_ref[k] = before[:, :LANES]

        applied = collect(par, False) - known

        def renew():
            block_u = dot_nn(left, applied, HIGHEST)
            u_ref[1 - par] = block_u
            return block_u

        @pl.when(k < ITERS - 2)
        def _():
            block_u = renew()
            depart(1 - par)
            inner_products(1 - par, applied)
            lr_ref[...] = block_u + sigma * residual

        @pl.when(k == ITERS - 2)
        def _():
            renew()

        return carry

    lax.fori_loop(0, ITERS - 1, step, 0)

    k = ITERS - 1
    par = ITERS % 2
    quarter = width // 4
    block_u, block_r = u_ref[par], stack[1]
    both = dot_nt(block_u, jnp.concatenate([block_r, block_u] * (LANES // (2 * width)), axis=0), HIGHEST)
    both = fold(both)
    odd = lax.rem(lax.div(lane[:quarter], 2 * width), 2) == 1
    late[grp * col_size + col] = jnp.where(odd, both[quarter:], both[:quarter])
    spread_all(late, late_sem)
    spread("grp", early_grp, early_grp_sem, False)
    early_col[col] = jnp.sum(early_grp[...], axis=0)
    spread("col", early_col, early_col_sem, True)
    proj_ref[...] = jnp.zeros_like(proj_ref)

    def keep_coeffs(k, left, coeffs, shift):
        found = dot_nn(left, coeffs, HIGHEST) + jnp.where(lane == row, shift, 0.0)
        for j in range(k):
            proj_ref[k, j] = found[:, (j + 2) * width : (j + 3) * width]
        proj_ref[k, k] = found[:, :width]

    for n in range(ITERS - 1):
        keep_coeffs(n, left_ref[n, :, :width], coeff_ref[n], shift_ref[n])
        factors_ref[n] = factor_of(upper_ref[n])
    spread("col", early_col, early_col_sem, False)
    total = unfold(jnp.sum(early_col[...], axis=0) / node_total)
    upper, inverse = factorize(total)
    left = inverse[:, :width]
    newest = dot_nn(left, block_r, HIGHEST)
    stack[0] = newest
    basis_ref[k] = newest
    factors_ref[k] = factor_of(upper)
    older = jnp.where((lane >= 2 * width) & (lane < 5 * width), total, 0.0)
    pad = jnp.concatenate([inverse, jnp.zeros((LANES - width, LANES), F32)], axis=0)[:, :width]
    await_all(late, late_sem)
    packed = jnp.sum(late[...], axis=0) / node_total
    total = jnp.concatenate(
        [packed] + [pltpu.roll(packed, LANES - n * 2 * width, 1) for n in range(1, 4)], axis=0
    )
    coeffs = dot_nt(total[:, :width], pad, HIGHEST) + older
    middle = jnp.zeros((width, LANES), F32)
    beside = jnp.concatenate([middle, coeffs] + [middle] * (LANES // width - 2), axis=0)
    gram = total - dot_nt(coeffs, beside, HIGHEST)
    rest = block_u - dot_nn(coeffs, stack[...].reshape(LANES, tile_size), HIGHEST)
    upper, inverse = factorize(gram)
    basis_ref[ITERS] = dot_nn(inverse[:, :width], rest, HIGHEST)
    factors_ref[ITERS] = dot_nt(left, upper[:, width : 2 * width], HIGHEST)
    keep_coeffs(k, left, coeffs, sigma_ref[:, :LANES])


def deliver(basis, proj, factors, basis_out, proj_out, factors_out, sem):
    pairs = ((basis, basis_out), (proj, proj_out), (factors, factors_out))
    copies = [pltpu.make_async_copy(source, target, sem.at[n]) for n, (source, target) in enumerate(pairs)]
    for copy in copies:
        copy.start()
    for copy in copies:
        copy.wait()


def solution(mesh):
    grp_size, col_size = mesh.shape["grp"], mesh.shape["col"]

    def body(start_block, tile_values, tile_row, tile_col, tile_count):
        width, shard_len = start_block.shape
        slots, tile_size = tile_values.shape[2], tile_values.shape[3]
        assert shard_len == tile_size and LANES // width == 8
        assert grp_size > 2 and col_size % CHUNK == 0
        assert grp_size & (grp_size - 1) == 0 and col_size & (col_size - 1) == 0
        places = LANES // width
        node_total = shard_len * grp_size * col_size
        spots = -(-max(grp_size * col_size, slots) // LANES) * LANES
        vmem = pl.BlockSpec(memory_space=pltpu.VMEM)
        smem = pl.BlockSpec(memory_space=pltpu.SMEM)
        hbm = pl.BlockSpec(memory_space=pl.ANY)
        block = (width, tile_size)
        line = (1, tile_size)
        tiles = (slots + 1, tile_size, tile_size)
        packed = (width // 2, LANES)
        small = (width, LANES)

        def sems(*sizes):
            return pltpu.SemaphoreType.DMA(sizes)

        def pinned(value):
            return pltpu.with_memory_space_constraint(value, pltpu.HBM)

        shapes = (
            jax.ShapeDtypeStruct((ITERS + 1,) + block, F32),
            jax.ShapeDtypeStruct((ITERS, ITERS, width, width), F32),
            jax.ShapeDtypeStruct((ITERS + 1, width, width), F32),
        )
        results = pl.pallas_call(
            functools.partial(kernel, grp_size, col_size, node_total),
            out_shape=shapes,
            in_specs=[hbm, hbm, hbm, hbm, smem],
            out_specs=(vmem, vmem, vmem),
            scratch_shapes=[
                pltpu.VMEM((slots, tile_size, tile_size), F32),
                pltpu.VMEM(tiles, F32),
                pltpu.VMEM(tiles, BF16),
                pltpu.VMEM(tiles, BF16),
                pltpu.VMEM(tiles, BF16),
                pltpu.VMEM(tiles, BF16),
                pltpu.VMEM((1, slots), I32),
                pltpu.VMEM((1, slots), I32),
                pltpu.VMEM((8, spots), I32),
                pltpu.SMEM((8, spots), I32),
                pltpu.VMEM((2,) + block, F32),
                pltpu.VMEM(block, F32),
                pltpu.VMEM((places,) + block, F32),
                pltpu.VMEM((places,) + block, F32),
                pltpu.VMEM((2, col_size) + block, F32),
                pltpu.VMEM((2, grp_size) + block, F32),
                pltpu.VMEM((col_size,) + block, F32),
                pltpu.VMEM((grp_size,) + block, F32),
                pltpu.VMEM((2, col_size) + block, F32),
                pltpu.VMEM((2, grp_size) + block, F32),
                pltpu.VMEM((col_size,) + line, F32),
                pltpu.VMEM((grp_size,) + line, F32),
                pltpu.VMEM((col_size,) + line, F32),
                pltpu.VMEM((grp_size,) + line, F32),
                pltpu.VMEM(line, F32),
                pltpu.VMEM(block, F32),
                pltpu.VMEM((ITERS,) + small, F32),
                pltpu.VMEM((ITERS + 1,) + small, F32),
                pltpu.VMEM((ITERS,) + small, F32),
                pltpu.VMEM((ITERS,) + small, F32),
                pltpu.VMEM((2, col_size) + packed, F32),
                pltpu.VMEM((2, grp_size) + packed, F32),
                pltpu.VMEM((grp_size,) + packed, F32),
                pltpu.VMEM((col_size,) + packed, F32),
                pltpu.VMEM((grp_size * col_size, width // 4, LANES), F32),
                sems(8 if slots % 8 == 0 else slots),
                sems(4),
                sems(2, 4), sems(2, 3), sems(2, 2), sems(2, 2),
                sems(2), sems(2), sems(2, 2), sems(2, 2), sems(2), sems(2), sems(2),
            ],
            compiler_params=pltpu.CompilerParams(
                collective_id=0, has_side_effects=True, vmem_limit_bytes=40 * 1024 * 1024
            ),
        )(
            pinned(start_block),
            pinned(tile_values.reshape(slots, tile_size, tile_size)),
            pinned(tile_row.reshape(1, slots)),
            pinned(tile_col.reshape(1, slots)),
            tile_count.reshape(1),
        )
        return pl.pallas_call(
            deliver,
            out_shape=shapes,
            in_specs=[vmem] * 3,
            out_specs=[hbm] * 3,
            scratch_shapes=[sems(3)],
        )(*(pltpu.with_memory_space_constraint(value, pltpu.VMEM) for value in results))

    in_specs = (
        P(None, ("grp", "col")),
        P("grp", "col", None, None, None),
        P("grp", "col", None),
        P("grp", "col", None),
        P("grp", "col"),
    )
    out_specs = (P(None, None, ("grp", "col")), P(), P())
    return jax.shard_map(body, mesh=mesh, in_specs=in_specs, out_specs=out_specs, check_vma=False)
```

```python
import functools

import jax
import jax.numpy as jnp
from jax import lax
from jax.experimental import pallas as pl
from jax.experimental.pallas import tpu as pltpu
from jax.sharding import PartitionSpec as P

ITERS = 4
HIGHEST = lax.Precision.HIGHEST
MESH = pl.DeviceIdType.MESH
F32 = jnp.float32
BF16 = jnp.bfloat16
I32 = jnp.int32
LANES = 128
CHUNK = 8
STRIDE = 8
UNROLL = 4


def dot_nt(left, right, precision=None):
    dims = (((1,), (1,)), ((), ()))
    return lax.dot_general(left, right, dims, precision=precision, preferred_element_type=F32)


def dot_nn(left, right, precision=None):
    dims = (((1,), (0,)), ((), ()))
    return lax.dot_general(left, right, dims, precision=precision, preferred_element_type=F32)


def split_two(value):
    high = value.astype(BF16)
    low = (value - high.astype(F32)).astype(BF16)
    return high, low


def factorize(gram):
    width = gram.shape[0]
    shape = gram.shape
    row = lax.broadcasted_iota(I32, shape, 0)
    lane = lax.broadcasted_iota(I32, shape, 1)
    unit = jnp.where(lane == row, 1.0, 0.0).astype(F32)
    work = jnp.where((lane >= width) & (lane < 2 * width), gram, unit)
    diagonal = jnp.ones(shape, F32)
    for base in range(0, width, STRIDE):
        tall = [jnp.broadcast_to(work[:, width + base + i : width + base + i + 1], shape) for i in range(STRIDE)]
        wide = [jnp.broadcast_to(work[base + i : base + i + 1, :], shape) for i in range(STRIDE)]
        cell = {
            (m, i): jnp.broadcast_to(tall[i][base + m : base + m + 1, :], shape)
            for i in range(STRIDE)
            for m in range(i, STRIDE)
        }
        for i in range(STRIDE):
            inverse = 1.0 / cell[i, i]
            diagonal = jnp.where(row == base + i, cell[i, i], diagonal)
            scale = jnp.where(row > base + i, tall[i] * inverse, 0.0)
            work = work - scale * wide[i]
            for m in range(i + 1, STRIDE):
                ratio = cell[m, i] * inverse
                wide[m] = wide[m] - ratio * wide[i]
                tall[m] = tall[m] - scale * cell[m, i]
                for n in range(m, STRIDE):
                    cell[n, m] = cell[n, m] - ratio * cell[n, i]
    work = work / jnp.sqrt(diagonal)
    upper = jnp.where((lane < 2 * width) & (lane >= row + width), work, 0.0)
    inverse = jnp.where(lane <= row, work, 0.0)
    return upper, inverse


def factor_of(upper):
    width = upper.shape[0]
    return upper[:, width : 2 * width].T


def flip(index, distance, size):
    total, bit = 0, 1
    while bit < size:
        total = total + bit * lax.rem(lax.div(index, bit) + lax.div(distance, bit), 2)
        bit *= 2
    return total


def kernel(
    grp_size, col_size, node_total,
    start_ref, tiles_ref, row_ref, col_ref, count_ref,
    basis_ref, proj_ref, factors_ref,
    raw, merged, high, low, high_t, low_t, rows_v, cols_v, table_v, table,
    u_ref, lr_ref, stack, lstack, row_panel, col_panel,
    acc_row, acc_col, got_row, got_col, deg_row, deg_col, deg_got_row, deg_got_col,
    degree_ref, sigma_ref, shift_ref, left_ref, upper_ref, coeff_ref, red_col, red_grp, early_grp, early_col, late,
    tile_sem, in_sem, gather_row_sem, gather_col_sem, scatter_row_sem, scatter_col_sem,
    deg_row_sem, deg_col_sem, red_col_sem, red_grp_sem, early_grp_sem, early_col_sem, late_sem,
):
    grp = lax.axis_index("grp")
    col = lax.axis_index("col")
    slots, tile_size = raw.shape[0], raw.shape[1]
    width = u_ref.shape[1]
    small = (width, LANES)
    row = lax.broadcasted_iota(I32, small, 0)
    lane = lax.broadcasted_iota(I32, small, 1)

    def other(t):
        dg, dc = lax.div(t, col_size), lax.rem(t, col_size)
        return flip(grp, dg, grp_size), flip(col, dc, col_size)

    loads_of = tile_sem.shape[0]
    share = slots // loads_of

    def load_tile(n):
        at = pl.ds(n * share, share)
        return pltpu.make_async_copy(tiles_ref.at[at], raw.at[at], tile_sem.at[n])

    loads = (
        pltpu.make_async_copy(start_ref, u_ref.at[0], in_sem.at[0]),
        pltpu.make_async_copy(row_ref, rows_v, in_sem.at[1]),
        pltpu.make_async_copy(col_ref, cols_v, in_sem.at[2]),
    )
    for copy in loads:
        copy.start()

    def start_load(s, carry):
        load_tile(s).start()
        return carry

    lax.fori_loop(0, loads_of, start_load, 0)

    barrier = pltpu.get_barrier_semaphore()

    def greet(t, carry):
        pl.semaphore_signal(barrier, inc=1, device_id=other(t), device_id_type=MESH)
        return carry

    everyone = grp_size * col_size
    lax.fori_loop(1, everyone, greet, 0, unroll=everyone <= 32)

    def copy_to(axis, d, source, target, send_sem, recv_sem):
        size = col_size if axis == "col" else grp_size
        peer = flip(col if axis == "col" else grp, d, size)
        return pltpu.make_async_remote_copy(
            src_ref=source(peer),
            dst_ref=target,
            send_sem=send_sem,
            recv_sem=recv_sem,
            device_id=(grp, peer) if axis == "col" else (peer, col),
            device_id_type=MESH,
        )

    def send(axis, source, target, sems):
        size = col_size if axis == "col" else grp_size

        def visit(d, carry):
            copy_to(axis, size - d, source, target, sems.at[0], sems.at[1]).start()
            return carry

        lax.fori_loop(1, size, visit, 0, unroll=size <= 8)

    def bytes_of(part, send_sem, recv_sem):
        return pltpu.make_async_remote_copy(
            src_ref=part, dst_ref=part, send_sem=send_sem, recv_sem=recv_sem,
            device_id=other(1), device_id_type=MESH,
        )

    def await_all(buf, sems):
        bytes_of(buf.at[pl.ds(0, buf.shape[0] - 1)], sems.at[0], sems.at[1]).wait()

    col_groups = ((1, grp_size - 1), (grp_size - 1, grp_size))
    row_groups = ((1, 4), (4, 6), (6, col_size))

    def gather(axis, par, panel, sems, groups):
        me = col if axis == "col" else grp
        for n, (low_d, high_d) in enumerate(groups):

            def visit(i, carry):
                d = low_d + i
                target = panel.at[par, me]
                copy_to(axis, d, lambda peer: u_ref.at[par], target, sems.at[par, 0], sems.at[par, n + 1]).start()
                return carry

            lax.fori_loop(0, high_d - low_d, visit, 0, unroll=high_d - low_d <= 8)

    def arrive(par, panel, sems, groups, n):
        count = groups[n][1] - groups[n][0]
        bytes_of(panel.at[par, pl.ds(0, count)], sems.at[par, 0], sems.at[par, n + 1]).wait_recv()

    def leave(par, panel, sems):
        count = panel.shape[1] - 1
        bytes_of(panel.at[par, pl.ds(0, count)], sems.at[par, 0], sems.at[par, 1]).wait_send()

    col_side = (col_panel, gather_col_sem, col_groups)
    row_side = (row_panel, gather_row_sem, row_groups)

    def spread(axis, buf, sems, start):
        me = col if axis == "col" else grp
        if start:
            send(axis, lambda peer: buf.at[me], buf.at[me], sems)
        else:
            await_all(buf, sems)

    def spread_all(buf, sems):
        me = grp * col_size + col

        def visit(t, carry):
            pltpu.make_async_remote_copy(
                src_ref=buf.at[me], dst_ref=buf.at[me], send_sem=sems.at[0], recv_sem=sems.at[1],
                device_id=other(everyone - t), device_id_type=MESH,
            ).start()
            return carry

        lax.fori_loop(1, everyone, visit, 0, unroll=everyone <= 32)

    def position(r, q):
        return table[0, r * grp_size + q]

    def send_rows(par, r, d, with_degree):
        sems = scatter_row_sem.at[par]
        copy_to("col", d, lambda peer: acc_row.at[r], got_row.at[par, col], sems.at[0], sems.at[1]).start()
        if with_degree:
            sems = deg_row_sem
            copy_to("col", d, lambda peer: deg_row.at[r], deg_got_row.at[col], sems.at[0], sems.at[1]).start()

    def combine(total, rest):
        piece = total[:width] + total[2 * width :] + rest[:width]
        return piece, total[width : width + 1] + rest[width : width + 1]

    def with_ones(pieces):
        ones = jnp.ones((width, tile_size), BF16)
        parts = [split_two(piece) for piece in pieces]
        return jnp.concatenate([jnp.concatenate([a, ones, b], axis=0) for a, b in parts], axis=1)

    def rows_of(r, left, places):
        at = [position(r, q) for q in places]
        firsts = jnp.concatenate([high_t[p] for p in at], axis=0)
        seconds = jnp.concatenate([low[p] for p in at], axis=1)
        return combine(dot_nn(left, firsts), dot_nt(left[: 2 * width], seconds))

    def cols_of(q, left, places):
        at = [position(r, q) for r in places]
        firsts = jnp.concatenate([high[p] for p in at], axis=0)
        seconds = jnp.concatenate([low[p] for p in at], axis=0)
        return combine(dot_nn(left, firsts), dot_nn(left[: 2 * width], seconds))

    def first_own():
        left = with_ones([u_ref[0]])

        def visit(r, carry):
            acc_row[r], deg_row[r] = rows_of(r, left, [grp])
            return carry

        lax.fori_loop(0, col_size, visit, 0, unroll=min(col_size, 8))
        for q in range(grp_size):
            acc_col[q], deg_col[q] = cols_of(q, left, [col])

    def first_rows():
        places = [flip(grp, d, grp_size) for d in range(1, grp_size)]
        left = with_ones([col_panel[0, q] for q in places])

        def visit(d):
            r = flip(col, d, col_size)
            piece, degree = rows_of(r, left, places)
            acc_row[r] = acc_row[r] + piece
            deg_row[r] = deg_row[r] + degree

        def go(ds):
            for d in ds:
                visit(d)
            for d in ds:
                if not isinstance(d, int) or d:
                    send_rows(0, flip(col, d, col_size), d, True)

        if col_size <= 8:
            go(range(col_size // 2, col_size))
            go(range(col_size // 2))
        else:
            def each(d, carry):
                go([d])
                return carry

            lax.fori_loop(1, col_size, each, 0)
            visit(0)
        got_row[0, col] = acc_row[col]
        deg_got_row[col] = deg_row[col]

    def first_cols():
        def batch(places):
            left = with_ones([row_panel[0, r] for r in places])
            for q in range(grp_size):
                piece, degree = cols_of(q, left, places)
                acc_col[q] = acc_col[q] + piece
                deg_col[q] = deg_col[q] + degree

        def visit(n, carry):
            batch([flip(col, n * CHUNK + i, col_size) for i in range(CHUNK)])
            return carry

        batch([flip(col, i, col_size) for i in range(1, CHUNK)])
        if col_size > CHUNK:
            lax.fori_loop(1, col_size // CHUNK, visit, 0)
        send("grp", lambda peer: acc_col.at[peer], got_col.at[0, grp], scatter_col_sem.at[0])
        got_col[0, grp] = acc_col[grp]
        send("grp", lambda peer: deg_col.at[peer], deg_got_col.at[grp], deg_col_sem)
        deg_got_col[grp] = deg_col[grp]

    def stacked(pieces):
        pairs = [split_two(piece) for piece in pieces]
        return jnp.concatenate([jnp.concatenate(pair, axis=0) for pair in pairs], axis=1)

    def product(left, firsts, seconds):
        total = dot_nn(left, jnp.concatenate(firsts, axis=0))
        rest = dot_nn(left[:width], jnp.concatenate(seconds, axis=0))
        return total[:width] + total[width:] + rest

    def rows_batch(par, ds):
        places = [flip(grp, d, grp_size) for d in ds]
        left = stacked([u_ref[par] if d == 0 else col_panel[par, q] for d, q in zip(ds, places)])

        def visit(r, carry):
            at = [position(r, q) for q in places]
            piece = product(left, [high_t[p] for p in at], [low_t[p] for p in at])
            acc_row[r] = piece if ds[0] == 0 else acc_row[r] + piece
            return carry

        if col_size <= 8:
            for r in range(col_size):
                visit(r, 0)
        else:
            lax.fori_loop(0, col_size, visit, 0)

    def cols_batch(par, base, count):
        places = [flip(col, base + i, col_size) for i in range(count)]
        own = isinstance(base, int) and base == 0
        left = stacked([u_ref[par]] if own else [row_panel[par, r] for r in places])
        for q in range(grp_size):
            at = [position(r, q) for r in places]
            piece = product(left, [high[p] for p in at], [low[p] for p in at])
            acc_col[q] = piece if own else acc_col[q] + piece

    def collect(par, with_degree):
        leave(par, col_panel, gather_col_sem)
        leave(par, row_panel, gather_row_sem)
        await_all(got_row.at[par], scatter_row_sem.at[par])
        await_all(got_col.at[par], scatter_col_sem.at[par])
        if with_degree:
            await_all(deg_got_row, deg_row_sem)
            await_all(deg_got_col, deg_col_sem)
            degree_ref[...] = jnp.sum(deg_got_row[...], axis=0) + jnp.sum(deg_got_col[...], axis=0)
        total = jnp.sum(got_row[par], axis=0) + jnp.sum(got_col[par], axis=0)
        return degree_ref[...] * u_ref[par] - total

    stack[...] = jnp.zeros_like(stack)
    lstack[...] = jnp.zeros_like(lstack)
    loads[1].wait()
    loads[2].wait()
    spots = table.shape[1]
    offset = rows_v[...] - grp * col_size
    pick = lax.div(cols_v[...] - col, col_size)
    place = jnp.clip(offset, 0, col_size - 1) * grp_size + jnp.clip(pick, 0, grp_size - 1)
    square = (slots, slots)
    down = lax.broadcasted_iota(I32, square, 0)
    across = lax.broadcasted_iota(I32, square, 1)
    wide = jnp.broadcast_to(place, square)
    tall = jnp.sum(jnp.where(down == across, wide, 0), axis=1, keepdims=True)
    same = (wide == jnp.broadcast_to(tall, square)) & (down < across)
    before = jnp.max(jnp.where(same, down, -1), axis=0, keepdims=True)
    before = jnp.where(before < 0, slots, before)
    long = (slots, spots)
    depth = lax.broadcasted_iota(I32, long, 0)
    spot = lax.broadcasted_iota(I32, long, 1)
    here = (jnp.broadcast_to(tall, long) == spot) & (depth < count_ref[0])
    last = jnp.max(jnp.where(here, depth, -1), axis=0, keepdims=True)
    table_v[0:1, :] = jnp.where(last < 0, slots, last)
    table_v[1:2, :slots] = before
    move = pltpu.make_async_copy(table_v, table, in_sem.at[3])
    move.start()
    empty = jnp.zeros((tile_size, tile_size), F32)
    merged[slots] = empty
    high[slots] = empty.astype(BF16)
    low[slots] = empty.astype(BF16)
    high_t[slots] = empty.astype(BF16)
    low_t[slots] = empty.astype(BF16)
    loads[0].wait()
    start = u_ref[0]
    stack[0] = start
    stack[1] = start
    pl.semaphore_wait(barrier, everyone - 1)
    gather("grp", 0, *col_side)
    gather("col", 0, *row_side)
    move.wait()

    def merge(n, carry):
        load_tile(n).wait()

        def visit(m, carry):
            s = n * share + m
            value = raw[s] + merged[table[1, s]]
            merged[s] = value
            first, second = split_two(value)
            high[s] = first
            high_t[s] = first.T
            low[s] = second
            return carry

        return lax.fori_loop(0, share, visit, carry, unroll=UNROLL)

    lax.fori_loop(0, loads_of, merge, 0)

    first_own()
    for n in range(len(col_groups)):
        arrive(0, *col_side, n)
    first_rows()
    for n in range(len(row_groups)):
        arrive(0, *row_side, n)
    first_cols()

    def turn(s, carry):
        low_t[s] = low[s].T
        return carry

    lax.fori_loop(0, slots, turn, 0, unroll=4)
    applied = collect(0, True)
    lr_ref[...] = applied
    u_ref[1] = applied
    sigma_ref[...] = jnp.zeros_like(sigma_ref)
    left_ref[ITERS] = jnp.where(lane == row, 1.0, 0.0)

    half = width // 2

    def fold(value):
        return jnp.where(lane[:half] < LANES // 2, value[:half], value[half:])

    def unfold(packed):
        turned = pltpu.roll(packed, LANES // 2, 1)
        low_lanes = lane[:half] < LANES // 2
        return jnp.concatenate(
            [jnp.where(low_lanes, packed, turned), jnp.where(low_lanes, turned, packed)], axis=0
        )

    def inner_products(par, block_v):
        block = stack[0:4].reshape(4 * width, tile_size)
        block = jnp.concatenate([block, block], axis=0)
        both = dot_nt(jnp.concatenate([block_v, stack[1]], axis=0), block, HIGHEST)
        inner = lax.rem(lane, 4 * width)
        red_grp[par, grp] = fold(jnp.where((inner >= width) & (inner < 2 * width), both[width:], both[:width]))
        spread("grp", red_grp.at[par], red_grp_sem.at[par], True)

    def depart(par):
        gather("grp", par, *col_side)
        gather("col", par, *row_side)

    depart(1)
    inner_products(1, applied)

    def step(k, carry):
        par = lax.rem(k + 1, 2)
        block_u, block_r = u_ref[par], stack[1]
        rows_batch(par, [0])
        cols_batch(par, 0, 1)
        arrive(par, *col_side, 0)
        rows_batch(par, list(range(1, grp_size - 1)))
        spread("grp", red_grp.at[par], red_grp_sem.at[par], False)
        red_col[par, col] = jnp.sum(red_grp[par], axis=0)
        spread("col", red_col.at[par], red_col_sem.at[par], True)
        arrive(par, *col_side, 1)
        rows_batch(par, [grp_size - 1])
        send("col", lambda peer: acc_row.at[peer], got_row.at[par, col], scatter_row_sem.at[par])
        got_row[par, col] = acc_row[col]
        arrive(par, *row_side, 0)
        cols_batch(par, 1, 3)
        arrive(par, *row_side, 1)
        cols_batch(par, 4, 2)
        arrive(par, *row_side, 2)
        cols_batch(par, 6, 2)

        def visit(n, carry):
            cols_batch(par, 4 * n, 4)
            return carry

        if col_size > 8:
            lax.fori_loop(2, col_size // 4, visit, 0)
        send("grp", lambda peer: acc_col.at[peer], got_col.at[par, grp], scatter_col_sem.at[par])
        got_col[par, grp] = acc_col[grp]

        spread("col", red_col.at[par], red_col_sem.at[par], False)
        total = unfold(jnp.sum(red_col[par], axis=0) / node_total)
        former = left_ref[lax.rem(k + ITERS, ITERS + 1)]
        turned = dot_nn(former[:, :width], total, HIGHEST)
        upper, inverse = factorize(total)
        left = inverse[:, :width]
        fresh = dot_nn(left, jnp.concatenate([block_r, lr_ref[...]], axis=1), HIGHEST)
        newest, image = fresh[:, :tile_size], fresh[:, tile_size:]
        pad = jnp.concatenate([inverse, jnp.zeros((LANES - width, LANES), F32)], axis=0)
        mixed = dot_nt(turned[:, :width], pad[:, :width], HIGHEST)
        older = (lane >= 2 * width) & (lane < 4 * width)
        coeffs = jnp.where(lane < width, mixed, jnp.where(older, turned, 0.0))
        stack[0] = newest
        lstack[0] = image
        now = dot_nn(coeffs, jnp.concatenate([stack[...].reshape(LANES, tile_size),
                                              lstack[...].reshape(LANES, tile_size)], axis=1), HIGHEST)
        rest = block_u - now[:, :tile_size]
        residual = dot_nn(left, rest, HIGHEST)
        on_block = jnp.sum(jnp.where(lane == row, turned, 0.0), axis=1, keepdims=True)
        on_gram = jnp.sum(jnp.where(lane == row + width, total, 0.0), axis=1, keepdims=True)
        mean = jnp.sum(on_block, axis=0, keepdims=True) / jnp.sum(on_gram, axis=0, keepdims=True)
        before = sigma_ref[...]
        sigma = before + jnp.broadcast_to(mean, sigma_ref.shape)
        known = now[:, tile_size:] + sigma * rest
        stack[0] = residual
        stack[1] = residual
        stack[k + 2] = newest
        lstack[k + 2] = image

        @pl.when(k == ITERS - 2)
        def _():
            shifted = [lstack[j] - sigma * stack[j] for j in (4, 2, 3)]
            block = jnp.concatenate([shifted[0], residual, shifted[1], shifted[2]] * 2, axis=0)
            early_grp[grp] = fold(dot_nt(residual, block, HIGHEST))
            spread("grp", early_grp, early_grp_sem, True)

        basis_ref[k] = newest
        left_ref[k] = inverse
        upper_ref[k] = upper
        coeff_ref[k] = coeffs
        sigma_ref[...] = sigma
        shift_ref[k] = before[:, :LANES]

        applied = collect(par, False) - known

        def renew():
            block_u = dot_nn(left, applied, HIGHEST)
            u_ref[1 - par] = block_u
            return block_u

        @pl.when(k < ITERS - 2)
        def _():
            block_u = renew()
            depart(1 - par)
            inner_products(1 - par, applied)
            lr_ref[...] = block_u + sigma * residual

        @pl.when(k == ITERS - 2)
        def _():
            renew()

        return carry

    lax.fori_loop(0, ITERS - 1, step, 0)

    k = ITERS - 1
    par = ITERS % 2
    quarter = width // 4
    block_u, block_r = u_ref[par], stack[1]
    both = dot_nt(block_u, jnp.concatenate([block_r, block_u] * (LANES // (2 * width)), axis=0), HIGHEST)
    both = fold(both)
    odd = lax.rem(lax.div(lane[:quarter], 2 * width), 2) == 1
    late[grp * col_size + col] = jnp.where(odd, both[quarter:], both[:quarter])
    spread_all(late, late_sem)
    spread("grp", early_grp, early_grp_sem, False)
    early_col[col] = jnp.sum(early_grp[...], axis=0)
    spread("col", early_col, early_col_sem, True)
    proj_ref[...] = jnp.zeros_like(proj_ref)

    def keep_coeffs(k, left, coeffs, shift):
        found = dot_nn(left, coeffs, HIGHEST) + jnp.where(lane == row, shift, 0.0)
        for j in range(k):
            proj_ref[k, j] = found[:, (j + 2) * width : (j + 3) * width]
        proj_ref[k, k] = found[:, :width]

    for n in range(ITERS - 1):
        keep_coeffs(n, left_ref[n, :, :width], coeff_ref[n], shift_ref[n])
        factors_ref[n] = factor_of(upper_ref[n])
    await_all(late, late_sem)
    packed = jnp.sum(late[...], axis=0) / node_total
    newer = jnp.concatenate(
        [packed] + [pltpu.roll(packed, LANES - n * 2 * width, 1) for n in range(1, 4)], axis=0
    )
    spread("col", early_col, early_col_sem, False)
    total = unfold(jnp.sum(early_col[...], axis=0) / node_total)
    upper, inverse = factorize(total)
    left = inverse[:, :width]
    newest = dot_nn(left, block_r, HIGHEST)
    stack[0] = newest
    basis_ref[k] = newest
    factors_ref[k] = factor_of(upper)
    older = jnp.where((lane >= 2 * width) & (lane < 5 * width), total, 0.0)
    pad = jnp.concatenate([inverse, jnp.zeros((LANES - width, LANES), F32)], axis=0)[:, :width]
    coeffs = dot_nt(newer[:, :width], pad, HIGHEST) + older
    middle = jnp.zeros((width, LANES), F32)
    beside = jnp.concatenate([middle, coeffs] + [middle] * (LANES // width - 2), axis=0)
    gram = newer - dot_nt(coeffs, beside, HIGHEST)
    rest = block_u - dot_nn(coeffs, stack[...].reshape(LANES, tile_size), HIGHEST)
    upper, inverse = factorize(gram)
    basis_ref[ITERS] = dot_nn(inverse[:, :width], rest, HIGHEST)
    factors_ref[ITERS] = dot_nt(left, upper[:, width : 2 * width], HIGHEST)
    keep_coeffs(k, left, coeffs, sigma_ref[:, :LANES])


def deliver(basis, proj, factors, basis_out, proj_out, factors_out, sem):
    pairs = ((basis, basis_out), (proj, proj_out), (factors, factors_out))
    copies = [pltpu.make_async_copy(source, target, sem.at[n]) for n, (source, target) in enumerate(pairs)]
    for copy in copies:
        copy.start()
    for copy in copies:
        copy.wait()


def solution(mesh):
    grp_size, col_size = mesh.shape["grp"], mesh.shape["col"]

    def body(start_block, tile_values, tile_row, tile_col, tile_count):
        width, shard_len = start_block.shape
        slots, tile_size = tile_values.shape[2], tile_values.shape[3]
        assert shard_len == tile_size and LANES // width == 8
        assert grp_size > 2 and col_size % CHUNK == 0
        assert grp_size & (grp_size - 1) == 0 and col_size & (col_size - 1) == 0
        places = LANES // width
        node_total = shard_len * grp_size * col_size
        spots = -(-max(grp_size * col_size, slots) // LANES) * LANES
        vmem = pl.BlockSpec(memory_space=pltpu.VMEM)
        smem = pl.BlockSpec(memory_space=pltpu.SMEM)
        hbm = pl.BlockSpec(memory_space=pl.ANY)
        block = (width, tile_size)
        line = (1, tile_size)
        tiles = (slots + 1, tile_size, tile_size)
        packed = (width // 2, LANES)
        small = (width, LANES)

        def sems(*sizes):
            return pltpu.SemaphoreType.DMA(sizes)

        def pinned(value):
            return pltpu.with_memory_space_constraint(value, pltpu.HBM)

        shapes = (
            jax.ShapeDtypeStruct((ITERS + 1,) + block, F32),
            jax.ShapeDtypeStruct((ITERS, ITERS, width, width), F32),
            jax.ShapeDtypeStruct((ITERS + 1, width, width), F32),
        )
        results = pl.pallas_call(
            functools.partial(kernel, grp_size, col_size, node_total),
            out_shape=shapes,
            in_specs=[hbm, hbm, hbm, hbm, smem],
            out_specs=(vmem, vmem, vmem),
            scratch_shapes=[
                pltpu.VMEM((slots, tile_size, tile_size), F32),
                pltpu.VMEM(tiles, F32),
                pltpu.VMEM(tiles, BF16),
                pltpu.VMEM(tiles, BF16),
                pltpu.VMEM(tiles, BF16),
                pltpu.VMEM(tiles, BF16),
                pltpu.VMEM((1, slots), I32),
                pltpu.VMEM((1, slots), I32),
                pltpu.VMEM((8, spots), I32),
                pltpu.SMEM((8, spots), I32),
                pltpu.VMEM((2,) + block, F32),
                pltpu.VMEM(block, F32),
                pltpu.VMEM((places,) + block, F32),
                pltpu.VMEM((places,) + block, F32),
                pltpu.VMEM((2, col_size) + block, F32),
                pltpu.VMEM((2, grp_size) + block, F32),
                pltpu.VMEM((col_size,) + block, F32),
                pltpu.VMEM((grp_size,) + block, F32),
                pltpu.VMEM((2, col_size) + block, F32),
                pltpu.VMEM((2, grp_size) + block, F32),
                pltpu.VMEM((col_size,) + line, F32),
                pltpu.VMEM((grp_size,) + line, F32),
                pltpu.VMEM((col_size,) + line, F32),
                pltpu.VMEM((grp_size,) + line, F32),
                pltpu.VMEM(line, F32),
                pltpu.VMEM(block, F32),
                pltpu.VMEM((ITERS,) + small, F32),
                pltpu.VMEM((ITERS + 1,) + small, F32),
                pltpu.VMEM((ITERS,) + small, F32),
                pltpu.VMEM((ITERS,) + small, F32),
                pltpu.VMEM((2, col_size) + packed, F32),
                pltpu.VMEM((2, grp_size) + packed, F32),
                pltpu.VMEM((grp_size,) + packed, F32),
                pltpu.VMEM((col_size,) + packed, F32),
                pltpu.VMEM((grp_size * col_size, width // 4, LANES), F32),
                sems(8 if slots % 8 == 0 else slots),
                sems(4),
                sems(2, 4), sems(2, 3), sems(2, 2), sems(2, 2),
                sems(2), sems(2), sems(2, 2), sems(2, 2), sems(2), sems(2), sems(2),
            ],
            compiler_params=pltpu.CompilerParams(
                collective_id=0, has_side_effects=True, vmem_limit_bytes=40 * 1024 * 1024
            ),
        )(
            pinned(start_block),
            pinned(tile_values.reshape(slots, tile_size, tile_size)),
            pinned(tile_row.reshape(1, slots)),
            pinned(tile_col.reshape(1, slots)),
            tile_count.reshape(1),
        )
        return pl.pallas_call(
            deliver,
            out_shape=shapes,
            in_specs=[vmem] * 3,
            out_specs=[hbm] * 3,
            scratch_shapes=[sems(3)],
        )(*(pltpu.with_memory_space_constraint(value, pltpu.VMEM) for value in results))

    in_specs = (
        P(None, ("grp", "col")),
        P("grp", "col", None, None, None),
        P("grp", "col", None),
        P("grp", "col", None),
        P("grp", "col"),
    )
    out_specs = (P(None, None, ("grp", "col")), P(), P())
    return jax.shard_map(body, mesh=mesh, in_specs=in_specs, out_specs=out_specs, check_vma=False)
```
